32 devices in a mesh: dp: 1 (over z), tp: 32 (over y, x, core).
Axes of the slice: x: 4, y: 4, z: 1, core: 2. Of those that a mesh axis runs over, the one named last changes fastest.
The devices are a block of a 4x4x8 slice.
Arguments:
- x_norm: bfloat16 [256, 5120], P(('dp', 'tp'))
- w_gate: bfloat16 [5120, 13824], P(None, 'tp')
- w_up: bfloat16 [5120, 13824], P(None, 'tp')
- w_down: bfloat16 [13824, 5120], P('tp')
- u_gate: bfloat16 [256, 13824], P('dp', 'tp')
- u_up: bfloat16 [256, 13824], P('dp', 'tp')
- grad_out: bfloat16 [256, 5120], P(('dp', 'tp'))
Outputs:
- output 1: bfloat16 [256, 5120], P(('dp', 'tp'))
- output 2: float32 [5120, 13824], P('dp', 'tp')
- output 3: float32 [5120, 13824], P('dp', 'tp')
- output 4: float32 [13824, 5120], P(('dp', 'tp'))
All inputs are finite; a program needn't handle non-finite values.
Results may differ from the reference program's by a relative error of at most 0.0134744.
Values are sent between devices in bfloat16 or wider.
A program may use at most 768 MiB of HBM per device.

```python
import jax
import jax.numpy as jnp
from jax import lax

HIDDEN = 5120
FFN_DIM = 13824
TOKENS = 256
GROUP_SIZE = 32


def setup_inputs(seed: int = 0, part: int = 0) -> dict:
    base_key = jax.random.key(seed)
    w_keys = jax.random.split(base_key, 3)
    part_keys = jax.random.split(jax.random.fold_in(base_key, part), 4)
    w_gate = (jax.random.normal(w_keys[0], (HIDDEN, FFN_DIM), jnp.float32) * HIDDEN ** -0.5).astype(jnp.bfloat16)
    w_up = (jax.random.normal(w_keys[1], (HIDDEN, FFN_DIM), jnp.float32) * HIDDEN ** -0.5).astype(jnp.bfloat16)
    w_down = (jax.random.normal(w_keys[2], (FFN_DIM, HIDDEN), jnp.float32) * FFN_DIM ** -0.5).astype(jnp.bfloat16)
    x_norm = jax.random.normal(part_keys[0], (TOKENS, HIDDEN), jnp.float32).astype(jnp.bfloat16)
    u_gate = jax.random.normal(part_keys[1], (TOKENS, FFN_DIM), jnp.float32).astype(jnp.bfloat16)
    u_up = jax.random.normal(part_keys[2], (TOKENS, FFN_DIM), jnp.float32).astype(jnp.bfloat16)
    grad_out = jax.random.normal(part_keys[3], (TOKENS, HIDDEN), jnp.float32).astype(jnp.bfloat16)
    return dict(x_norm=x_norm, w_gate=w_gate, w_up=w_up, w_down=w_down, u_gate=u_gate, u_up=u_up, grad_out=grad_out)


def reference(x_norm, w_gate, w_up, w_down, u_gate, u_up, grad_out):
    col_block = FFN_DIM // GROUP_SIZE
    wg_blocks = w_gate.reshape(HIDDEN, GROUP_SIZE, col_block).transpose(1, 0, 2)
    wu_blocks = w_up.reshape(HIDDEN, GROUP_SIZE, col_block).transpose(1, 0, 2)
    wd_blocks = w_down.reshape(GROUP_SIZE, col_block, HIDDEN)
    ug_blocks = u_gate.reshape(TOKENS, GROUP_SIZE, col_block).transpose(1, 0, 2)
    uu_blocks = u_up.reshape(TOKENS, GROUP_SIZE, col_block).transpose(1, 0, 2)

    def one_block(dx_acc, operands):
        wg_blk, wu_blk, wd_blk, ug_blk, uu_blk = operands
        gate_f = ug_blk.astype(jnp.float32)
        up_f = uu_blk.astype(jnp.float32)
        sigmoid_g = jax.nn.sigmoid(gate_f)
        silu_g = gate_f * sigmoid_g
        z_act = (silu_g * up_f).astype(jnp.bfloat16)
        grad_wd = jnp.dot(z_act.T, grad_out, preferred_element_type=jnp.float32)
        grad_mid = jnp.dot(grad_out, wd_blk.T, preferred_element_type=jnp.float32)
        d_gate = (grad_mid * up_f * sigmoid_g * (1.0 + gate_f * (1.0 - sigmoid_g))).astype(jnp.bfloat16)
        d_up = (grad_mid * silu_g).astype(jnp.bfloat16)
        partial = (jnp.dot(d_gate, wg_blk.T, preferred_element_type=jnp.float32)
                   + jnp.dot(d_up, wu_blk.T, preferred_element_type=jnp.float32)).astype(jnp.bfloat16)
        grad_wg = jnp.dot(x_norm.T, d_gate, preferred_element_type=jnp.float32)
        grad_wu = jnp.dot(x_norm.T, d_up, preferred_element_type=jnp.float32)
        return dx_acc + partial.astype(jnp.float32), (grad_wg, grad_wu, grad_wd)

    dx_init = jnp.zeros((TOKENS, HIDDEN), jnp.float32)
    dx_sum, stacked = lax.scan(one_block, dx_init, (wg_blocks, wu_blocks, wd_blocks, ug_blocks, uu_blocks))
    gw_gate, gw_up, gw_down = stacked
    grad_x = dx_sum.astype(jnp.bfloat16)
    grad_w_gate = gw_gate.transpose(1, 0, 2).reshape(HIDDEN, FFN_DIM)
    grad_w_up = gw_up.transpose(1, 0, 2).reshape(HIDDEN, FFN_DIM)
    grad_w_down = gw_down.reshape(FFN_DIM, HIDDEN)
    return (grad_x, grad_w_gate, grad_w_up, grad_w_down)
```

```python
import math

import jax
import jax.numpy as jnp
from jax import lax
from jax.experimental import pallas as pl
from jax.experimental.pallas import tpu as pltpu
from jax.sharding import PartitionSpec as P

MESH = pl.DeviceIdType.MESH
BF16 = jnp.bfloat16
F32 = jnp.float32
CORES = 2
COL_TILE = 512
VMEM_BYTES = 67043328
NT = (((1,), (1,)), ((), ()))


def comm_kernel(ring, n_copies, x_hbm, dy_hbm, wd_hbm, wg_hbm, wu_hbm, ug_hbm, uu_hbm,
                dx_ref, xf, dyf, dg_t, du_t, z_t,
                wd, wg, wu, ug, uu, gate, up, dgs, dus, pb, pr, sx, sy,
                lf, mg, rw, rm, lf_y, mg_y, rw_y, rm_y, lsem, ssem, rsem):
    R = ring
    me = lax.axis_index("tp")
    c = lax.rem(me, CORES)
    x = lax.rem(me // CORES, R)
    y = me // (CORES * R)
    oc = 1 - c
    rows, hidden = x_hbm.shape
    ch = R * CORES * rows
    H2 = hidden // 2
    LO, HI = pl.ds(0, H2), pl.ds(H2, H2)
    xs = [lax.rem(x + d, R) for d in range(R)]
    ys = [lax.rem(y + d, R) for d in range(R)]

    def dev(yy, xx, cc):
        return {"tp": (yy * R + xx) * CORES + cc}

    xp, xm = dev(y, xs[1], c), dev(y, xs[R - 1], c)
    yp, ym = dev(ys[1], x, c), dev(ys[R - 1], x, c)
    mate = dev(y, x, oc)

    def local(src, dst, i):
        cp = pltpu.make_async_copy(src, dst, lsem.at[i])
        cp.start()
        return cp

    cp_dy = local(dy_hbm, dyf.at[y, x, c], 0)
    cp_x = local(x_hbm, xf.at[y, x, c], 1)
    cp_ug = local(ug_hbm, ug, 2)
    cp_uu = local(uu_hbm, uu, 3)
    cp_wd = local(wd_hbm, wd, 4)
    cp_wg = local(wg_hbm, wg, 5)
    cp_wu = local(wu_hbm, wu, 6)

    barrier = pltpu.get_barrier_semaphore()
    for d in (xp, xm, yp, ym, mate):
        pl.semaphore_signal(barrier, inc=1, device_id=d, device_id_type=MESH)
    pl.semaphore_wait(barrier, 5)

    sent = []

    def send(src, dst, device):
        i = len(sent)
        cp = pltpu.make_async_remote_copy(src_ref=src, dst_ref=dst, send_sem=ssem.at[i], recv_sem=rsem.at[i],
                                          device_id=device, device_id_type=MESH)
        cp.start()
        sent.append(cp)
        return cp

    class Gather:
        def __init__(self, buf):
            self.buf = buf
            self.mate = {}
            self.yp, self.ym, self.yfp, self.yfm = {}, {}, {}, {}

        def to_mate(self, dy_, dx_):
            ref = self.buf.at[ys[dy_], xs[dx_], c]
            self.mate[dy_, dx_] = send(ref, ref, mate)

        def x_send(self):
            ref = self.buf.at[y, x, c]
            self.sp, self.sm = send(ref, ref, xp), send(ref, ref, xm)

        def x_recv_near(self):
            self.sp.wait_recv()
            ref = self.buf.at[y, xs[R - 1], c, :, LO]
            self.fp = send(ref, ref, xp)
            self.sm.wait_recv()
            ref = self.buf.at[y, xs[1], c, :, HI]
            self.fm = send(ref, ref, xm)

        def x_recv_far(self):
            self.fp.wait_recv()
            self.fm.wait_recv()

        def y_send(self, d):
            ref = self.buf.at[y, xs[d], c]
            self.yp[d] = send(ref, ref, yp)
            self.ym[d] = send(ref, ref, ym)

        def y_recv_near(self, d):
            self.yp[d].wait_recv()
            ref = self.buf.at[ys[R - 1], xs[d], c, :, LO]
            self.yfp[d] = send(ref, ref, yp)
            self.ym[d].wait_recv()
            ref = self.buf.at[ys[1], xs[d], c, :, HI]
            self.yfm[d] = send(ref, ref, ym)
            self.to_mate(R - 1, d)
            self.to_mate(1, d)

        def y_recv_far(self, d):
            self.yfp[d].wait_recv()
            self.yfm[d].wait_recv()
            self.to_mate(2, d)

        def mate_recv(self, dy_):
            for d in range(R):
                self.mate[dy_, d].wait_recv()

    gd, gx = Gather(dyf), Gather(xf)
    cp_dy.wait()
    gd.x_send()
    gd.y_send(0)
    gd.to_mate(0, 0)
    cp_x.wait()
    gx.x_send()
    gx.to_mate(0, 0)

    cp_ug.wait()
    cp_uu.wait()
    g_f = ug[...].astype(F32)
    u_f = uu[...].astype(F32)
    z_t[...] = (g_f * jax.nn.sigmoid(g_f) * u_f).astype(BF16)
    gate[...] = g_f.T
    up[...] = u_f.T

    gd.x_recv_near()
    gd.y_send(R - 1)
    gd.y_send(1)
    gd.to_mate(0, R - 1)
    gd.to_mate(0, 1)
    gd.y_recv_near(0)
    gx.x_recv_near()
    gx.to_mate(0, R - 1)
    gx.to_mate(0, 1)
    gd.x_recv_far()
    gd.y_send(2)
    gd.to_mate(0, 2)
    gd.y_recv_near(R - 1)
    gd.y_recv_near(1)
    gx.x_recv_far()
    gx.to_mate(0, 2)

    order = (0, 1, R - 1, 2)

    def grads(k):
        yy = ys[k]
        tok = pl.ds(pl.multiple_of(yy * ch, ch), ch)
        dyc = dyf[yy].reshape(ch, hidden)
        g_mid = lax.dot_general(dyc, wd[...], NT, preferred_element_type=F32)
        g_f, u_f = gate[tok, :], up[tok, :]
        s = jax.nn.sigmoid(g_f)
        dg = (g_mid * u_f * s * (1.0 + g_f * (1.0 - s))).astype(BF16)
        du = (g_mid * (g_f * s)).astype(BF16)
        dgs[tok, :] = dg
        dus[tok, :] = du

    def partial(k, half):
        yy = ys[k]
        tok = pl.ds(pl.multiple_of(yy * ch, ch), ch)
        dg, du = dgs[tok, :], dus[tok, :]

        @pl.loop(0, H2 // COL_TILE)
        def _(t):
            cols = pl.ds(pl.multiple_of(half * H2 + t * COL_TILE, COL_TILE), COL_TILE)
            p = (jnp.dot(dg, wg[:, cols], preferred_element_type=F32)
                 + jnp.dot(du, wu[:, cols], preferred_element_type=F32))
            pb[k, :, :, :, cols] = p.astype(BF16).reshape(R, CORES, rows, COL_TILE)

        cols = (LO, HI)[half]
        return send(pb.at[k, :, oc, :, cols], pr.at[k, :, :, cols], mate)

    def pair_sum(k, half, cp):
        cp.wait_recv()
        cols = (LO, HI)[half]
        for j in range(R):
            sx[k, j, :, cols] = pb[k, j, c, :, cols].astype(F32) + pr[k, j, :, cols].astype(F32)

    leaf, raw, merged = {}, {}, {}

    def scatter_first(k):
        leaf[k] = (send(sx.at[k, xs[2], :, LO], lf.at[k, 0], xp), send(sx.at[k, xs[2], :, HI], lf.at[k, 1], xm))
        raw[k] = (send(sx.at[k, xs[1], :, HI], rw.at[k, 0], xp), send(sx.at[k, xs[R - 1], :, LO], rw.at[k, 1], xm))

    def scatter_merge(k):
        leaf[k][0].wait_recv()
        mg[k, 0] = lf[k, 0] + sx[k, xs[1], :, LO]
        a = send(mg.at[k, 0], rm.at[k, 0], xp)
        leaf[k][1].wait_recv()
        mg[k, 1] = lf[k, 1] + sx[k, xs[R - 1], :, HI]
        merged[k] = (a, send(mg.at[k, 1], rm.at[k, 1], xm))

    def scatter_last(k):
        for cp in raw[k] + merged[k]:
            cp.wait_recv()
        sy[k, :, LO] = sx[k, x, :, LO] + rm[k, 0] + rw[k, 1]
        sy[k, :, HI] = sx[k, x, :, HI] + rw[k, 0] + rm[k, 1]

    gd.mate_recv(0)
    cp_wd.wait()
    grads(0)
    gd.y_recv_near(2)
    cp_wg.wait()
    cp_wu.wait()
    p0 = partial(0, 0)
    gd.y_recv_far(0)
    gd.y_recv_far(R - 1)
    gd.y_recv_far(1)
    p1 = partial(0, 1)
    pair_sum(0, 0, p0)
    pair_sum(0, 1, p1)
    scatter_first(0)
    gd.y_recv_far(2)
    for d in (0, R - 1, 1, 2):
        gx.y_send(d)
    gd.mate_recv(1)
    grads(1)
    p0 = partial(1, 0)
    scatter_merge(0)
    p1 = partial(1, 1)
    pair_sum(1, 0, p0)
    pair_sum(1, 1, p1)
    scatter_first(1)
    gd.mate_recv(R - 1)
    grads(R - 1)
    p0 = partial(R - 1, 0)
    gx.y_recv_near(0)
    scatter_last(0)
    scatter_merge(1)
    p1 = partial(R - 1, 1)
    pair_sum(R - 1, 0, p0)
    pair_sum(R - 1, 1, p1)
    scatter_first(R - 1)
    gx.y_recv_near(R - 1)
    gd.mate_recv(2)
    grads(2)
    p0 = partial(2, 0)
    gx.y_recv_near(1)
    scatter_merge(R - 1)
    p1 = partial(2, 1)
    pair_sum(2, 0, p0)
    pair_sum(2, 1, p1)
    scatter_first(2)
    gx.y_recv_near(2)
    dg_t[...] = dgs[...].astype(F32).T.astype(BF16)
    du_t[...] = dus[...].astype(F32).T.astype(BF16)
    scatter_last(1)
    raw_p = send(sy.at[1, :, HI], rw_y.at[0], yp)
    scatter_merge(2)
    scatter_last(R - 1)
    raw_m = send(sy.at[R - 1, :, LO], rw_y.at[1], ym)
    for d in (0, R - 1, 1, 2):
        gx.y_recv_far(d)
    scatter_last(2)
    leaf_p = send(sy.at[2, :, LO], lf_y.at[0], yp)
    leaf_m = send(sy.at[2, :, HI], lf_y.at[1], ym)
    leaf_p.wait_recv()
    mg_y[0] = lf_y[0] + sy[1, :, LO]
    mp = send(mg_y.at[0], rm_y.at[0], yp)
    leaf_m.wait_recv()
    mg_y[1] = lf_y[1] + sy[R - 1, :, HI]
    mm = send(mg_y.at[1], rm_y.at[1], ym)
    for k in range(R):
        gx.mate_recv(k)
    for cp in (raw_p, raw_m, mp, mm):
        cp.wait_recv()
    dx_ref[:, LO] = (sy[0, :, LO] + rm_y[0] + rw_y[1]).astype(BF16)
    dx_ref[:, HI] = (sy[0, :, HI] + rw_y[0] + rm_y[1]).astype(BF16)
    for cp in sent:
        cp.wait_send()
    assert len(sent) == n_copies, len(sent)


def weight_kernel(xf, dyf, dg_t, du_t, z_t, og, ou, od):
    tile = og.shape[1]
    tokens = dg_t.shape[1]
    cols = pl.ds(pl.multiple_of(pl.program_id(0) * tile, tile), tile)
    xc = xf[:, :, :, :, cols].reshape(tokens, tile)
    og[...] = jnp.dot(dg_t[...], xc, preferred_element_type=F32)
    ou[...] = jnp.dot(du_t[...], xc, preferred_element_type=F32)
    od[...] = jnp.dot(z_t[...], dyf[:, :, :, :, cols].reshape(tokens, tile), preferred_element_type=F32)


def solution(mesh):
    tp = mesh.shape["tp"]
    ring = math.isqrt(tp // CORES)

    def local_backward(x_loc, wg_loc, wu_loc, wd_loc, ug_loc, uu_loc, dy_loc):
        rows, hidden = x_loc.shape
        ffn = wd_loc.shape[0]
        tokens = tp * rows
        H2 = hidden // 2
        R = ring
        n_copies = 2 * (4 + 4 * R + R * R) + 8 * R + 6
        full = (R, R, CORES, rows, hidden)
        half = (rows, H2)
        vm = pltpu.VMEM
        out_bytes = 2 * (rows * hidden + 2 * tokens * hidden + 3 * ffn * tokens)
        dx, xf, dyf, dg_t, du_t, z_t = pl.pallas_call(
            lambda *refs: comm_kernel(R, n_copies, *refs),
            name="comm",
            out_shape=(vm((rows, hidden), BF16), vm(full, BF16), vm(full, BF16),
                       vm((ffn, tokens), BF16), vm((ffn, tokens), BF16), vm((ffn, tokens), BF16)),
            in_specs=[pl.BlockSpec(memory_space=pltpu.HBM)] * 7,
            out_specs=(pl.BlockSpec(memory_space=vm),) * 6,
            scratch_shapes=[
                vm((ffn, hidden), BF16), vm((ffn, hidden), BF16), vm((ffn, hidden), BF16),
                vm((ffn, tokens), BF16), vm((ffn, tokens), BF16),
                vm((tokens, ffn), F32), vm((tokens, ffn), F32),
                vm((tokens, ffn), BF16), vm((tokens, ffn), BF16),
                vm((R,) + full[1:], BF16), vm((R, R, rows, hidden), BF16),
                vm((R, R, rows, hidden), F32), vm((R, rows, hidden), F32),
                vm((R, 2) + half, F32), vm((R, 2) + half, F32), vm((R, 2) + half, F32), vm((R, 2) + half, F32),
                vm((2,) + half, F32), vm((2,) + half, F32), vm((2,) + half, F32), vm((2,) + half, F32),
                pltpu.SemaphoreType.DMA((7,)),
                pltpu.SemaphoreType.DMA((n_copies,)),
                pltpu.SemaphoreType.DMA((n_copies,)),
            ],
            compiler_params=pltpu.CompilerParams(collective_id=0, has_side_effects=True, vmem_limit_bytes=VMEM_BYTES - out_bytes - 40960),
        )(x_loc, dy_loc, wd_loc, wg_loc.T, wu_loc.T, ug_loc.T, uu_loc.T)
        out = jax.ShapeDtypeStruct((ffn, hidden), F32)
        ospec = pl.BlockSpec((ffn, COL_TILE), lambda j: (0, j))
        gw_g, gw_u, gw_d = pl.pallas_call(
            weight_kernel,
            name="weight_grads",
            grid=(hidden // COL_TILE,),
            out_shape=(out, out, out),
            in_specs=[pl.BlockSpec(memory_space=vm)] * 5,
            out_specs=(ospec, ospec, ospec),
            compiler_params=pltpu.CompilerParams(vmem_limit_bytes=24 << 20),
        )(xf, dyf, dg_t, du_t, z_t)
        return dx, gw_g.T, gw_u.T, gw_d

    row_spec = P(("dp", "tp"), None)
    col_spec = P(None, "tp")
    part_cols = P("dp", "tp")
    return jax.shard_map(local_backward, mesh=mesh,
                         in_specs=(row_spec, col_spec, col_spec, P("tp", None), part_cols, part_cols, row_spec),
                         out_specs=(row_spec, part_cols, part_cols, row_spec),
                         check_vma=False)
```

```python
import math

import jax
import jax.numpy as jnp
from jax import lax
from jax.experimental import pallas as pl
from jax.experimental.pallas import tpu as pltpu
from jax.sharding import PartitionSpec as P

MESH = pl.DeviceIdType.MESH
BF16 = jnp.bfloat16
F32 = jnp.float32
CORES = 2
COL_TILE = 512
MXU_TILE = 256
GROUPS = 2
VMEM_BYTES = 67043328
NT = (((1,), (1,)), ((), ()))


def comm_kernel(ring, n_copies, x_hbm, dy_hbm, wd_hbm, wg_hbm, wu_hbm, ug_hbm, uu_hbm,
                dx_ref, xf, dyf, dg_t, du_t, z_t,
                wd, wg, wu, ug, uu, gate, up, mid, dgs, dus, pb, pr, sx, sy,
                lf, mg, rw, rm, lf2, mg2, rw2, rm2, lsem, ssem, rsem):
    R = ring
    me = lax.axis_index("tp")
    c = lax.rem(me, CORES)
    x = lax.rem(me // CORES, R)
    y = me // (CORES * R)
    oc = 1 - c
    rows, hidden = x_hbm.shape
    tokens = R * R * CORES * rows
    H2, Q = hidden // 2, hidden // 4
    xs = [lax.rem(x + d, R) for d in range(R)]
    ys = [lax.rem(y + d, R) for d in range(R)]

    def dev(yy, xx, cc):
        return {"tp": (yy * R + xx) * CORES + cc}

    nbr = {(0, 1): dev(y, xs[1], c), (0, -1): dev(y, xs[R - 1], c),
           (1, 1): dev(ys[1], x, c), (1, -1): dev(ys[R - 1], x, c)}
    mate = dev(y, x, oc)

    def local(src, dst, i):
        cp = pltpu.make_async_copy(src, dst, lsem.at[i])
        cp.start()
        return cp

    cp_dy = local(dy_hbm, dyf.at[y, x, c], 0)
    cp_x = local(x_hbm, xf.at[y, x, c], 1)
    cp_ug = local(ug_hbm, ug, 2)
    cp_uu = local(uu_hbm, uu, 3)
    cp_wd = local(wd_hbm, wd, 4)
    cp_wg = local(wg_hbm, wg, 5)
    cp_wu = local(wu_hbm, wu, 6)

    barrier = pltpu.get_barrier_semaphore()
    for d in (*nbr.values(), mate):
        pl.semaphore_signal(barrier, inc=1, device_id=d, device_id_type=MESH)
    pl.semaphore_wait(barrier, 5)

    sent = []

    def send(src, dst, device):
        i = len(sent)
        cp = pltpu.make_async_remote_copy(src_ref=src, dst_ref=dst, send_sem=ssem.at[i], recv_sem=rsem.at[i],
                                          device_id=device, device_id_type=MESH)
        cp.start()
        sent.append(cp)
        return cp

    class Half:
        def __init__(self, buf, first):
            self.buf, self.first = buf, first
            base = first * H2
            self.all, self.lo, self.hi = pl.ds(base, H2), pl.ds(base, Q), pl.ds(base + Q, Q)
            self.near, self.far, self.rows = {}, {}, {}

        def ref(self, d1, d2, cols):
            if self.first == 0:
                return self.buf.at[ys[d2], xs[d1], c, :, cols]
            return self.buf.at[ys[d1], xs[d2], c, :, cols]

        def push(self, key, d1, d2, axis):
            ref = self.ref(d1, d2, self.all)
            self.near[key] = (send(ref, ref, nbr[axis, 1]), send(ref, ref, nbr[axis, -1]))

        def relay(self, key, minus, plus, axis):
            self.near[key][0].wait_recv()
            ref = self.ref(*minus, self.lo)
            a = send(ref, ref, nbr[axis, 1])
            self.near[key][1].wait_recv()
            ref = self.ref(*plus, self.hi)
            self.far[key] = (a, send(ref, ref, nbr[axis, -1]))

        def first_send(self):
            self.push("f", 0, 0, self.first)

        def first_relay(self):
            self.relay("f", (R - 1, 0), (1, 0), self.first)

        def first_far(self):
            for cp in self.far["f"]:
                cp.wait_recv()

        def second_send(self, d1):
            self.push(d1, d1, 0, 1 - self.first)

        def second_relay(self, d1):
            self.relay(d1, (d1, R - 1), (d1, 1), 1 - self.first)

        def second_far(self, d1):
            for cp in self.far[d1]:
                cp.wait_recv()

        def to_mate(self, d2):
            if self.first == 0:
                ref = self.buf.at[ys[d2], :, c, :, self.all]
            else:
                ref = self.buf.at[:, xs[d2], c, :, self.all]
            self.rows[d2] = send(ref, ref, mate)

        def mate_recv(self):
            for cp in self.rows.values():
                cp.wait_recv()

    class Gather:
        def __init__(self, buf):
            self.halves = (Half(buf, 0), Half(buf, 1))

        def __getattr__(self, name):
            def both(*args):
                for h in self.halves:
                    getattr(h, name)(*args)
            return both

    def prepare():
        g_f = ug[...].astype(F32)
        u_f = uu[...].astype(F32)
        z_t[...] = (g_f * jax.nn.sigmoid(g_f) * u_f).astype(BF16)
        gate[...] = g_f.T
        up[...] = u_f.T

    def grads():
        mid[...] = lax.dot_general(dyf[...].reshape(tokens, hidden), wd[...], NT, preferred_element_type=F32)
        step = tokens // 8
        for i in range(8):
            tok = pl.ds(i * step, step)
            g_mid, g_f, u_f = mid[tok, :], gate[tok, :], up[tok, :]
            s = jax.nn.sigmoid(g_f)
            dgs[tok, :] = (g_mid * u_f * s * (1.0 + g_f * (1.0 - s))).astype(BF16)
            dus[tok, :] = (g_mid * (g_f * s)).astype(BF16)

    kinds = ((0, 1, 0), (1, 1, H2), (0, -1, Q), (1, -1, H2 + Q))
    W = Q // GROUPS
    pair, leaf, raw, merged, leaf2, raw2, merged2 = {}, {}, {}, {}, {}, {}, {}

    def piece_cols(n, g):
        return pl.ds(kinds[n][2] + g * W, W)

    def partial(n):
        dg, du = dgs[...], dus[...]
        for t in range(Q // MXU_TILE):
            cols = pl.ds(kinds[n][2] + t * MXU_TILE, MXU_TILE)
            p = (jnp.dot(dg, wg[:, cols], preferred_element_type=F32)
                 + jnp.dot(du, wu[:, cols], preferred_element_type=F32))
            pb[:, :, :, :, cols] = p.astype(BF16).reshape(R, R, CORES, rows, MXU_TILE)
        for g in range(GROUPS):
            cols = piece_cols(n, g)
            pair[n, g] = send(pb.at[:, :, oc, :, cols], pr.at[:, :, :, cols], mate)

    def line(n, d, cols):
        if kinds[n][0] == 0:
            return sx.at[:, xs[d], :, cols]
        return sx.at[ys[d], :, :, cols]

    def spot(n, d):
        return (ys if kinds[n][0] == 0 else xs)[d]

    def scatter_first(n, g):
        axis, s, _ = kinds[n]
        cols = piece_cols(n, g)
        pair[n, g].wait_recv()
        for yy in range(R):
            sx[yy, :, :, cols] = pb[yy, :, c, :, cols].astype(F32) + pr[yy, :, :, cols].astype(F32)
        leaf[n, g] = send(line(n, 2, cols), lf.at[:, :, cols], nbr[axis, s])
        raw[n, g] = send(line(n, -s % R, cols), rw.at[:, :, cols], nbr[axis, -s])

    def scatter_merge(n, g):
        axis, s, _ = kinds[n]
        cols = piece_cols(n, g)
        leaf[n, g].wait_recv()
        mg[:, :, cols] = lf[:, :, cols] + line(n, s % R, cols)[...]
        merged[n, g] = send(mg.at[:, :, cols], rm.at[:, :, cols], nbr[axis, s])

    def scatter_second(n, g):
        axis, s, _ = kinds[n]
        cols = piece_cols(n, g)
        raw[n, g].wait_recv()
        merged[n, g].wait_recv()
        sy[:, :, cols] = line(n, 0, cols)[...] + rm[:, :, cols] + rw[:, :, cols]
        leaf2[n, g] = send(sy.at[spot(n, 2), :, cols], lf2.at[:, cols], nbr[1 - axis, s])
        raw2[n, g] = send(sy.at[spot(n, -s % R), :, cols], rw2.at[:, cols], nbr[1 - axis, -s])

    def scatter_merge2(n, g):
        axis, s, _ = kinds[n]
        cols = piece_cols(n, g)
        leaf2[n, g].wait_recv()
        mg2[:, cols] = lf2[:, cols] + sy[spot(n, s % R), :, cols]
        merged2[n, g] = send(mg2.at[:, cols], rm2.at[:, cols], nbr[1 - axis, s])

    def scatter_last(n, g):
        cols = piece_cols(n, g)
        raw2[n, g].wait_recv()
        merged2[n, g].wait_recv()
        dx_ref[:, cols] = (sy[spot(n, 0), :, cols] + rm2[:, cols] + rw2[:, cols]).astype(BF16)

    def pieces(f, g):
        for n in range(len(kinds)):
            f(n, g)

    def transposes():
        dg_t[...] = dgs[...].astype(F32).T.astype(BF16)
        du_t[...] = dus[...].astype(F32).T.astype(BF16)

    gd, gx = Gather(dyf), Gather(xf)
    cp_dy.wait()
    gd.first_send()
    gd.second_send(0)
    cp_x.wait()
    cp_ug.wait()
    cp_uu.wait()
    prepare()
    gd.first_relay()
    gd.second_send(R - 1)
    gd.second_send(1)
    gx.first_send()
    gd.second_relay(0)
    gd.first_far()
    gd.second_send(2)
    gd.to_mate(0)
    gd.second_relay(R - 1)
    gd.second_relay(1)
    gx.first_relay()
    gx.second_send(0)
    gd.second_relay(2)
    gd.to_mate(R - 1)
    gd.to_mate(1)
    gx.second_send(R - 1)
    gx.second_send(1)
    gx.first_far()
    gx.second_send(2)
    gx.to_mate(0)
    gd.second_far(0)
    gd.second_far(R - 1)
    gd.second_far(1)
    gd.second_far(2)
    gd.to_mate(2)
    gx.second_relay(0)
    cp_wd.wait()
    gd.mate_recv()
    grads()
    gx.second_relay(R - 1)
    gx.second_relay(1)
    cp_wg.wait()
    cp_wu.wait()
    partial(0)
    partial(1)
    scatter_first(0, 0)
    partial(2)
    scatter_first(1, 0)
    gx.second_relay(2)
    partial(3)
    scatter_first(2, 0)
    scatter_first(3, 0)
    gx.to_mate(R - 1)
    gx.to_mate(1)
    for g in range(1, GROUPS):
        pieces(scatter_first, g)
    pieces(scatter_merge, 0)
    transposes()
    gx.second_far(0)
    gx.second_far(R - 1)
    gx.second_far(1)
    gx.second_far(2)
    gx.to_mate(2)
    pieces(scatter_merge, 1)
    pieces(scatter_second, 0)
    pieces(scatter_second, 1)
    pieces(scatter_merge2, 0)
    pieces(scatter_merge2, 1)
    gx.mate_recv()
    pieces(scatter_last, 0)
    pieces(scatter_last, 1)
    for cp in sent:
        cp.wait_send()
    assert len(sent) == n_copies, len(sent)


def weight_kernel(xf, dyf, dg_t, du_t, z_t, dx, og, ou, od, odx):
    tile = og.shape[1]
    tokens = dg_t.shape[1]
    cols = pl.ds(pl.multiple_of(pl.program_id(0) * tile, tile), tile)
    xc = xf[:, :, :, :, cols].reshape(tokens, tile)
    og[...] = jnp.dot(dg_t[...], xc, preferred_element_type=F32)
    ou[...] = jnp.dot(du_t[...], xc, preferred_element_type=F32)
    od[...] = jnp.dot(z_t[...], dyf[:, :, :, :, cols].reshape(tokens, tile), preferred_element_type=F32)
    odx[...] = dx[:, cols]


def solution(mesh):
    tp = mesh.shape["tp"]
    ring = math.isqrt(tp // CORES)

    def local_backward(x_loc, wg_loc, wu_loc, wd_loc, ug_loc, uu_loc, dy_loc):
        rows, hidden = x_loc.shape
        ffn = wd_loc.shape[0]
        tokens = tp * rows
        R = ring
        n_copies = 2 * 2 * (4 + 4 * R + R) + 4 * GROUPS * 7
        full = (R, R, CORES, rows, hidden)
        vm = pltpu.VMEM
        out_bytes = 2 * (rows * hidden + 2 * tokens * hidden + 3 * ffn * tokens)
        dx, xf, dyf, dg_t, du_t, z_t = pl.pallas_call(
            lambda *refs: comm_kernel(R, n_copies, *refs),
            name="comm",
            out_shape=(vm((rows, hidden), BF16), vm(full, BF16), vm(full, BF16),
                       vm((ffn, tokens), BF16), vm((ffn, tokens), BF16), vm((ffn, tokens), BF16)),
            in_specs=[pl.BlockSpec(memory_space=pltpu.HBM)] * 7,
            out_specs=(pl.BlockSpec(memory_space=vm),) * 6,
            scratch_shapes=[
                vm((ffn, hidden), BF16), vm((ffn, hidden), BF16), vm((ffn, hidden), BF16),
                vm((ffn, tokens), BF16), vm((ffn, tokens), BF16),
                vm((tokens, ffn), F32), vm((tokens, ffn), F32), vm((tokens, ffn), F32),
                vm((tokens, ffn), BF16), vm((tokens, ffn), BF16),
                vm(full, BF16), vm((R, R, rows, hidden), BF16),
                vm((R, R, rows, hidden), F32), vm((R, rows, hidden), F32),
                *[vm((R, rows, hidden), F32)] * 4, *[vm((rows, hidden), F32)] * 4,
                pltpu.SemaphoreType.DMA((7,)),
                pltpu.SemaphoreType.DMA((n_copies,)),
                pltpu.SemaphoreType.DMA((n_copies,)),
            ],
            compiler_params=pltpu.CompilerParams(collective_id=0, has_side_effects=True,
                                                 vmem_limit_bytes=VMEM_BYTES - out_bytes - 40960),
        )(x_loc, dy_loc, wd_loc, wg_loc.T, wu_loc.T, ug_loc.T, uu_loc.T)
        out = jax.ShapeDtypeStruct((ffn, hidden), F32)
        ospec = pl.BlockSpec((ffn, COL_TILE), lambda j: (0, j))
        gw_g, gw_u, gw_d, dx = pl.pallas_call(
            weight_kernel,
            name="weight_grads",
            grid=(hidden // COL_TILE,),
            out_shape=(out, out, out, jax.ShapeDtypeStruct((rows, hidden), BF16)),
            in_specs=[pl.BlockSpec(memory_space=vm)] * 6,
            out_specs=(ospec, ospec, ospec, pl.BlockSpec((rows, COL_TILE), lambda j: (0, j))),
            compiler_params=pltpu.CompilerParams(vmem_limit_bytes=24 << 20),
        )(xf, dyf, dg_t, du_t, z_t, dx)
        return dx, gw_g.T, gw_u.T, gw_d

    row_spec = P(("dp", "tp"), None)
    col_spec = P(None, "tp")
    part_cols = P("dp", "tp")
    return jax.shard_map(local_backward, mesh=mesh,
                         in_specs=(row_spec, col_spec, col_spec, P("tp", None), part_cols, part_cols, row_spec),
                         out_specs=(row_spec, part_cols, part_cols, row_spec),
                         check_vma=False)
```

```python
import math

import jax
import jax.numpy as jnp
from jax import lax
from jax.experimental import pallas as pl
from jax.experimental.pallas import tpu as pltpu
from jax.sharding import PartitionSpec as P

MESH = pl.DeviceIdType.MESH
BF16 = jnp.bfloat16
F32 = jnp.float32
CORES = 2
COL_TILE = 1024
MXU_TILE = 256
GROUPS = (2, 2, 1)
VMEM_BYTES = 67043328
NT = (((1,), (1,)), ((), ()))


def comm_kernel(ring, n_copies, x_hbm, dy_hbm, wd_hbm, wg_hbm, wu_hbm, ug_hbm, uu_hbm,
                dx_ref, xf, dyf, dg_t, du_t, z_t,
                wd, wg, wu, ug, uu, gate, up, mid, dgs, dus, pb, pr, sx, sy,
                lf, mg, rw, rm, lf2, mg2, rw2, rm2, lsem, ssem, rsem):
    R = ring
    me = lax.axis_index("tp")
    c = lax.rem(me, CORES)
    x = lax.rem(me // CORES, R)
    y = me // (CORES * R)
    oc = 1 - c
    rows, hidden = x_hbm.shape
    tokens = R * R * CORES * rows
    H2, Q = hidden // 2, hidden // 4
    xs = [lax.rem(x + d, R) for d in range(R)]
    ys = [lax.rem(y + d, R) for d in range(R)]

    def dev(yy, xx, cc):
        return {"tp": (yy * R + xx) * CORES + cc}

    nbr = {(0, 1): dev(y, xs[1], c), (0, -1): dev(y, xs[R - 1], c),
           (1, 1): dev(ys[1], x, c), (1, -1): dev(ys[R - 1], x, c),
           (0, 2): dev(y, xs[2], c), (1, 2): dev(ys[2], x, c)}
    mate = dev(y, x, oc)

    def local(src, dst, i):
        cp = pltpu.make_async_copy(src, dst, lsem.at[i])
        cp.start()
        return cp

    cp_dy = local(dy_hbm, dyf.at[y, x, c], 0)
    cp_x = local(x_hbm, xf.at[y, x, c], 1)
    cp_ug = local(ug_hbm, ug, 2)
    cp_uu = local(uu_hbm, uu, 3)
    cp_wd = local(wd_hbm, wd, 4)
    cp_wg = local(wg_hbm, wg, 5)
    cp_wu = local(wu_hbm, wu, 6)

    barrier = pltpu.get_barrier_semaphore()
    for d in (*nbr.values(), mate):
        pl.semaphore_signal(barrier, inc=1, device_id=d, device_id_type=MESH)
    pl.semaphore_wait(barrier, len(nbr) + 1)

    sent = []

    def send(src, dst, device):
        i = len(sent)
        cp = pltpu.make_async_remote_copy(src_ref=src, dst_ref=dst, send_sem=ssem.at[i], recv_sem=rsem.at[i],
                                          device_id=device, device_id_type=MESH)
        cp.start()
        sent.append(cp)
        return cp

    class Half:
        def __init__(self, buf, first):
            self.buf, self.first = buf, first
            base = first * H2
            self.all, self.lo, self.hi = pl.ds(base, H2), pl.ds(base, Q), pl.ds(base + Q, Q)
            self.near, self.far, self.rows = {}, {}, {}

        def ref(self, d1, d2, cols):
            if self.first == 0:
                return self.buf.at[ys[d2], xs[d1], c, :, cols]
            return self.buf.at[ys[d1], xs[d2], c, :, cols]

        def push(self, key, d1, d2, axis):
            ref = self.ref(d1, d2, self.all)
            self.near[key] = (send(ref, ref, nbr[axis, 1]), send(ref, ref, nbr[axis, -1]))

        def relay(self, key, minus, plus, axis):
            self.near[key][0].wait_recv()
            ref = self.ref(*minus, self.lo)
            a = send(ref, ref, nbr[axis, 1])
            self.near[key][1].wait_recv()
            ref = self.ref(*plus, self.hi)
            self.far[key] = (a, send(ref, ref, nbr[axis, -1]))

        def first_send(self):
            self.push("f", 0, 0, self.first)

        def first_relay(self):
            self.relay("f", (R - 1, 0), (1, 0), self.first)

        def first_far(self):
            for cp in self.far["f"]:
                cp.wait_recv()

        def first_direct(self):
            self.push("f", 0, 0, self.first)
            ref = self.ref(0, 0, self.all)
            self.far["f"] = (send(ref, ref, nbr[self.first, 2]),)

        def first_near(self):
            for cp in self.near["f"]:
                cp.wait_recv()

        def second_send(self, d1):
            self.push(d1, d1, 0, 1 - self.first)

        def second_relay(self, d1):
            self.relay(d1, (d1, R - 1), (d1, 1), 1 - self.first)

        def second_far(self, d1):
            for cp in self.far[d1]:
                cp.wait_recv()

        def to_mate(self, d2):
            if self.first == 0:
                ref = self.buf.at[ys[d2], :, c, :, self.all]
            else:
                ref = self.buf.at[:, xs[d2], c, :, self.all]
            self.rows[d2] = send(ref, ref, mate)

        def spot_to_mate(self, d1, d2):
            ref = self.ref(d1, d2, self.all)
            self.rows[d1, d2] = send(ref, ref, mate)

        def mate_recv(self):
            for cp in self.rows.values():
                cp.wait_recv()

    class Gather:
        def __init__(self, buf):
            self.halves = (Half(buf, 0), Half(buf, 1))

        def __getattr__(self, name):
            def both(*args):
                for h in self.halves:
                    getattr(h, name)(*args)
            return both

    def prepare():
        g_f = ug[...].astype(F32)
        u_f = uu[...].astype(F32)
        z_t[...] = (g_f * jax.nn.sigmoid(g_f) * u_f).astype(BF16)
        gate[...] = g_f.T
        up[...] = u_f.T

    def grads():
        mid[...] = lax.dot_general(dyf[...].reshape(tokens, hidden), wd[...], NT, preferred_element_type=F32)
        step = tokens // 8
        for i in range(8):
            tok = pl.ds(i * step, step)
            g_mid, g_f, u_f = mid[tok, :], gate[tok, :], up[tok, :]
            s = jax.nn.sigmoid(g_f)
            dgs[tok, :] = (g_mid * u_f * s * (1.0 + g_f * (1.0 - s))).astype(BF16)
            dus[tok, :] = (g_mid * (g_f * s)).astype(BF16)

    kinds = ((0, 1, 0), (1, 1, H2), (0, -1, Q), (1, -1, H2 + Q))
    widths = [t * MXU_TILE for t in GROUPS]
    starts = [sum(widths[:g]) for g in range(len(widths))]
    pair, leaf, raw, merged, leaf2, raw2, merged2 = {}, {}, {}, {}, {}, {}, {}

    def piece_cols(n, g):
        return pl.ds(kinds[n][2] + starts[g], widths[g])

    def partial(n, g):
        dg, du = dgs[...], dus[...]
        for t in range(GROUPS[g]):
            cols = pl.ds(kinds[n][2] + starts[g] + t * MXU_TILE, MXU_TILE)
            p = (jnp.dot(dg, wg[:, cols], preferred_element_type=F32)
                 + jnp.dot(du, wu[:, cols], preferred_element_type=F32))
            pb[:, :, :, :, cols] = p.astype(BF16).reshape(R, R, CORES, rows, MXU_TILE)
        cols = piece_cols(n, g)
        pair[n, g] = send(pb.at[:, :, oc, :, cols], pr.at[:, :, :, cols], mate)

    def line(n, d, cols):
        if kinds[n][0] == 0:
            return sx.at[:, xs[d], :, cols]
        return sx.at[ys[d], :, :, cols]

    def spot(n, d):
        return (ys if kinds[n][0] == 0 else xs)[d]

    def scatter_first(n, g):
        axis, s, _ = kinds[n]
        cols = piece_cols(n, g)
        pair[n, g].wait_recv()
        for yy in range(R):
            sx[yy, :, :, cols] = pb[yy, :, c, :, cols].astype(F32) + pr[yy, :, :, cols].astype(F32)
        leaf[n, g] = send(line(n, 2, cols), lf.at[:, :, cols], nbr[axis, s])

    def scatter_raw(n, g):
        axis, s, _ = kinds[n]
        cols = piece_cols(n, g)
        raw[n, g] = send(line(n, -s % R, cols), rw.at[:, :, cols], nbr[axis, -s])

    def scatter_merge(n, g):
        axis, s, _ = kinds[n]
        cols = piece_cols(n, g)
        leaf[n, g].wait_recv()
        mg[:, :, cols] = lf[:, :, cols] + line(n, s % R, cols)[...]
        merged[n, g] = send(mg.at[:, :, cols], rm.at[:, :, cols], nbr[axis, s])

    def scatter_second(n, g):
        axis, s, _ = kinds[n]
        cols = piece_cols(n, g)
        raw[n, g].wait_recv()
        merged[n, g].wait_recv()
        sy[:, :, cols] = line(n, 0, cols)[...] + rm[:, :, cols] + rw[:, :, cols]
        leaf2[n, g] = send(sy.at[spot(n, 2), :, cols], lf2.at[:, cols], nbr[1 - axis, s])
        raw2[n, g] = send(sy.at[spot(n, -s % R), :, cols], rw2.at[:, cols], nbr[1 - axis, -s])

    def scatter_merge2(n, g):
        axis, s, _ = kinds[n]
        cols = piece_cols(n, g)
        leaf2[n, g].wait_recv()
        mg2[:, cols] = lf2[:, cols] + sy[spot(n, s % R), :, cols]
        merged2[n, g] = send(mg2.at[:, cols], rm2.at[:, cols], nbr[1 - axis, s])

    def scatter_last(n, g):
        cols = piece_cols(n, g)
        raw2[n, g].wait_recv()
        merged2[n, g].wait_recv()
        dx_ref[:, cols] = (sy[spot(n, 0), :, cols] + rm2[:, cols] + rw2[:, cols]).astype(BF16)

    def pieces(f, g):
        for n in range(len(kinds)):
            f(n, g)

    def transposes():
        dg_t[...] = dgs[...].astype(F32).T.astype(BF16)
        du_t[...] = dus[...].astype(F32).T.astype(BF16)

    gd, gx = Gather(dyf), Gather(xf)
    cp_dy.wait()
    gd.first_direct()
    gd.second_send(0)
    cp_x.wait()
    cp_ug.wait()
    cp_uu.wait()
    prepare()
    gd.first_near()
    gd.second_send(R - 1)
    gd.second_send(1)
    gd.first_far()
    gd.second_send(2)
    gd.second_relay(0)
    gd.to_mate(0)
    gx.first_send()
    gd.second_relay(R - 1)
    gd.second_relay(1)
    gx.second_send(0)
    gd.second_relay(2)
    gd.to_mate(R - 1)
    gd.to_mate(1)
    gd.second_far(0)
    gd.spot_to_mate(0, 2)
    gx.first_relay()
    gx.second_send(R - 1)
    gx.second_send(1)
    gd.second_far(R - 1)
    gd.spot_to_mate(R - 1, 2)
    gd.second_far(1)
    gd.spot_to_mate(1, 2)
    gd.second_far(2)
    gd.spot_to_mate(2, 2)
    gx.first_far()
    gx.second_send(2)
    gx.to_mate(0)
    gx.second_relay(0)
    cp_wd.wait()
    gd.mate_recv()
    grads()
    gx.second_relay(R - 1)
    gx.second_relay(1)
    cp_wg.wait()
    cp_wu.wait()
    partial(0, 0)
    partial(1, 0)
    partial(2, 0)
    partial(3, 0)
    scatter_first(0, 0)
    scatter_first(1, 0)
    gx.second_relay(2)
    partial(0, 1)
    scatter_first(2, 0)
    scatter_first(3, 0)
    pieces(scatter_raw, 0)
    partial(1, 1)
    partial(2, 1)
    partial(3, 1)
    gx.to_mate(R - 1)
    gx.to_mate(1)
    pieces(scatter_first, 1)
    partial(0, 2)
    partial(1, 2)
    partial(2, 2)
    partial(3, 2)
    pieces(scatter_merge, 0)
    pieces(scatter_raw, 1)
    pieces(scatter_first, 2)
    gx.second_far(0)
    gx.second_far(R - 1)
    gx.second_far(1)
    gx.second_far(2)
    gx.to_mate(2)
    pieces(scatter_merge, 1)
    pieces(scatter_raw, 2)
    transposes()
    pieces(scatter_second, 0)
    pieces(scatter_merge, 2)
    pieces(scatter_second, 1)
    pieces(scatter_merge2, 0)
    pieces(scatter_second, 2)
    pieces(scatter_merge2, 1)
    gx.mate_recv()
    pieces(scatter_last, 0)
    pieces(scatter_merge2, 2)
    pieces(scatter_last, 1)
    pieces(scatter_last, 2)
    for cp in sent:
        cp.wait_send()
    assert len(sent) == n_copies, len(sent)


def weight_kernel(xf, dyf, dg_t, du_t, z_t, dx, og, ou, od, odx):
    tile = og.shape[1]
    tokens = dg_t.shape[1]
    cols = pl.ds(pl.multiple_of(pl.program_id(0) * tile, tile), tile)
    xc = xf[:, :, :, :, cols].reshape(tokens, tile)
    og[...] = jnp.dot(dg_t[...], xc, preferred_element_type=F32)
    ou[...] = jnp.dot(du_t[...], xc, preferred_element_type=F32)
    od[...] = jnp.dot(z_t[...], dyf[:, :, :, :, cols].reshape(tokens, tile), preferred_element_type=F32)
    odx[...] = dx[:, cols]


def solution(mesh):
    tp = mesh.shape["tp"]
    ring = math.isqrt(tp // CORES)

    def local_backward(x_loc, wg_loc, wu_loc, wd_loc, ug_loc, uu_loc, dy_loc):
        rows, hidden = x_loc.shape
        ffn = wd_loc.shape[0]
        tokens = tp * rows
        R = ring
        n_copies = 2 * 2 * (4 + 4 * R + R) - 2 + 2 * (R - 1) + 4 * len(GROUPS) * 7
        full = (R, R, CORES, rows, hidden)
        vm = pltpu.VMEM
        out_bytes = 2 * (rows * hidden + 2 * tokens * hidden + 3 * ffn * tokens)
        dx, xf, dyf, dg_t, du_t, z_t = pl.pallas_call(
            lambda *refs: comm_kernel(R, n_copies, *refs),
            name="comm",
            out_shape=(vm((rows, hidden), BF16), vm(full, BF16), vm(full, BF16),
                       vm((ffn, tokens), BF16), vm((ffn, tokens), BF16), vm((ffn, tokens), BF16)),
            in_specs=[pl.BlockSpec(memory_space=pltpu.HBM)] * 7,
            out_specs=(pl.BlockSpec(memory_space=vm),) * 6,
            scratch_shapes=[
                vm((ffn, hidden), BF16), vm((ffn, hidden), BF16), vm((ffn, hidden), BF16),
                vm((ffn, tokens), BF16), vm((ffn, tokens), BF16),
                vm((tokens, ffn), F32), vm((tokens, ffn), F32), vm((tokens, ffn), F32),
                vm((tokens, ffn), BF16), vm((tokens, ffn), BF16),
                vm(full, BF16), vm((R, R, rows, hidden), BF16),
                vm((R, R, rows, hidden), F32), vm((R, rows, hidden), F32),
                *[vm((R, rows, hidden), F32)] * 4, *[vm((rows, hidden), F32)] * 4,
                pltpu.SemaphoreType.DMA((7,)),
                pltpu.SemaphoreType.DMA((n_copies,)),
                pltpu.SemaphoreType.DMA((n_copies,)),
            ],
            compiler_params=pltpu.CompilerParams(collective_id=0, has_side_effects=True,
                                                 vmem_limit_bytes=VMEM_BYTES - out_bytes - 40960),
        )(x_loc, dy_loc, wd_loc, wg_loc.T, wu_loc.T, ug_loc.T, uu_loc.T)
        out = jax.ShapeDtypeStruct((ffn, hidden), F32)
        ospec = pl.BlockSpec((ffn, COL_TILE), lambda j: (0, j))
        gw_g, gw_u, gw_d, dx = pl.pallas_call(
            weight_kernel,
            name="weight_grads",
            grid=(hidden // COL_TILE,),
            out_shape=(out, out, out, jax.ShapeDtypeStruct((rows, hidden), BF16)),
            in_specs=[pl.BlockSpec(memory_space=vm)] * 6,
            out_specs=(ospec, ospec, ospec, pl.BlockSpec((rows, COL_TILE), lambda j: (0, j))),
            compiler_params=pltpu.CompilerParams(vmem_limit_bytes=24 << 20),
        )(xf, dyf, dg_t, du_t, z_t, dx)
        return dx, gw_g.T, gw_u.T, gw_d

    row_spec = P(("dp", "tp"), None)
    col_spec = P(None, "tp")
    part_cols = P("dp", "tp")
    return jax.shard_map(local_backward, mesh=mesh,
                         in_specs=(row_spec, col_spec, col_spec, P("tp", None), part_cols, part_cols, row_spec),
                         out_specs=(row_spec, part_cols, part_cols, row_spec),
                         check_vma=False)
```

```python
import functools
import math

import jax
import jax.numpy as jnp
from jax import lax
from jax.experimental import pallas as pl
from jax.experimental.pallas import tpu as pltpu
from jax.sharding import PartitionSpec as P

MESH = pl.DeviceIdType.MESH
BF16 = jnp.bfloat16
F32 = jnp.float32
CORES = 2
COL_TILE = 512
SLOTS = 4
MXU_TILE = 256
MERGED = 1
GROUPS = (2, 2, 1)
VMEM_BYTES = 67043328
NT = (((1,), (1,)), ((), ()))


def comm_kernel(ring, n_copies, x_hbm, dy_hbm, wd_hbm, wg_hbm, wu_hbm, ug_hbm, uu_hbm,
                dx_ref, xf, dyf, dg_t, du_t, z_t,
                wd, wg, wu, ug, uu, gate, up, mid, dgs, dus, pb, pr, sx, sy,
                lf, mg, rw, rm, lf2, mg2, rw2, rm2, lsem, ssem, rsem):
    R = ring
    me = lax.axis_index("tp")
    c = lax.rem(me, CORES)
    x = lax.rem(me // CORES, R)
    y = me // (CORES * R)
    oc = 1 - c
    rows, hidden = x_hbm.shape
    tokens = R * R * CORES * rows
    H2, Q = hidden // 2, hidden // 4
    xs = [lax.rem(x + d, R) for d in range(R)]
    ys = [lax.rem(y + d, R) for d in range(R)]

    def dev(yy, xx, cc):
        return {"tp": (yy * R + xx) * CORES + cc}

    def at(axis, s, core):
        return dev(y, xs[s % R], core) if axis == 0 else dev(ys[s % R], x, core)

    steps = [(axis, s) for axis in (0, 1) for s in (1, -1, 2)]
    nbr = {step: at(*step, c) for step in steps}
    across = {step: at(*step, oc) for step in steps}
    to_core = [{step: at(*step, core) for step in steps} for core in range(CORES)]
    mate = dev(y, x, oc)

    def local(src, dst, i):
        cp = pltpu.make_async_copy(src, dst, lsem.at[i])
        cp.start()
        return cp

    cp_dy = local(dy_hbm, dyf.at[y, x, c], 0)
    cp_x = local(x_hbm, xf.at[y, x, c], 1)
    cp_ug = local(ug_hbm, ug, 2)
    cp_uu = local(uu_hbm, uu, 3)
    cp_wd = local(wd_hbm, wd, 4)
    cp_wg = local(wg_hbm, wg, 5)
    cp_wu = local(wu_hbm, wu, 6)

    barrier = pltpu.get_barrier_semaphore()
    for d in (*nbr.values(), *across.values(), mate):
        pl.semaphore_signal(barrier, inc=1, device_id=d, device_id_type=MESH)
    pl.semaphore_wait(barrier, 2 * len(nbr) + 1)

    sent = []

    class Copy:
        def __init__(self, make, device):
            self.make, self.device, self.i = make, device, len(sent)
            sent.append(self)
            self.describe().start()

        def describe(self):
            src, dst = self.make()
            return pltpu.make_async_remote_copy(src_ref=src, dst_ref=dst, send_sem=ssem.at[self.i],
                                                recv_sem=rsem.at[self.i], device_id=self.device,
                                                device_id_type=MESH)

        def wait_recv(self):
            self.describe().wait_recv()

        def wait_send(self):
            self.describe().wait_send()

    def send(src, dst, device):
        return Copy(lambda: (src, dst), device)

    def share(make, device):
        return Copy(lambda: (make(), make()), device)

    class Half:
        def __init__(self, buf, first, own):
            self.buf, self.first, self.own = buf, first, own
            base = first * H2
            self.all, self.lo, self.hi = pl.ds(base, H2), pl.ds(base, Q), pl.ds(base + Q, Q)
            self.near, self.far, self.rows = {}, {}, {}

        def ref(self, d1, d2, cols, cores=slice(None)):
            if self.first == 0:
                return self.buf.at[ys[d2], xs[d1], cores, :, cols]
            return self.buf.at[ys[d1], xs[d2], cores, :, cols]

        def push(self, key, d1, axis, core=None):
            cores = slice(None) if core is None else pl.ds(core, 1)
            ref = functools.partial(self.ref, d1, 0, self.all, cores)
            to = to_core[self.own]
            self.near.setdefault(key, []).append((share(ref, to[axis, 1]), share(ref, to[axis, -1])))
            return ref

        def relay(self, key, minus, plus, axis):
            for cp, _ in self.near[key]:
                cp.wait_recv()
            a = share(functools.partial(self.ref, *minus, self.lo), nbr[axis, 1])
            for _, cp in self.near[key]:
                cp.wait_recv()
            self.far[key] = [a, share(functools.partial(self.ref, *plus, self.hi), nbr[axis, -1])]

        def first_send(self, core):
            self.push("f", 0, self.first, core)

        def first_direct(self, core):
            ref = self.push("f", 0, self.first, core)
            self.far.setdefault("f", []).append(share(ref, to_core[self.own][self.first, 2]))

        def first_near(self):
            for pair in self.near["f"]:
                for cp in pair:
                    cp.wait_recv()

        def first_relay(self):
            self.relay("f", (R - 1, 0), (1, 0), self.first)

        def first_far(self):
            for cp in self.far["f"]:
                cp.wait_recv()

        def second_home(self, core):
            self.push(0, 0, 1 - self.first, core)

        def second_send(self, d1):
            self.push(d1, d1, 1 - self.first)

        def second_relay(self, d1):
            self.relay(d1, (d1, R - 1), (d1, 1), 1 - self.first)

        def second_far(self, d1):
            for cp in self.far[d1]:
                cp.wait_recv()

        def to_mate(self, d2):
            def ref():
                if self.first == 0:
                    return self.buf.at[ys[d2], :, :, :, self.all]
                return self.buf.at[:, xs[d2], :, :, self.all]

            self.rows[d2] = share(ref, mate)

        def spot_to_mate(self, d1, d2, cores=slice(None)):
            self.rows[d1, d2] = share(functools.partial(self.ref, d1, d2, self.all, cores), mate)

        def home_to_mate(self):
            self.spot_to_mate(0, 0, pl.ds(self.own, 1))
            for d1 in range(1, R):
                self.spot_to_mate(d1, 0)

        def mate_rows(self, row):
            for key, cp in self.rows.items():
                if key == row or (isinstance(key, tuple) and key[1] == row):
                    cp.wait_recv()

    class Gather:
        def __init__(self, buf, own):
            self.halves = (Half(buf, 0, own), Half(buf, 1, own))

        def __getattr__(self, name):
            def both(*args):
                for h in self.halves:
                    getattr(h, name)(*args)
            return both

    def prepare():
        g_f = ug[...].astype(F32)
        u_f = uu[...].astype(F32)
        z_t[...] = (g_f * jax.nn.sigmoid(g_f) * u_f).astype(BF16)
        gate[...] = g_f.T
        up[...] = u_f.T

    def grads():
        mid[...] = lax.dot_general(dyf[...].reshape(tokens, hidden), wd[...], NT, preferred_element_type=F32)
        step = tokens // 8
        for i in range(8):
            tok = pl.ds(i * step, step)
            g_mid, g_f, u_f = mid[tok, :], gate[tok, :], up[tok, :]
            s = jax.nn.sigmoid(g_f)
            dgs[tok, :] = (g_mid * u_f * s * (1.0 + g_f * (1.0 - s))).astype(BF16)
            dus[tok, :] = (g_mid * (g_f * s)).astype(BF16)

    kinds = ((0, 1, 0), (1, 1, H2), (0, -1, Q), (1, -1, H2 + Q))
    widths = [t * MXU_TILE for t in GROUPS]
    starts = [sum(widths[:g]) for g in range(len(widths))]
    pair, leaf, raw, merged, leaf2, raw2, merged2 = {}, {}, {}, {}, {}, {}, {}

    def piece_cols(n, g):
        return pl.ds(kinds[n][2] + starts[g], widths[g])

    def partial(n, g):
        dg, du = dgs[...], dus[...]
        for t in range(GROUPS[g]):
            cols = pl.ds(kinds[n][2] + starts[g] + t * MXU_TILE, MXU_TILE)
            p = (jnp.dot(dg, wg[:, cols], preferred_element_type=F32)
                 + jnp.dot(du, wu[:, cols], preferred_element_type=F32))
            pb[:, :, :, :, cols] = p.astype(BF16).reshape(R, R, CORES, rows, MXU_TILE)
        cols = piece_cols(n, g)
        pair[n, g] = send(pb.at[:, :, oc, :, cols], pr.at[:, :, :, cols], mate)

    def line(n, d, cols):
        if kinds[n][0] == 0:
            return sx.at[:, xs[d], :, cols]
        return sx.at[ys[d], :, :, cols]

    def spot(n, d):
        return (ys if kinds[n][0] == 0 else xs)[d]

    def scatter_first(n, g):
        axis, s, _ = kinds[n]
        cols = piece_cols(n, g)
        pair[n, g].wait_recv()
        for yy in range(R):
            sx[yy, :, :, cols] = pb[yy, :, c, :, cols].astype(F32) + pr[yy, :, :, cols].astype(F32)
        leaf[n, g] = send(line(n, 2, cols), lf.at[:, :, cols], nbr[axis, s])

    def scatter_raw(n, g):
        axis, s, _ = kinds[n]
        cols = piece_cols(n, g)
        raw[n, g] = send(line(n, -s % R, cols), rw.at[:, :, cols], nbr[axis, -s])

    def scatter_merge(n, g):
        axis, s, _ = kinds[n]
        cols = piece_cols(n, g)
        leaf[n, g].wait_recv()
        mg[:, :, cols] = lf[:, :, cols] + line(n, s % R, cols)[...]
        merged[n, g] = send(mg.at[:, :, cols], rm.at[:, :, cols], nbr[axis, s])

    def scatter_second(n, g):
        axis, s, _ = kinds[n]
        cols = piece_cols(n, g)
        raw[n, g].wait_recv()
        merged[n, g].wait_recv()
        sy[:, :, cols] = line(n, 0, cols)[...] + rm[:, :, cols] + rw[:, :, cols]
        direct = g >= MERGED
        leaf2[n, g] = send(sy.at[spot(n, 2), :, cols], lf2.at[:, cols], nbr[1 - axis, 2 if direct else s])
        if direct:
            merged2[n, g] = send(sy.at[spot(n, s % R), :, cols], rm2.at[:, cols], nbr[1 - axis, s])
        raw2[n, g] = send(sy.at[spot(n, -s % R), :, cols], rw2.at[:, cols], nbr[1 - axis, -s])

    def scatter_merge2(n, g):
        assert g < MERGED
        axis, s, _ = kinds[n]
        cols = piece_cols(n, g)
        leaf2[n, g].wait_recv()
        mg2[:, cols] = lf2[:, cols] + sy[spot(n, s % R), :, cols]
        merged2[n, g] = send(mg2.at[:, cols], rm2.at[:, cols], nbr[1 - axis, s])

    def scatter_last(n, g):
        cols = piece_cols(n, g)
        raw2[n, g].wait_recv()
        merged2[n, g].wait_recv()
        total = sy[spot(n, 0), :, cols] + rm2[:, cols] + rw2[:, cols]
        if g >= MERGED:
            leaf2[n, g].wait_recv()
            total = total + lf2[:, cols]
        dx_ref[:, cols] = total.astype(BF16)

    def pieces(f, g):
        for n in range(len(kinds)):
            f(n, g)

    def transposes():
        dg_t[...] = dgs[...].astype(F32).T.astype(BF16)
        du_t[...] = dus[...].astype(F32).T.astype(BF16)

    gd, gx = Gather(dyf, 1), Gather(xf, 0)
    only = ([], [])

    def on(core):
        def run(f):
            @pl.when(c == core)
            def _():
                n = len(sent)
                f()
                only[core].extend(sent[n:])
        return run

    cp_dy.wait()
    swap = []

    @on(0)
    def _():
        gd.first_direct(0)
        gd.second_home(0)
        swap.append(share(lambda: dyf.at[y, x, 0], mate))
        cp_x.wait()
        gx.first_send(0)
        cp_ug.wait()
        cp_uu.wait()
        prepare()

    @on(1)
    def _():
        gd.first_direct(1)
        gd.second_home(1)
        cp_x.wait()
        gx.first_send(1)
        swap.append(share(lambda: xf.at[y, x, 1], mate))
        cp_ug.wait()
        cp_uu.wait()
        prepare()
        gd.first_near()
        gd.second_send(R - 1)
        gd.second_send(1)
        gd.first_far()
        gd.second_send(2)
        gd.second_relay(0)
        swap[0].wait_recv()
        gd.home_to_mate()
        gd.second_relay(R - 1)
        gd.second_relay(1)
        gd.second_relay(2)
        gd.to_mate(R - 1)
        gd.to_mate(1)
        gx.second_home(1)
        gd.second_far(0)
        gd.spot_to_mate(0, 2)
        gd.second_far(R - 1)
        gd.spot_to_mate(R - 1, 2)
        gd.second_far(1)
        gd.spot_to_mate(1, 2)
        gd.second_far(2)
        gd.spot_to_mate(2, 2)
        cp_wd.wait()

    @on(0)
    def _():
        gx.first_relay()
        gd.mate_rows(0)
        gx.first_far()
        gd.mate_rows(R - 1)
        gd.mate_rows(1)
        gx.second_home(0)
        gx.second_send(R - 1)
        gx.second_send(1)
        gx.second_send(2)
        cp_wd.wait()
        gd.mate_rows(2)

    grads()

    @on(0)
    def _():
        gx.second_relay(0)

    cp_wg.wait()
    cp_wu.wait()
    partial(0, 0)
    partial(1, 0)
    partial(2, 0)

    @on(0)
    def _():
        gx.second_relay(R - 1)

    partial(3, 0)
    scatter_first(0, 0)
    scatter_first(1, 0)
    partial(0, 1)
    scatter_first(2, 0)
    scatter_first(3, 0)

    @on(0)
    def _():
        gx.second_relay(1)

    pieces(scatter_raw, 0)
    partial(1, 1)
    partial(2, 1)

    @on(0)
    def _():
        gx.second_relay(2)

    partial(3, 1)
    partial(0, 2)
    scatter_first(0, 1)
    scatter_first(1, 1)
    partial(1, 2)
    scatter_first(2, 1)
    scatter_first(3, 1)
    pieces(scatter_merge, 0)
    partial(2, 2)
    partial(3, 2)
    pieces(scatter_raw, 1)
    pieces(scatter_first, 2)

    @on(0)
    def _():
        swap[1].wait_recv()
        gx.home_to_mate()
        gx.to_mate(R - 1)
        gx.to_mate(1)

    pieces(scatter_merge, 1)
    pieces(scatter_raw, 2)
    transposes()
    pieces(scatter_second, 0)
    pieces(scatter_merge, 2)
    pieces(scatter_merge2, 0)
    pieces(scatter_second, 1)

    @on(0)
    def _():
        gx.second_far(0)
        gx.second_far(R - 1)
        gx.second_far(1)
        gx.second_far(2)
        gx.to_mate(2)

    pieces(scatter_second, 2)

    @on(1)
    def _():
        for d in range(R):
            gx.mate_rows(d)

    pieces(scatter_last, 0)
    pieces(scatter_last, 1)
    pieces(scatter_last, 2)
    common = [cp for cp in sent if not any(cp is other for other in only[0] + only[1])]
    for core in range(CORES):
        @on(core)
        def _():
            for cp in list(only[core]):
                cp.wait_send()

    for cp in common:
        cp.wait_send()
    assert len(sent) == n_copies, len(sent)


def weight_kernel(xf, dyf, dg_t, du_t, z_t, dx, og, ou, od, odx, buf, sem, dx_sem):
    slots, tile = buf.shape[1], buf.shape[3]
    tokens, hidden = dg_t.shape[1], og.shape[1]
    out = pltpu.make_async_copy(dx, odx, dx_sem)
    out.start()
    jobs = ((dg_t, xf, og), (du_t, xf, ou), (z_t, dyf, od))
    flight = {}
    for t in range(hidden // tile):
        cols = pl.ds(t * tile, tile)
        for i, (lhs, rhs, dst) in enumerate(jobs):
            slot = t % slots
            if (i, t - slots) in flight:
                flight[i, t - slots].wait()
            buf[i, slot] = jnp.dot(lhs[...], rhs[:, :, :, :, cols].reshape(tokens, tile), preferred_element_type=F32)
            flight[i, t] = pltpu.make_async_copy(buf.at[i, slot], dst.at[:, cols], sem.at[i, slot])
            flight[i, t].start()
    for t in range(hidden // tile - slots, hidden // tile):
        for i in range(len(jobs)):
            flight[i, t].wait()
    out.wait()


def solution(mesh):
    tp = mesh.shape["tp"]
    ring = math.isqrt(tp // CORES)

    def local_backward(x_loc, wg_loc, wu_loc, wd_loc, ug_loc, uu_loc, dy_loc):
        rows, hidden = x_loc.shape
        ffn = wd_loc.shape[0]
        tokens = tp * rows
        R = ring
        n_copies = 2 + 2 * (6 + 4 * R + 3 * R) + 2 * (8 + 4 * R + 2 * R - 1) + 4 * len(GROUPS) * 7
        full = (R, R, CORES, rows, hidden)
        vm = pltpu.VMEM
        out_bytes = 2 * (rows * hidden + 2 * tokens * hidden + 3 * ffn * tokens)
        dx, xf, dyf, dg_t, du_t, z_t = pl.pallas_call(
            lambda *refs: comm_kernel(R, n_copies, *refs),
            name="comm",
            out_shape=(vm((rows, hidden), BF16), vm(full, BF16), vm(full, BF16),
                       vm((ffn, tokens), BF16), vm((ffn, tokens), BF16), vm((ffn, tokens), BF16)),
            in_specs=[pl.BlockSpec(memory_space=pltpu.HBM)] * 7,
            out_specs=(pl.BlockSpec(memory_space=vm),) * 6,
            scratch_shapes=[
                vm((ffn, hidden), BF16), vm((ffn, hidden), BF16), vm((ffn, hidden), BF16),
                vm((ffn, tokens), BF16), vm((ffn, tokens), BF16),
                vm((tokens, ffn), F32), vm((tokens, ffn), F32), vm((tokens, ffn), F32),
                vm((tokens, ffn), BF16), vm((tokens, ffn), BF16),
                vm(full, BF16), vm((R, R, rows, hidden), BF16),
                vm((R, R, rows, hidden), F32), vm((R, rows, hidden), F32),
                *[vm((R, rows, hidden), F32)] * 4, *[vm((rows, hidden), F32)] * 4,
                pltpu.SemaphoreType.DMA((7,)),
                pltpu.SemaphoreType.DMA((n_copies,)),
                pltpu.SemaphoreType.DMA((n_copies,)),
            ],
            compiler_params=pltpu.CompilerParams(collective_id=0, has_side_effects=True,
                                                 vmem_limit_bytes=VMEM_BYTES - out_bytes - 40960),
        )(x_loc, dy_loc, wd_loc, wg_loc.T, wu_loc.T, ug_loc.T, uu_loc.T)
        out = jax.ShapeDtypeStruct((ffn, hidden), F32)
        hbm = pl.BlockSpec(memory_space=pltpu.HBM)
        gw_g, gw_u, gw_d, dx = pl.pallas_call(
            weight_kernel,
            name="weight_grads",
            out_shape=(out, out, out, jax.ShapeDtypeStruct((rows, hidden), BF16)),
            in_specs=[pl.BlockSpec(memory_space=vm)] * 6,
            out_specs=(hbm,) * 4,
            scratch_shapes=[vm((3, SLOTS, ffn, COL_TILE), F32), pltpu.SemaphoreType.DMA((3, SLOTS)),
                            pltpu.SemaphoreType.DMA],
            compiler_params=pltpu.CompilerParams(vmem_limit_bytes=24 << 20),
        )(xf, dyf, dg_t, du_t, z_t, dx)
        return dx, gw_g.T, gw_u.T, gw_d

    row_spec = P(("dp", "tp"), None)
    col_spec = P(None, "tp")
    part_cols = P("dp", "tp")
    return jax.shard_map(local_backward, mesh=mesh,
                         in_specs=(row_spec, col_spec, col_spec, P("tp", None), part_cols, part_cols, row_spec),
                         out_specs=(row_spec, part_cols, part_cols, row_spec),
                         check_vma=False)
```

```python
import functools
import math

import jax
import jax.numpy as jnp
from jax import lax
from jax.experimental import pallas as pl
from jax.experimental.pallas import tpu as pltpu
from jax.sharding import PartitionSpec as P

MESH = pl.DeviceIdType.MESH
BF16 = jnp.bfloat16
F32 = jnp.float32
CORES = 2
COL_TILE = 1024
SLOTS = 3
MXU_TILE = 256
MERGED = 0
GROUPS = (1, 2, 1, 1)
VMEM_BYTES = 67043328
NT = (((1,), (1,)), ((), ()))


def comm_kernel(ring, n_copies, x_hbm, dy_hbm, wd_hbm, wg_hbm, wu_hbm, ug_hbm, uu_hbm,
                dx_ref, xf, dyf, dg_t, du_t, z_t,
                wd, wg, wu, ug, uu, gate, up, mid, dgs, dus, pb, pr, sx, sy,
                lf, mg, rw, rm, lf2, mg2, rw2, rm2, lsem, ssem, rsem):
    R = ring
    me = lax.axis_index("tp")
    c = lax.rem(me, CORES)
    x = lax.rem(me // CORES, R)
    y = me // (CORES * R)
    oc = 1 - c
    rows, hidden = x_hbm.shape
    tokens = R * R * CORES * rows
    H2, Q = hidden // 2, hidden // 4
    xs = [lax.rem(x + d, R) for d in range(R)]
    ys = [lax.rem(y + d, R) for d in range(R)]

    def dev(yy, xx, cc):
        return {"tp": (yy * R + xx) * CORES + cc}

    def at(axis, s, core):
        return dev(y, xs[s % R], core) if axis == 0 else dev(ys[s % R], x, core)

    steps = [(axis, s) for axis in (0, 1) for s in (1, -1, 2)]
    nbr = {step: at(*step, c) for step in steps}
    across = {step: at(*step, oc) for step in steps}
    to_core = [{step: at(*step, core) for step in steps} for core in range(CORES)]
    mate = dev(y, x, oc)

    def local(src, dst, i):
        cp = pltpu.make_async_copy(src, dst, lsem.at[i])
        cp.start()
        return cp

    cp_dy = local(dy_hbm, dyf.at[y, x, c], 0)
    cp_x = local(x_hbm, xf.at[y, x, c], 1)
    cp_ug = local(ug_hbm, ug, 2)
    cp_uu = local(uu_hbm, uu, 3)
    cp_wd = local(wd_hbm, wd, 4)
    cp_wg = local(wg_hbm, wg, 5)
    cp_wu = local(wu_hbm, wu, 6)

    barrier = pltpu.get_barrier_semaphore()
    for d in (*nbr.values(), *across.values(), mate):
        pl.semaphore_signal(barrier, inc=1, device_id=d, device_id_type=MESH)
    pl.semaphore_wait(barrier, 2 * len(nbr) + 1)

    sent = []

    class Copy:
        def __init__(self, make, device):
            self.make, self.device, self.i = make, device, len(sent)
            sent.append(self)
            self.describe().start()

        def describe(self):
            src, dst = self.make()
            return pltpu.make_async_remote_copy(src_ref=src, dst_ref=dst, send_sem=ssem.at[self.i],
                                                recv_sem=rsem.at[self.i], device_id=self.device,
                                                device_id_type=MESH)

        def wait_recv(self):
            self.describe().wait_recv()

        def wait_send(self):
            self.describe().wait_send()

    def send(src, dst, device):
        return Copy(lambda: (src, dst), device)

    def share(make, device):
        return Copy(lambda: (make(), make()), device)

    class Half:
        def __init__(self, buf, first, own):
            self.buf, self.first, self.own = buf, first, own
            base = first * H2
            self.all, self.lo, self.hi = pl.ds(base, H2), pl.ds(base, Q), pl.ds(base + Q, Q)
            self.near, self.far, self.rows = {}, {}, {}

        def ref(self, d1, d2, cols, cores=slice(None)):
            if self.first == 0:
                return self.buf.at[ys[d2], xs[d1], cores, :, cols]
            return self.buf.at[ys[d1], xs[d2], cores, :, cols]

        def push(self, key, d1, axis, core=None):
            cores = slice(None) if core is None else pl.ds(core, 1)
            ref = functools.partial(self.ref, d1, 0, self.all, cores)
            to = to_core[self.own]
            self.near.setdefault(key, []).append((share(ref, to[axis, 1]), share(ref, to[axis, -1])))
            return ref

        def relay(self, key, minus, plus, axis):
            for cp, _ in self.near[key]:
                cp.wait_recv()
            a = share(functools.partial(self.ref, *minus, self.lo), nbr[axis, 1])
            for _, cp in self.near[key]:
                cp.wait_recv()
            self.far[key] = [a, share(functools.partial(self.ref, *plus, self.hi), nbr[axis, -1])]

        def first_send(self, core):
            self.push("f", 0, self.first, core)

        def first_direct(self, core):
            ref = self.push("f", 0, self.first, core)
            self.far.setdefault("f", []).append(share(ref, to_core[self.own][self.first, 2]))

        def first_near(self):
            for pair in self.near["f"]:
                for cp in pair:
                    cp.wait_recv()

        def first_relay(self):
            self.relay("f", (R - 1, 0), (1, 0), self.first)

        def first_far(self):
            for cp in self.far["f"]:
                cp.wait_recv()

        def second_home(self, core):
            self.push(0, 0, 1 - self.first, core)

        def second_send(self, d1):
            self.push(d1, d1, 1 - self.first)

        def second_relay(self, d1):
            self.relay(d1, (d1, R - 1), (d1, 1), 1 - self.first)

        def second_far(self, d1):
            for cp in self.far[d1]:
                cp.wait_recv()

        def to_mate(self, d2):
            def ref():
                if self.first == 0:
                    return self.buf.at[ys[d2], :, :, :, self.all]
                return self.buf.at[:, xs[d2], :, :, self.all]

            self.rows[d2] = share(ref, mate)

        def spot_to_mate(self, d1, d2, cores=slice(None)):
            self.rows[d1, d2] = share(functools.partial(self.ref, d1, d2, self.all, cores), mate)

        def home_to_mate(self):
            self.spot_to_mate(0, 0, pl.ds(self.own, 1))
            for d1 in range(1, R):
                self.spot_to_mate(d1, 0)

        def mate_rows(self, row):
            for key, cp in self.rows.items():
                if key == row or (isinstance(key, tuple) and key[1] == row):
                    cp.wait_recv()

    class Gather:
        def __init__(self, buf, own):
            self.halves = (Half(buf, 0, own), Half(buf, 1, own))

        def __getattr__(self, name):
            def both(*args):
                for h in self.halves:
                    getattr(h, name)(*args)
            return both

    def prepare():
        g_f = ug[...].astype(F32)
        u_f = uu[...].astype(F32)
        z_t[...] = (g_f * jax.nn.sigmoid(g_f) * u_f).astype(BF16)
        gate[...] = g_f.T
        up[...] = u_f.T

    def grads():
        mid[...] = lax.dot_general(dyf[...].reshape(tokens, hidden), wd[...], NT, preferred_element_type=F32)
        step = tokens // 8
        for i in range(8):
            tok = pl.ds(i * step, step)
            g_mid, g_f, u_f = mid[tok, :], gate[tok, :], up[tok, :]
            s = jax.nn.sigmoid(g_f)
            dgs[tok, :] = (g_mid * u_f * s * (1.0 + g_f * (1.0 - s))).astype(BF16)
            dus[tok, :] = (g_mid * (g_f * s)).astype(BF16)

    kinds = ((0, 1, 0), (1, 1, H2), (0, -1, Q), (1, -1, H2 + Q))
    widths = [t * MXU_TILE for t in GROUPS]
    starts = [sum(widths[:g]) for g in range(len(widths))]
    pair, leaf, raw, merged, leaf2, raw2, merged2 = {}, {}, {}, {}, {}, {}, {}

    def piece_cols(n, g):
        return pl.ds(kinds[n][2] + starts[g], widths[g])

    def partial(n, g):
        dg, du = dgs[...], dus[...]
        for t in range(GROUPS[g]):
            cols = pl.ds(kinds[n][2] + starts[g] + t * MXU_TILE, MXU_TILE)
            p = (jnp.dot(dg, wg[:, cols], preferred_element_type=F32)
                 + jnp.dot(du, wu[:, cols], preferred_element_type=F32))
            pb[:, :, :, :, cols] = p.astype(BF16).reshape(R, R, CORES, rows, MXU_TILE)
        cols = piece_cols(n, g)
        pair[n, g] = send(pb.at[:, :, oc, :, cols], pr.at[:, :, :, cols], mate)

    def line(n, d, cols):
        if kinds[n][0] == 0:
            return sx.at[:, xs[d], :, cols]
        return sx.at[ys[d], :, :, cols]

    def spot(n, d):
        return (ys if kinds[n][0] == 0 else xs)[d]

    def scatter_first(n, g):
        axis, s, _ = kinds[n]
        cols = piece_cols(n, g)
        pair[n, g].wait_recv()
        for yy in range(R):
            sx[yy, :, :, cols] = pb[yy, :, c, :, cols].astype(F32) + pr[yy, :, :, cols].astype(F32)
        leaf[n, g] = send(line(n, 2, cols), lf.at[:, :, cols], nbr[axis, s])

    def scatter_raw(n, g):
        axis, s, _ = kinds[n]
        cols = piece_cols(n, g)
        raw[n, g] = send(line(n, -s % R, cols), rw.at[:, :, cols], nbr[axis, -s])

    def scatter_merge(n, g):
        axis, s, _ = kinds[n]
        cols = piece_cols(n, g)
        leaf[n, g].wait_recv()
        mg[:, :, cols] = lf[:, :, cols] + line(n, s % R, cols)[...]
        merged[n, g] = send(mg.at[:, :, cols], rm.at[:, :, cols], nbr[axis, s])

    def scatter_second(n, g):
        axis, s, _ = kinds[n]
        cols = piece_cols(n, g)
        raw[n, g].wait_recv()
        merged[n, g].wait_recv()
        sy[:, :, cols] = line(n, 0, cols)[...] + rm[:, :, cols] + rw[:, :, cols]
        direct = g >= MERGED
        leaf2[n, g] = send(sy.at[spot(n, 2), :, cols], lf2.at[:, cols], nbr[1 - axis, 2 if direct else s])
        if direct:
            merged2[n, g] = send(sy.at[spot(n, s % R), :, cols], rm2.at[:, cols], nbr[1 - axis, s])
        raw2[n, g] = send(sy.at[spot(n, -s % R), :, cols], rw2.at[:, cols], nbr[1 - axis, -s])

    def scatter_merge2(n, g):
        assert g < MERGED
        axis, s, _ = kinds[n]
        cols = piece_cols(n, g)
        leaf2[n, g].wait_recv()
        mg2[:, cols] = lf2[:, cols] + sy[spot(n, s % R), :, cols]
        merged2[n, g] = send(mg2.at[:, cols], rm2.at[:, cols], nbr[1 - axis, s])

    def scatter_last(n, g):
        cols = piece_cols(n, g)
        raw2[n, g].wait_recv()
        merged2[n, g].wait_recv()
        total = sy[spot(n, 0), :, cols] + rm2[:, cols] + rw2[:, cols]
        if g >= MERGED:
            leaf2[n, g].wait_recv()
            total = total + lf2[:, cols]
        dx_ref[:, cols] = total.astype(BF16)

    def pieces(f, g):
        for n in range(len(kinds)):
            f(n, g)

    def transposes():
        dg_t[...] = dgs[...].astype(F32).T.astype(BF16)
        du_t[...] = dus[...].astype(F32).T.astype(BF16)

    gd, gx = Gather(dyf, 1), Gather(xf, 0)
    only = ([], [])

    def on(core):
        def run(f):
            @pl.when(c == core)
            def _():
                n = len(sent)
                f()
                only[core].extend(sent[n:])
        return run

    cp_dy.wait()
    swap = []

    @on(0)
    def _():
        gd.first_direct(0)
        gd.second_home(0)
        swap.append(share(lambda: dyf.at[y, x, 0], mate))
        cp_x.wait()
        gx.first_send(0)
        cp_ug.wait()
        cp_uu.wait()
        prepare()

    @on(1)
    def _():
        gd.first_direct(1)
        gd.second_home(1)
        cp_x.wait()
        gx.first_send(1)
        swap.append(share(lambda: xf.at[y, x, 1], mate))
        cp_ug.wait()
        cp_uu.wait()
        prepare()
        gd.first_near()
        gd.second_send(R - 1)
        gd.second_send(1)
        gd.first_far()
        gd.second_send(2)
        gd.second_relay(0)
        swap[0].wait_recv()
        gd.home_to_mate()
        gd.second_relay(R - 1)
        gd.second_relay(1)
        gd.second_relay(2)
        gd.to_mate(R - 1)
        gd.to_mate(1)
        gx.second_home(1)
        gd.second_far(0)
        gd.spot_to_mate(0, 2)
        gd.second_far(R - 1)
        gd.spot_to_mate(R - 1, 2)
        gd.second_far(1)
        gd.spot_to_mate(1, 2)
        gd.second_far(2)
        gd.spot_to_mate(2, 2)
        cp_wd.wait()

    @on(0)
    def _():
        gx.first_relay()
        gd.mate_rows(0)
        gx.first_far()
        gx.second_home(0)
        gx.second_send(R - 1)
        gx.second_send(1)
        gx.second_send(2)
        gd.mate_rows(R - 1)
        gd.mate_rows(1)
        gx.second_relay(0)
        cp_wd.wait()
        gd.mate_rows(2)

    grads()

    def x_relay(d1):
        @on(0)
        def _():
            gx.second_relay(d1)

    x_relay(R - 1)
    cp_wg.wait()
    cp_wu.wait()
    partial(0, 0)
    partial(1, 0)
    partial(2, 0)
    partial(3, 0)
    x_relay(1)
    partial(0, 1)
    scatter_first(0, 0)
    scatter_first(1, 0)
    partial(1, 1)
    scatter_first(2, 0)
    scatter_first(3, 0)
    pieces(scatter_raw, 0)
    x_relay(2)
    partial(2, 1)
    partial(3, 1)
    partial(0, 2)
    scatter_first(0, 1)
    scatter_first(1, 1)
    partial(1, 2)
    scatter_first(2, 1)
    scatter_first(3, 1)
    pieces(scatter_merge, 0)
    pieces(scatter_raw, 1)
    partial(2, 2)
    partial(3, 2)
    partial(0, 3)
    scatter_first(0, 2)
    scatter_first(1, 2)
    partial(1, 3)
    scatter_first(2, 2)
    scatter_first(3, 2)
    partial(2, 3)
    partial(3, 3)
    pieces(scatter_raw, 2)
    pieces(scatter_merge, 1)
    pieces(scatter_first, 3)

    @on(0)
    def _():
        swap[1].wait_recv()
        gx.home_to_mate()
        gx.to_mate(R - 1)
        gx.to_mate(1)

    pieces(scatter_raw, 3)
    pieces(scatter_merge, 2)
    transposes()
    pieces(scatter_second, 0)
    pieces(scatter_merge, 3)
    pieces(scatter_second, 1)

    @on(0)
    def _():
        gx.second_far(0)
        gx.second_far(R - 1)
        gx.second_far(1)
        gx.second_far(2)
        gx.to_mate(2)

    pieces(scatter_second, 2)
    pieces(scatter_second, 3)

    @on(1)
    def _():
        for d in range(R):
            gx.mate_rows(d)

    for g in range(len(GROUPS)):
        pieces(scatter_last, g)
    common = [cp for cp in sent if not any(cp is other for other in only[0] + only[1])]
    for core in range(CORES):
        @on(core)
        def _():
            for cp in list(only[core]):
                cp.wait_send()

    for cp in common:
        cp.wait_send()
    assert len(sent) == n_copies, len(sent)


def weight_kernel(xf, dyf, dg_t, du_t, z_t, dx, og, ou, od, odx, buf, sem, dx_sem):
    slots, tile = buf.shape[1], buf.shape[3]
    tokens, hidden = dg_t.shape[1], og.shape[1]
    out = pltpu.make_async_copy(dx, odx, dx_sem)
    out.start()
    jobs = ((dg_t, xf, og), (du_t, xf, ou), (z_t, dyf, od))
    flight = {}
    for t in range(hidden // tile):
        cols = pl.ds(t * tile, tile)
        for i, (lhs, rhs, dst) in enumerate(jobs):
            slot = t % slots
            if (i, t - slots) in flight:
                flight[i, t - slots].wait()
            buf[i, slot] = jnp.dot(lhs[...], rhs[:, :, :, :, cols].reshape(tokens, tile), preferred_element_type=F32)
            flight[i, t] = pltpu.make_async_copy(buf.at[i, slot], dst.at[:, cols], sem.at[i, slot])
            flight[i, t].start()
    for t in range(hidden // tile - slots, hidden // tile):
        for i in range(len(jobs)):
            flight[i, t].wait()
    out.wait()


def solution(mesh):
    tp = mesh.shape["tp"]
    ring = math.isqrt(tp // CORES)

    def local_backward(x_loc, wg_loc, wu_loc, wd_loc, ug_loc, uu_loc, dy_loc):
        rows, hidden = x_loc.shape
        ffn = wd_loc.shape[0]
        tokens = tp * rows
        R = ring
        n_copies = 2 + 2 * (6 + 4 * R + 3 * R) + 2 * (8 + 4 * R + 2 * R - 1) + 4 * len(GROUPS) * 7
        full = (R, R, CORES, rows, hidden)
        vm = pltpu.VMEM
        out_bytes = 2 * (rows * hidden + 2 * tokens * hidden + 3 * ffn * tokens)
        dx, xf, dyf, dg_t, du_t, z_t = pl.pallas_call(
            lambda *refs: comm_kernel(R, n_copies, *refs),
            name="comm",
            out_shape=(vm((rows, hidden), BF16), vm(full, BF16), vm(full, BF16),
                       vm((ffn, tokens), BF16), vm((ffn, tokens), BF16), vm((ffn, tokens), BF16)),
            in_specs=[pl.BlockSpec(memory_space=pltpu.HBM)] * 7,
            out_specs=(pl.BlockSpec(memory_space=vm),) * 6,
            scratch_shapes=[
                vm((ffn, hidden), BF16), vm((ffn, hidden), BF16), vm((ffn, hidden), BF16),
                vm((ffn, tokens), BF16), vm((ffn, tokens), BF16),
                vm((tokens, ffn), F32), vm((tokens, ffn), F32), vm((tokens, ffn), F32),
                vm((tokens, ffn), BF16), vm((tokens, ffn), BF16),
                vm(full, BF16), vm((R, R, rows, hidden), BF16),
                vm((R, R, rows, hidden), F32), vm((R, rows, hidden), F32),
                *[vm((R, rows, hidden), F32)] * 4, *[vm((rows, hidden), F32)] * 4,
                pltpu.SemaphoreType.DMA((7,)),
                pltpu.SemaphoreType.DMA((n_copies,)),
                pltpu.SemaphoreType.DMA((n_copies,)),
            ],
            compiler_params=pltpu.CompilerParams(collective_id=0, has_side_effects=True,
                                                 vmem_limit_bytes=VMEM_BYTES - out_bytes - 40960),
        )(x_loc, dy_loc, wd_loc, wg_loc.T, wu_loc.T, ug_loc.T, uu_loc.T)
        out = jax.ShapeDtypeStruct((ffn, hidden), F32)
        hbm = pl.BlockSpec(memory_space=pltpu.HBM)
        gw_g, gw_u, gw_d, dx = pl.pallas_call(
            weight_kernel,
            name="weight_grads",
            out_shape=(out, out, out, jax.ShapeDtypeStruct((rows, hidden), BF16)),
            in_specs=[pl.BlockSpec(memory_space=vm)] * 6,
            out_specs=(hbm,) * 4,
            scratch_shapes=[vm((3, SLOTS, ffn, COL_TILE), F32), pltpu.SemaphoreType.DMA((3, SLOTS)),
                            pltpu.SemaphoreType.DMA],
            compiler_params=pltpu.CompilerParams(vmem_limit_bytes=28 << 20),
        )(xf, dyf, dg_t, du_t, z_t, dx)
        return dx, gw_g.T, gw_u.T, gw_d

    row_spec = P(("dp", "tp"), None)
    col_spec = P(None, "tp")
    part_cols = P("dp", "tp")
    return jax.shard_map(local_backward, mesh=mesh,
                         in_specs=(row_spec, col_spec, col_spec, P("tp", None), part_cols, part_cols, row_spec),
                         out_specs=(row_spec, part_cols, part_cols, row_spec),
                         check_vma=False)
```

```python
import functools
import math

import jax
import jax.numpy as jnp
from jax import lax
from jax.experimental import pallas as pl
from jax.experimental.pallas import tpu as pltpu
from jax.sharding import PartitionSpec as P

MESH = pl.DeviceIdType.MESH
BF16 = jnp.bfloat16
F32 = jnp.float32
CORES = 2
COL_TILE = 512
SLOTS = 4
MXU_TILE = 256
GROUPS = (2, 2, 1)
VMEM_BYTES = 67043328
NT = (((1,), (1,)), ((), ()))


def comm_kernel(ring, n_copies, x_hbm, dy_hbm, wd_hbm, wg_hbm, wu_hbm, ug_hbm, uu_hbm,
                own_ref, a1, a2, a3, b1, b2, b3, xf, dyf, dg_t, du_t, z_t,
                wd, wg, wu, ug, uu, gate, up, mid, dgs, dus, pb, pr, sx,
                lf, mg, rw, rm, lsem, ssem, rsem):
    R = ring
    me = lax.axis_index("tp")
    c = lax.rem(me, CORES)
    x = lax.rem(me // CORES, R)
    y = me // (CORES * R)
    oc = 1 - c
    rows, hidden = x_hbm.shape
    tokens = R * R * CORES * rows
    H2, Q = hidden // 2, hidden // 4
    xs = [lax.rem(x + d, R) for d in range(R)]
    ys = [lax.rem(y + d, R) for d in range(R)]

    def dev(yy, xx, cc):
        return {"tp": (yy * R + xx) * CORES + cc}

    def at(axis, s, core):
        return dev(y, xs[s % R], core) if axis == 0 else dev(ys[s % R], x, core)

    steps = [(axis, s) for axis in (0, 1) for s in (1, -1, 2)]
    nbr = {step: at(*step, c) for step in steps}
    across = {step: at(*step, oc) for step in steps}
    to_core = [{step: at(*step, core) for step in steps} for core in range(CORES)]
    mate = dev(y, x, oc)

    def local(src, dst, i):
        cp = pltpu.make_async_copy(src, dst, lsem.at[i])
        cp.start()
        return cp

    cp_dy = local(dy_hbm, dyf.at[y, x, c], 0)
    cp_x = local(x_hbm, xf.at[y, x, c], 1)
    cp_ug = local(ug_hbm, ug, 2)
    cp_uu = local(uu_hbm, uu, 3)
    cp_wd = local(wd_hbm, wd, 4)
    cp_wg = local(wg_hbm, wg, 5)
    cp_wu = local(wu_hbm, wu, 6)

    barrier = pltpu.get_barrier_semaphore()
    for d in (*nbr.values(), *across.values(), mate):
        pl.semaphore_signal(barrier, inc=1, device_id=d, device_id_type=MESH)
    pl.semaphore_wait(barrier, 2 * len(nbr) + 1)

    sent = []

    class Copy:
        def __init__(self, make, device):
            self.make, self.device, self.i = make, device, len(sent)
            sent.append(self)
            self.describe().start()

        def describe(self):
            src, dst = self.make()
            return pltpu.make_async_remote_copy(src_ref=src, dst_ref=dst, send_sem=ssem.at[self.i],
                                                recv_sem=rsem.at[self.i], device_id=self.device,
                                                device_id_type=MESH)

        def wait_recv(self):
            self.describe().wait_recv()

        def wait_send(self):
            self.describe().wait_send()

    def send(src, dst, device):
        return Copy(lambda: (src, dst), device)

    def share(make, device):
        return Copy(lambda: (make(), make()), device)

    class Half:
        def __init__(self, buf, first, own):
            self.buf, self.first, self.own = buf, first, own
            base = first * H2
            self.all, self.lo, self.hi = pl.ds(base, H2), pl.ds(base, Q), pl.ds(base + Q, Q)
            self.near, self.far, self.rows = {}, {}, {}

        def ref(self, d1, d2, cols, cores=slice(None)):
            if self.first == 0:
                return self.buf.at[ys[d2], xs[d1], cores, :, cols]
            return self.buf.at[ys[d1], xs[d2], cores, :, cols]

        def push(self, key, d1, axis, core=None):
            cores = slice(None) if core is None else pl.ds(core, 1)
            ref = functools.partial(self.ref, d1, 0, self.all, cores)
            to = to_core[self.own]
            self.near.setdefault(key, []).append((share(ref, to[axis, 1]), share(ref, to[axis, -1])))
            return ref

        def relay(self, key, minus, plus, axis):
            for cp, _ in self.near[key]:
                cp.wait_recv()
            a = share(functools.partial(self.ref, *minus, self.lo), nbr[axis, 1])
            for _, cp in self.near[key]:
                cp.wait_recv()
            self.far[key] = [a, share(functools.partial(self.ref, *plus, self.hi), nbr[axis, -1])]

        def first_send(self, core):
            self.push("f", 0, self.first, core)

        def first_direct(self, core):
            ref = self.push("f", 0, self.first, core)
            self.far.setdefault("f", []).append(share(ref, to_core[self.own][self.first, 2]))

        def first_near(self):
            for pair in self.near["f"]:
                for cp in pair:
                    cp.wait_recv()

        def first_relay(self):
            self.relay("f", (R - 1, 0), (1, 0), self.first)

        def first_far(self):
            for cp in self.far["f"]:
                cp.wait_recv()

        def second_home(self, core):
            self.push(0, 0, 1 - self.first, core)

        def second_send(self, d1):
            self.push(d1, d1, 1 - self.first)

        def second_relay(self, d1):
            self.relay(d1, (d1, R - 1), (d1, 1), 1 - self.first)

        def second_far(self, d1):
            for cp in self.far[d1]:
                cp.wait_recv()

        def to_mate(self, d2):
            def ref():
                if self.first == 0:
                    return self.buf.at[ys[d2], :, :, :, self.all]
                return self.buf.at[:, xs[d2], :, :, self.all]

            self.rows[d2] = share(ref, mate)

        def spot_to_mate(self, d1, d2, cores=slice(None)):
            self.rows[d1, d2] = share(functools.partial(self.ref, d1, d2, self.all, cores), mate)

        def home_to_mate(self):
            self.spot_to_mate(0, 0, pl.ds(self.own, 1))
            for d1 in range(1, R):
                self.spot_to_mate(d1, 0)

        def mate_rows(self, row):
            for key, cp in self.rows.items():
                if key == row or (isinstance(key, tuple) and key[1] == row):
                    cp.wait_recv()

    class Gather:
        def __init__(self, buf, own):
            self.halves = (Half(buf, 0, own), Half(buf, 1, own))

        def __getattr__(self, name):
            def both(*args):
                for h in self.halves:
                    getattr(h, name)(*args)
            return both

    def prepare():
        g_f = ug[...].astype(F32)
        u_f = uu[...].astype(F32)
        z_t[...] = (g_f * jax.nn.sigmoid(g_f) * u_f).astype(BF16)
        gate[...] = g_f.T
        up[...] = u_f.T

    def grads():
        mid[...] = lax.dot_general(dyf[...].reshape(tokens, hidden), wd[...], NT, preferred_element_type=F32)
        step = tokens // 8
        for i in range(8):
            tok = pl.ds(i * step, step)
            g_mid, g_f, u_f = mid[tok, :], gate[tok, :], up[tok, :]
            s = jax.nn.sigmoid(g_f)
            dgs[tok, :] = (g_mid * u_f * s * (1.0 + g_f * (1.0 - s))).astype(BF16)
            dus[tok, :] = (g_mid * (g_f * s)).astype(BF16)

    kinds = ((0, 1, 0), (1, 1, H2), (0, -1, Q), (1, -1, H2 + Q))
    widths = [t * MXU_TILE for t in GROUPS]
    starts = [sum(widths[:g]) for g in range(len(widths))]
    pair, leaf, raw, merged = {}, {}, {}, {}

    def piece_cols(n, g):
        return pl.ds(kinds[n][2] + starts[g], widths[g])

    def partial(g, *ns):
        dg, du = dgs[...], dus[...]
        for n in ns:
            for t in range(GROUPS[g]):
                cols = pl.ds(kinds[n][2] + starts[g] + t * MXU_TILE, MXU_TILE)
                p = (jnp.dot(dg, wg[:, cols], preferred_element_type=F32)
                     + jnp.dot(du, wu[:, cols], preferred_element_type=F32))
                pb[:, :, :, :, cols] = p.astype(BF16).reshape(R, R, CORES, rows, MXU_TILE)
        for n in ns:
            cols = piece_cols(n, g)
            pair[n, g] = send(pb.at[:, :, oc, :, cols], pr.at[:, :, :, cols], mate)

    def line(n, d, cols):
        if kinds[n][0] == 0:
            return sx.at[:, xs[d], :, cols]
        return sx.at[ys[d], :, :, cols]

    def spot(n, d):
        return (ys if kinds[n][0] == 0 else xs)[d]

    def scatter_first(n, g):
        axis, s, _ = kinds[n]
        cols = piece_cols(n, g)
        pair[n, g].wait_recv()
        for yy in range(R):
            sx[yy, :, :, cols] = pb[yy, :, c, :, cols].astype(F32) + pr[yy, :, :, cols].astype(F32)
        leaf[n, g] = send(line(n, 2, cols), lf.at[:, :, cols], nbr[axis, s])

    def scatter_raw(n, g):
        axis, s, _ = kinds[n]
        cols = piece_cols(n, g)
        raw[n, g] = send(line(n, -s % R, cols), rw.at[:, :, cols], nbr[axis, -s])

    def scatter_merge(n, g):
        axis, s, _ = kinds[n]
        cols = piece_cols(n, g)
        leaf[n, g].wait_recv()
        mg[:, :, cols] = lf[:, :, cols] + line(n, s % R, cols)[...]
        merged[n, g] = send(mg.at[:, :, cols], rm.at[:, :, cols], nbr[axis, s])

    def scatter_second(n, g):
        cols = piece_cols(n, g)
        axis, _, base = kinds[n]
        raw[n, g].wait_recv()
        merged[n, g].wait_recv()
        inner = pl.ds(base - axis * H2 + starts[g], widths[g])
        for d, out in enumerate(((own_ref, a1, a2, a3), (own_ref, b1, b2, b3))[axis]):
            j = spot(n, d)
            mine = sx[j, x, :, cols] if axis == 0 else sx[y, j, :, cols]
            out[:, inner if d else cols] = mine + rm[j, :, cols] + rw[j, :, cols]

    def pieces(f, g):
        for n in range(len(kinds)):
            f(n, g)

    def transposes():
        dg_t[...] = dgs[...].astype(F32).T.astype(BF16)
        du_t[...] = dus[...].astype(F32).T.astype(BF16)

    gd, gx = Gather(dyf, 1), Gather(xf, 0)
    only = ([], [])

    def on(core):
        def run(f):
            @pl.when(c == core)
            def _():
                n = len(sent)
                f()
                only[core].extend(sent[n:])
        return run

    cp_dy.wait()
    swap = []

    @on(0)
    def _():
        gd.first_direct(0)
        gd.second_home(0)
        swap.append(share(lambda: dyf.at[y, x, 0], mate))
        cp_x.wait()
        gx.first_send(0)
        cp_ug.wait()
        cp_uu.wait()
        prepare()

    @on(1)
    def _():
        gd.first_direct(1)
        gd.second_home(1)
        cp_x.wait()
        gx.first_send(1)
        swap.append(share(lambda: xf.at[y, x, 1], mate))
        cp_ug.wait()
        cp_uu.wait()
        prepare()
        gd.first_near()
        gd.second_send(R - 1)
        gd.second_send(1)
        gd.first_far()
        gd.second_send(2)
        gd.second_relay(0)
        swap[0].wait_recv()
        gd.home_to_mate()
        gd.second_relay(R - 1)
        gd.second_relay(1)
        gd.second_relay(2)
        gd.to_mate(R - 1)
        gd.to_mate(1)
        gx.second_home(1)
        gd.second_far(0)
        gd.spot_to_mate(0, 2)
        gd.second_far(R - 1)
        gd.spot_to_mate(R - 1, 2)
        gd.second_far(1)
        gd.spot_to_mate(1, 2)
        gd.second_far(2)
        gd.spot_to_mate(2, 2)
        cp_wd.wait()

    @on(0)
    def _():
        gx.first_relay()
        gd.mate_rows(0)
        gx.first_far()
        gx.second_home(0)
        gx.second_send(R - 1)
        gx.second_send(1)
        gx.second_send(2)
        gd.mate_rows(R - 1)
        gd.mate_rows(1)
        gx.second_relay(0)
        cp_wd.wait()
        gd.mate_rows(2)

    grads()

    def x_relay(d1):
        @on(0)
        def _():
            gx.second_relay(d1)

    x_relay(R - 1)
    cp_wg.wait()
    cp_wu.wait()
    partial(0, 0)
    partial(0, 1)
    partial(0, 2)
    partial(0, 3)
    x_relay(1)
    scatter_first(0, 0)
    scatter_first(1, 0)
    partial(1, 0)
    scatter_first(2, 0)
    scatter_first(3, 0)
    pieces(scatter_raw, 0)
    partial(1, 1)
    x_relay(2)
    partial(1, 2)
    partial(1, 3)
    partial(2, 0, 1)
    scatter_first(0, 1)
    scatter_first(1, 1)
    partial(2, 2, 3)
    scatter_first(2, 1)
    scatter_first(3, 1)
    pieces(scatter_merge, 0)
    pieces(scatter_raw, 1)
    pieces(scatter_first, 2)

    @on(0)
    def _():
        swap[1].wait_recv()
        gx.home_to_mate()
        gx.to_mate(R - 1)
        gx.to_mate(1)

    pieces(scatter_merge, 1)
    pieces(scatter_raw, 2)
    transposes()
    pieces(scatter_second, 0)
    pieces(scatter_merge, 2)

    @on(0)
    def _():
        gx.second_far(0)
        gx.second_far(R - 1)
        gx.second_far(1)
        gx.second_far(2)
        gx.to_mate(2)

    pieces(scatter_second, 1)
    pieces(scatter_second, 2)

    @on(1)
    def _():
        for d in range(R):
            gx.mate_rows(d)

    common = [cp for cp in sent if not any(cp is other for other in only[0] + only[1])]
    for core in range(CORES):
        @on(core)
        def _():
            for cp in list(only[core]):
                cp.wait_send()

    for cp in common:
        cp.wait_send()
    assert len(sent) == n_copies, len(sent)


def weight_kernel(xf, dyf, dg_t, du_t, z_t, og, ou, od, buf, sem):
    slots, tile = buf.shape[1], buf.shape[3]
    tokens, hidden = dg_t.shape[1], og.shape[1]
    jobs = ((dg_t, xf, og), (du_t, xf, ou), (z_t, dyf, od))
    flight = {}
    for t in range(hidden // tile):
        cols = pl.ds(t * tile, tile)
        for i, (lhs, rhs, dst) in enumerate(jobs):
            slot = t % slots
            if (i, t - slots) in flight:
                flight[i, t - slots].wait()
            buf[i, slot] = jnp.dot(lhs[...], rhs[:, :, :, :, cols].reshape(tokens, tile), preferred_element_type=F32)
            flight[i, t] = pltpu.make_async_copy(buf.at[i, slot], dst.at[:, cols], sem.at[i, slot])
            flight[i, t].start()
    for t in range(hidden // tile - slots, hidden // tile):
        for i in range(len(jobs)):
            flight[i, t].wait()


def solution(mesh):
    tp = mesh.shape["tp"]
    ring = math.isqrt(tp // CORES)

    def local_backward(x_loc, wg_loc, wu_loc, wd_loc, ug_loc, uu_loc, dy_loc):
        rows, hidden = x_loc.shape
        ffn = wd_loc.shape[0]
        tokens = tp * rows
        R = ring
        n_copies = 2 + 2 * (6 + 4 * R + 3 * R) + 2 * (8 + 4 * R + 2 * R - 1) + 4 * len(GROUPS) * 4
        full = (R, R, CORES, rows, hidden)
        vm = pltpu.VMEM
        half = (rows, hidden // 2)
        out_bytes = 16 * rows * hidden + 2 * (2 * tokens * hidden + 3 * ffn * tokens)
        own, a1, a2, a3, b1, b2, b3, xf, dyf, dg_t, du_t, z_t = pl.pallas_call(
            lambda *refs: comm_kernel(R, n_copies, *refs),
            name="comm",
            out_shape=(vm((rows, hidden), F32), *[vm(half, F32)] * 6, vm(full, BF16), vm(full, BF16),
                       vm((ffn, tokens), BF16), vm((ffn, tokens), BF16), vm((ffn, tokens), BF16)),
            in_specs=[pl.BlockSpec(memory_space=pltpu.HBM)] * 7,
            out_specs=(pl.BlockSpec(memory_space=vm),) * 12,
            scratch_shapes=[
                vm((ffn, hidden), BF16), vm((ffn, hidden), BF16), vm((ffn, hidden), BF16),
                vm((ffn, tokens), BF16), vm((ffn, tokens), BF16),
                vm((tokens, ffn), F32), vm((tokens, ffn), F32), vm((tokens, ffn), F32),
                vm((tokens, ffn), BF16), vm((tokens, ffn), BF16),
                vm(full, BF16), vm((R, R, rows, hidden), BF16),
                vm((R, R, rows, hidden), F32), *[vm((R, rows, hidden), F32)] * 4,
                pltpu.SemaphoreType.DMA((7,)),
                pltpu.SemaphoreType.DMA((n_copies,)),
                pltpu.SemaphoreType.DMA((n_copies,)),
            ],
            compiler_params=pltpu.CompilerParams(collective_id=0, has_side_effects=True,
                                                 vmem_limit_bytes=VMEM_BYTES - out_bytes - 40960),
        )(x_loc, dy_loc, wd_loc, wg_loc.T, wu_loc.T, ug_loc.T, uu_loc.T)
        def shift(v, dy, dx):
            pairs = []
            for i in range(tp):
                core, col, row = i % CORES, i // CORES % R, i // (CORES * R)
                pairs.append((i, ((row + dy) % R * R + (col + dx) % R) * CORES + core))
            return lax.ppermute(v, "tp", pairs)

        got_a = [shift(v, d + 1, 0) for d, v in enumerate((a1, a2, a3))]
        got_b = [shift(v, 0, d + 1) for d, v in enumerate((b1, b2, b3))]
        out = jax.ShapeDtypeStruct((ffn, hidden), F32)
        hbm = pl.BlockSpec(memory_space=pltpu.HBM)
        gw_g, gw_u, gw_d = pl.pallas_call(
            weight_kernel,
            name="weight_grads",
            out_shape=(out, out, out),
            in_specs=[pl.BlockSpec(memory_space=vm)] * 5,
            out_specs=(hbm,) * 3,
            scratch_shapes=[vm((3, SLOTS, ffn, COL_TILE), F32), pltpu.SemaphoreType.DMA((3, SLOTS))],
            compiler_params=pltpu.CompilerParams(vmem_limit_bytes=28 << 20),
            cost_estimate=pl.CostEstimate(flops=6 * ffn * tokens * hidden, bytes_accessed=12 * ffn * hidden,
                                          transcendentals=0),
        )(xf, dyf, dg_t, du_t, z_t)
        both = [jnp.concatenate(v, axis=1) for v in zip(got_a, got_b)]
        dx = (own + both[0] + both[1] + both[2]).astype(BF16)
        return dx, gw_g.T, gw_u.T, gw_d

    row_spec = P(("dp", "tp"), None)
    col_spec = P(None, "tp")
    part_cols = P("dp", "tp")
    return jax.shard_map(local_backward, mesh=mesh,
                         in_specs=(row_spec, col_spec, col_spec, P("tp", None), part_cols, part_cols, row_spec),
                         out_specs=(row_spec, part_cols, part_cols, row_spec),
                         check_vma=False)
```

```python
import functools
import math

import jax
import jax.numpy as jnp
from jax import lax
from jax.experimental import pallas as pl
from jax.experimental.pallas import tpu as pltpu
from jax.sharding import PartitionSpec as P

MESH = pl.DeviceIdType.MESH
BF16 = jnp.bfloat16
F32 = jnp.float32
CORES = 2
COL_TILE = 256
SLOTS = 8
MXU_TILE = 256
MERGED = 1
GROUPS = (2, 2, 1)
VMEM_BYTES = 67043328
NT = (((1,), (1,)), ((), ()))


def comm_kernel(ring, n_copies, x_hbm, dy_hbm, wd_hbm, wg_hbm, wu_hbm, ug_hbm, uu_hbm,
                dx_ref, xf, dyf, dg_t, du_t, z_t,
                wd, wg, wu, ug, uu, gate, up, mid, dgs, dus, pb, pr, sx, sy,
                lf, mg, rw, rm, lf2, mg2, rw2, rm2, lsem, ssem, rsem):
    R = ring
    me = lax.axis_index("tp")
    c = lax.rem(me, CORES)
    x = lax.rem(me // CORES, R)
    y = me // (CORES * R)
    oc = 1 - c
    rows, hidden = x_hbm.shape
    tokens = R * R * CORES * rows
    H2, Q = hidden // 2, hidden // 4
    xs = [lax.rem(x + d, R) for d in range(R)]
    ys = [lax.rem(y + d, R) for d in range(R)]

    def dev(yy, xx, cc):
        return {"tp": (yy * R + xx) * CORES + cc}

    def at(axis, s, core):
        return dev(y, xs[s % R], core) if axis == 0 else dev(ys[s % R], x, core)

    steps = [(axis, s) for axis in (0, 1) for s in (1, -1, 2)]
    nbr = {step: at(*step, c) for step in steps}
    across = {step: at(*step, oc) for step in steps}
    to_core = [{step: at(*step, core) for step in steps} for core in range(CORES)]
    mate = dev(y, x, oc)

    def local(src, dst, i):
        cp = pltpu.make_async_copy(src, dst, lsem.at[i])
        cp.start()
        return cp

    cp_dy = local(dy_hbm, dyf.at[y, x, c], 0)
    cp_x = local(x_hbm, xf.at[y, x, c], 1)
    cp_ug = local(ug_hbm, ug, 2)
    cp_uu = local(uu_hbm, uu, 3)
    cp_wd = local(wd_hbm, wd, 4)
    cp_wg = local(wg_hbm, wg, 5)
    cp_wu = local(wu_hbm, wu, 6)

    barrier = pltpu.get_barrier_semaphore()
    for d in (*nbr.values(), *across.values(), mate):
        pl.semaphore_signal(barrier, inc=1, device_id=d, device_id_type=MESH)
    pl.semaphore_wait(barrier, 2 * len(nbr) + 1)

    sent = []

    class Copy:
        def __init__(self, make, device):
            self.make, self.device, self.i = make, device, len(sent)
            sent.append(self)
            self.describe().start()

        def describe(self):
            src, dst = self.make()
            return pltpu.make_async_remote_copy(src_ref=src, dst_ref=dst, send_sem=ssem.at[self.i],
                                                recv_sem=rsem.at[self.i], device_id=self.device,
                                                device_id_type=MESH)

        def wait_recv(self):
            self.describe().wait_recv()

        def wait_send(self):
            self.describe().wait_send()

    def send(src, dst, device):
        return Copy(lambda: (src, dst), device)

    def share(make, device):
        return Copy(lambda: (make(), make()), device)

    class Half:
        def __init__(self, buf, first, own):
            self.buf, self.first, self.own = buf, first, own
            base = first * H2
            self.all, self.lo, self.hi = pl.ds(base, H2), pl.ds(base, Q), pl.ds(base + Q, Q)
            self.near, self.far, self.rows = {}, {}, {}

        def ref(self, d1, d2, cols, cores=slice(None)):
            if self.first == 0:
                return self.buf.at[ys[d2], xs[d1], cores, :, cols]
            return self.buf.at[ys[d1], xs[d2], cores, :, cols]

        def push(self, key, d1, axis, core=None):
            cores = slice(None) if core is None else pl.ds(core, 1)
            ref = functools.partial(self.ref, d1, 0, self.all, cores)
            to = to_core[self.own]
            self.near.setdefault(key, []).append((share(ref, to[axis, 1]), share(ref, to[axis, -1])))
            return ref

        def relay(self, key, minus, plus, axis):
            for cp, _ in self.near[key]:
                cp.wait_recv()
            a = share(functools.partial(self.ref, *minus, self.lo), nbr[axis, 1])
            for _, cp in self.near[key]:
                cp.wait_recv()
            self.far[key] = [a, share(functools.partial(self.ref, *plus, self.hi), nbr[axis, -1])]

        def first_send(self, core):
            self.push("f", 0, self.first, core)

        def first_direct(self, core):
            ref = self.push("f", 0, self.first, core)
            self.far.setdefault("f", []).append(share(ref, to_core[self.own][self.first, 2]))

        def first_near(self):
            for pair in self.near["f"]:
                for cp in pair:
                    cp.wait_recv()

        def first_relay(self):
            self.relay("f", (R - 1, 0), (1, 0), self.first)

        def first_far(self):
            for cp in self.far["f"]:
                cp.wait_recv()

        def second_home(self, core):
            self.push(0, 0, 1 - self.first, core)

        def second_send(self, d1):
            self.push(d1, d1, 1 - self.first)

        def second_relay(self, d1):
            self.relay(d1, (d1, R - 1), (d1, 1), 1 - self.first)

        def second_far(self, d1):
            for cp in self.far[d1]:
                cp.wait_recv()

        def to_mate(self, d2):
            def ref():
                if self.first == 0:
                    return self.buf.at[ys[d2], :, :, :, self.all]
                return self.buf.at[:, xs[d2], :, :, self.all]

            self.rows[d2] = share(ref, mate)

        def spot_to_mate(self, d1, d2, cores=slice(None)):
            self.rows[d1, d2] = share(functools.partial(self.ref, d1, d2, self.all, cores), mate)

        def home_to_mate(self):
            self.spot_to_mate(0, 0, pl.ds(self.own, 1))
            for d1 in range(1, R):
                self.spot_to_mate(d1, 0)

        def mate_rows(self, row):
            for key, cp in self.rows.items():
                if key == row or (isinstance(key, tuple) and key[1] == row):
                    cp.wait_recv()

    class Gather:
        def __init__(self, buf, own):
            self.halves = (Half(buf, 0, own), Half(buf, 1, own))

        def __getattr__(self, name):
            def both(*args):
                for h in self.halves:
                    getattr(h, name)(*args)
            return both

    def prepare():
        g_f = ug[...].astype(F32)
        u_f = uu[...].astype(F32)
        z_t[...] = (g_f * jax.nn.sigmoid(g_f) * u_f).astype(BF16)
        gate[...] = g_f.T
        up[...] = u_f.T

    def grads():
        mid[...] = lax.dot_general(dyf[...].reshape(tokens, hidden), wd[...], NT, preferred_element_type=F32)
        step = tokens // 8
        for i in range(8):
            tok = pl.ds(i * step, step)
            g_mid, g_f, u_f = mid[tok, :], gate[tok, :], up[tok, :]
            s = jax.nn.sigmoid(g_f)
            dgs[tok, :] = (g_mid * u_f * s * (1.0 + g_f * (1.0 - s))).astype(BF16)
            dus[tok, :] = (g_mid * (g_f * s)).astype(BF16)

    kinds = ((0, 1, 0), (1, 1, H2), (0, -1, Q), (1, -1, H2 + Q))
    widths = [t * MXU_TILE for t in GROUPS]
    starts = [sum(widths[:g]) for g in range(len(widths))]
    pair, leaf, raw, merged, leaf2, raw2, merged2 = {}, {}, {}, {}, {}, {}, {}

    def piece_cols(n, g):
        return pl.ds(kinds[n][2] + starts[g], widths[g])

    def partial(g, *ns):
        dg, du = dgs[...], dus[...]
        for n in ns:
            for t in range(GROUPS[g]):
                cols = pl.ds(kinds[n][2] + starts[g] + t * MXU_TILE, MXU_TILE)
                p = (jnp.dot(dg, wg[:, cols], preferred_element_type=F32)
                     + jnp.dot(du, wu[:, cols], preferred_element_type=F32))
                pb[:, :, :, :, cols] = p.astype(BF16).reshape(R, R, CORES, rows, MXU_TILE)
        for n in ns:
            cols = piece_cols(n, g)
            pair[n, g] = send(pb.at[:, :, oc, :, cols], pr.at[:, :, :, cols], mate)

    def line(n, d, cols):
        if kinds[n][0] == 0:
            return sx.at[:, xs[d], :, cols]
        return sx.at[ys[d], :, :, cols]

    def spot(n, d):
        return (ys if kinds[n][0] == 0 else xs)[d]

    def scatter_first(n, g):
        axis, s, _ = kinds[n]
        cols = piece_cols(n, g)
        pair[n, g].wait_recv()
        for yy in range(R):
            sx[yy, :, :, cols] = pb[yy, :, c, :, cols].astype(F32) + pr[yy, :, :, cols].astype(F32)
        leaf[n, g] = send(line(n, 2, cols), lf.at[:, :, cols], nbr[axis, s])

    def scatter_raw(n, g):
        axis, s, _ = kinds[n]
        cols = piece_cols(n, g)
        raw[n, g] = send(line(n, -s % R, cols), rw.at[:, :, cols], nbr[axis, -s])

    def scatter_merge(n, g):
        axis, s, _ = kinds[n]
        cols = piece_cols(n, g)
        leaf[n, g].wait_recv()
        mg[:, :, cols] = lf[:, :, cols] + line(n, s % R, cols)[...]
        merged[n, g] = send(mg.at[:, :, cols], rm.at[:, :, cols], nbr[axis, s])

    def scatter_second(n, g):
        axis, s, _ = kinds[n]
        cols = piece_cols(n, g)
        raw[n, g].wait_recv()
        merged[n, g].wait_recv()
        sy[:, :, cols] = line(n, 0, cols)[...] + rm[:, :, cols] + rw[:, :, cols]
        direct = g >= MERGED
        leaf2[n, g] = send(sy.at[spot(n, 2), :, cols], lf2.at[:, cols], nbr[1 - axis, 2 if direct else s])
        if direct:
            merged2[n, g] = send(sy.at[spot(n, s % R), :, cols], rm2.at[:, cols], nbr[1 - axis, s])
        raw2[n, g] = send(sy.at[spot(n, -s % R), :, cols], rw2.at[:, cols], nbr[1 - axis, -s])

    def scatter_merge2(n, g):
        assert g < MERGED
        axis, s, _ = kinds[n]
        cols = piece_cols(n, g)
        leaf2[n, g].wait_recv()
        mg2[:, cols] = lf2[:, cols] + sy[spot(n, s % R), :, cols]
        merged2[n, g] = send(mg2.at[:, cols], rm2.at[:, cols], nbr[1 - axis, s])

    def scatter_last(n, g):
        cols = piece_cols(n, g)
        raw2[n, g].wait_recv()
        merged2[n, g].wait_recv()
        total = sy[spot(n, 0), :, cols] + rm2[:, cols] + rw2[:, cols]
        if g >= MERGED:
            leaf2[n, g].wait_recv()
            total = total + lf2[:, cols]
        dx_ref[:, cols] = total.astype(BF16)

    def pieces(f, g):
        for n in range(len(kinds)):
            f(n, g)

    def transposes():
        dg_t[...] = dgs[...].astype(F32).T.astype(BF16)
        du_t[...] = dus[...].astype(F32).T.astype(BF16)

    gd, gx = Gather(dyf, 1), Gather(xf, 0)
    only = ([], [])

    def on(core):
        def run(f):
            @pl.when(c == core)
            def _():
                n = len(sent)
                f()
                only[core].extend(sent[n:])
        return run

    cp_dy.wait()
    swap = []

    @on(0)
    def _():
        gd.first_direct(0)
        gd.second_home(0)
        swap.append(share(lambda: dyf.at[y, x, 0], mate))
        cp_x.wait()
        gx.first_send(0)
        cp_ug.wait()
        cp_uu.wait()
        prepare()

    @on(1)
    def _():
        gd.first_direct(1)
        gd.second_home(1)
        cp_x.wait()
        gx.first_send(1)
        swap.append(share(lambda: xf.at[y, x, 1], mate))
        cp_ug.wait()
        cp_uu.wait()
        prepare()
        gd.first_near()
        gd.second_send(R - 1)
        gd.second_send(1)
        gd.first_far()
        gd.second_send(2)
        gd.second_relay(0)
        swap[0].wait_recv()
        gd.home_to_mate()
        gd.second_relay(R - 1)
        gd.second_relay(1)
        gd.second_relay(2)
        gd.to_mate(R - 1)
        gd.to_mate(1)
        gx.second_home(1)
        gd.second_far(0)
        gd.spot_to_mate(0, 2)
        gd.second_far(R - 1)
        gd.spot_to_mate(R - 1, 2)
        gd.second_far(1)
        gd.spot_to_mate(1, 2)
        gd.second_far(2)
        gd.spot_to_mate(2, 2)
        cp_wd.wait()

    @on(0)
    def _():
        gx.first_relay()
        gd.mate_rows(0)
        gx.first_far()
        gx.second_home(0)
        gx.second_send(R - 1)
        gx.second_send(1)
        gx.second_send(2)
        gd.mate_rows(R - 1)
        gd.mate_rows(1)
        gx.second_relay(0)
        cp_wd.wait()
        gd.mate_rows(2)

    grads()

    def x_relay(d1):
        @on(0)
        def _():
            gx.second_relay(d1)

    cp_wg.wait()
    cp_wu.wait()
    partial(0, 0)
    partial(0, 1)
    partial(0, 2)
    partial(0, 3)
    scatter_first(0, 0)
    scatter_first(1, 0)
    x_relay(R - 1)
    partial(1, 0)
    scatter_first(2, 0)
    scatter_first(3, 0)
    x_relay(1)
    pieces(scatter_raw, 0)
    partial(1, 1)
    x_relay(2)
    partial(1, 2)
    partial(1, 3)
    partial(2, 0, 1)
    scatter_first(0, 1)
    scatter_first(1, 1)
    partial(2, 2, 3)
    scatter_first(2, 1)
    scatter_first(3, 1)
    pieces(scatter_merge, 0)
    pieces(scatter_raw, 1)
    pieces(scatter_first, 2)

    @on(0)
    def _():
        swap[1].wait_recv()
        gx.home_to_mate()
        gx.to_mate(R - 1)
        gx.to_mate(1)

    pieces(scatter_merge, 1)
    pieces(scatter_raw, 2)
    transposes()
    pieces(scatter_second, 0)
    pieces(scatter_merge, 2)
    pieces(scatter_second, 1)
    pieces(scatter_merge2, 0)

    @on(0)
    def _():
        gx.second_far(0)
        gx.second_far(R - 1)
        gx.second_far(1)
        gx.second_far(2)
        gx.to_mate(2)

    pieces(scatter_second, 2)

    @on(1)
    def _():
        for d in range(R):
            gx.mate_rows(d)

    pieces(scatter_last, 0)
    pieces(scatter_last, 1)
    pieces(scatter_last, 2)
    common = [cp for cp in sent if not any(cp is other for other in only[0] + only[1])]
    for core in range(CORES):
        @on(core)
        def _():
            for cp in list(only[core]):
                cp.wait_send()

    for cp in common:
        cp.wait_send()
    assert len(sent) == n_copies, len(sent)


def weight_kernel(xf, dyf, dg_t, du_t, z_t, dx, og, ou, od, odx, buf, sem, dx_sem):
    slots, tile = buf.shape[1], buf.shape[3]
    tokens, hidden = dg_t.shape[1], og.shape[1]
    out = pltpu.make_async_copy(dx, odx, dx_sem)
    out.start()
    jobs = ((dg_t, xf, og), (du_t, xf, ou), (z_t, dyf, od))
    flight = {}
    for t in range(hidden // tile):
        cols = pl.ds(t * tile, tile)
        for i, (lhs, rhs, dst) in enumerate(jobs):
            slot = t % slots
            if (i, t - slots) in flight:
                flight[i, t - slots].wait()
            buf[i, slot] = jnp.dot(lhs[...], rhs[:, :, :, :, cols].reshape(tokens, tile), preferred_element_type=F32)
            flight[i, t] = pltpu.make_async_copy(buf.at[i, slot], dst.at[:, cols], sem.at[i, slot])
            flight[i, t].start()
    for t in range(hidden // tile - slots, hidden // tile):
        for i in range(len(jobs)):
            flight[i, t].wait()
    out.wait()


def solution(mesh):
    tp = mesh.shape["tp"]
    ring = math.isqrt(tp // CORES)

    def local_backward(x_loc, wg_loc, wu_loc, wd_loc, ug_loc, uu_loc, dy_loc):
        rows, hidden = x_loc.shape
        ffn = wd_loc.shape[0]
        tokens = tp * rows
        R = ring
        n_copies = 2 + 2 * (6 + 4 * R + 3 * R) + 2 * (8 + 4 * R + 2 * R - 1) + 4 * len(GROUPS) * 7
        full = (R, R, CORES, rows, hidden)
        vm = pltpu.VMEM
        out_bytes = 2 * (rows * hidden + 2 * tokens * hidden + 3 * ffn * tokens)
        dx, xf, dyf, dg_t, du_t, z_t = pl.pallas_call(
            lambda *refs: comm_kernel(R, n_copies, *refs),
            name="comm",
            out_shape=(vm((rows, hidden), BF16), vm(full, BF16), vm(full, BF16),
                       vm((ffn, tokens), BF16), vm((ffn, tokens), BF16), vm((ffn, tokens), BF16)),
            in_specs=[pl.BlockSpec(memory_space=pltpu.HBM)] * 7,
            out_specs=(pl.BlockSpec(memory_space=vm),) * 6,
            scratch_shapes=[
                vm((ffn, hidden), BF16), vm((ffn, hidden), BF16), vm((ffn, hidden), BF16),
                vm((ffn, tokens), BF16), vm((ffn, tokens), BF16),
                vm((tokens, ffn), F32), vm((tokens, ffn), F32), vm((tokens, ffn), F32),
                vm((tokens, ffn), BF16), vm((tokens, ffn), BF16),
                vm(full, BF16), vm((R, R, rows, hidden), BF16),
                vm((R, R, rows, hidden), F32), vm((R, rows, hidden), F32),
                *[vm((R, rows, hidden), F32)] * 4, *[vm((rows, hidden), F32)] * 4,
                pltpu.SemaphoreType.DMA((7,)),
                pltpu.SemaphoreType.DMA((n_copies,)),
                pltpu.SemaphoreType.DMA((n_copies,)),
            ],
            compiler_params=pltpu.CompilerParams(collective_id=0, has_side_effects=True,
                                                 vmem_limit_bytes=VMEM_BYTES - out_bytes - 40960),
        )(x_loc, dy_loc, wd_loc, wg_loc.T, wu_loc.T, ug_loc.T, uu_loc.T)
        out = jax.ShapeDtypeStruct((ffn, hidden), F32)
        hbm = pl.BlockSpec(memory_space=pltpu.HBM)
        gw_g, gw_u, gw_d, dx = pl.pallas_call(
            weight_kernel,
            name="weight_grads",
            out_shape=(out, out, out, jax.ShapeDtypeStruct((rows, hidden), BF16)),
            in_specs=[pl.BlockSpec(memory_space=vm)] * 6,
            out_specs=(hbm,) * 4,
            scratch_shapes=[vm((3, SLOTS, ffn, COL_TILE), F32), pltpu.SemaphoreType.DMA((3, SLOTS)),
                            pltpu.SemaphoreType.DMA],
            compiler_params=pltpu.CompilerParams(vmem_limit_bytes=28 << 20),
        )(xf, dyf, dg_t, du_t, z_t, dx)
        return dx, gw_g.T, gw_u.T, gw_d

    row_spec = P(("dp", "tp"), None)
    col_spec = P(None, "tp")
    part_cols = P("dp", "tp")
    return jax.shard_map(local_backward, mesh=mesh,
                         in_specs=(row_spec, col_spec, col_spec, P("tp", None), part_cols, part_cols, row_spec),
                         out_specs=(row_spec, part_cols, part_cols, row_spec),
                         check_vma=False)
```

```python
import functools
import math

import jax
import jax.numpy as jnp
from jax import lax
from jax.experimental import pallas as pl
from jax.experimental.pallas import tpu as pltpu
from jax.sharding import PartitionSpec as P

MESH = pl.DeviceIdType.MESH
BF16 = jnp.bfloat16
F32 = jnp.float32
CORES = 2
COL_TILE = 512
SLOTS = 4
MXU_TILE = 256
MERGED = 1
GROUPS = (2, 2, 1)
VMEM_BYTES = 67043328
NT = (((1,), (1,)), ((), ()))


def comm_kernel(ring, n_copies, x_hbm, dy_hbm, wd_hbm, wg_hbm, wu_hbm, ug_hbm, uu_hbm,
                dx_ref, xf, dyf, dg_t, du_t, z_t,
                wd, wg, wu, ug, uu, gate, up, mid, dgs, dus, pb, pr, sx, sy,
                lf, mg, rw, rm, lf2, mg2, rw2, rm2, lsem, ssem, rsem):
    R = ring
    me = lax.axis_index("tp")
    c = lax.rem(me, CORES)
    x = lax.rem(me // CORES, R)
    y = me // (CORES * R)
    oc = 1 - c
    rows, hidden = x_hbm.shape
    tokens = R * R * CORES * rows
    H2, Q = hidden // 2, hidden // 4
    xs = [lax.rem(x + d, R) for d in range(R)]
    ys = [lax.rem(y + d, R) for d in range(R)]

    def dev(yy, xx, cc):
        return {"tp": (yy * R + xx) * CORES + cc}

    def at(axis, s, core):
        return dev(y, xs[s % R], core) if axis == 0 else dev(ys[s % R], x, core)

    steps = [(axis, s) for axis in (0, 1) for s in (1, -1, 2)]
    nbr = {step: at(*step, c) for step in steps}
    across = {step: at(*step, oc) for step in steps}
    to_core = [{step: at(*step, core) for step in steps} for core in range(CORES)]
    mate = dev(y, x, oc)

    def local(src, dst, i):
        cp = pltpu.make_async_copy(src, dst, lsem.at[i])
        cp.start()
        return cp

    cp_dy = local(dy_hbm, dyf.at[y, x, c], 0)
    cp_x = local(x_hbm, xf.at[y, x, c], 1)
    cp_ug = local(ug_hbm, ug, 2)
    cp_uu = local(uu_hbm, uu, 3)
    cp_wd = local(wd_hbm, wd, 4)
    cp_wg = local(wg_hbm, wg, 5)
    cp_wu = local(wu_hbm, wu, 6)

    barrier = pltpu.get_barrier_semaphore()
    for d in (*nbr.values(), *across.values(), mate):
        pl.semaphore_signal(barrier, inc=1, device_id=d, device_id_type=MESH)
    pl.semaphore_wait(barrier, 2 * len(nbr) + 1)

    sent = []

    class Copy:
        def __init__(self, make, device):
            self.make, self.device, self.i, self.left = make, device, len(sent), False
            sent.append(self)
            self.describe().start()

        def describe(self):
            src, dst = self.make()
            return pltpu.make_async_remote_copy(src_ref=src, dst_ref=dst, send_sem=ssem.at[self.i],
                                                recv_sem=rsem.at[self.i], device_id=self.device,
                                                device_id_type=MESH)

        def wait_recv(self):
            self.describe().wait_recv()

        def wait_send(self):
            if not self.left:
                self.describe().wait_send()
            self.left = True

    def send(src, dst, device):
        return Copy(lambda: (src, dst), device)

    def share(make, device):
        return Copy(lambda: (make(), make()), device)

    class Half:
        def __init__(self, buf, first, own):
            self.buf, self.first, self.own = buf, first, own
            base = first * H2
            self.all, self.lo, self.hi = pl.ds(base, H2), pl.ds(base, Q), pl.ds(base + Q, Q)
            self.near, self.far, self.rows = {}, {}, {}

        def ref(self, d1, d2, cols, cores=slice(None)):
            if self.first == 0:
                return self.buf.at[ys[d2], xs[d1], cores, :, cols]
            return self.buf.at[ys[d1], xs[d2], cores, :, cols]

        def push(self, key, d1, axis, core=None):
            cores = slice(None) if core is None else pl.ds(core, 1)
            ref = functools.partial(self.ref, d1, 0, self.all, cores)
            to = to_core[self.own]
            self.near.setdefault(key, []).append((share(ref, to[axis, 1]), share(ref, to[axis, -1])))

        def relay(self, key, minus, plus, axis):
            for cp, _ in self.near[key]:
                cp.wait_recv()
            a = share(functools.partial(self.ref, *minus, self.lo), nbr[axis, 1])
            for _, cp in self.near[key]:
                cp.wait_recv()
            self.far[key] = [a, share(functools.partial(self.ref, *plus, self.hi), nbr[axis, -1])]

        def first_send(self, core):
            self.push("f", 0, self.first, core)

        def first_direct(self, core):
            ref = functools.partial(self.ref, 0, 0, self.all, pl.ds(core, 1))
            self.far.setdefault("f", []).append(share(ref, to_core[self.own][self.first, 2]))

        def first_near(self):
            for pair in self.near["f"]:
                for cp in pair:
                    cp.wait_recv()

        def first_relay(self):
            self.relay("f", (R - 1, 0), (1, 0), self.first)

        def first_far(self):
            for cp in self.far["f"]:
                cp.wait_recv()

        def second_home(self, core):
            self.push(0, 0, 1 - self.first, core)

        def second_send(self, d1):
            self.push(d1, d1, 1 - self.first)

        def second_relay(self, d1):
            self.relay(d1, (d1, R - 1), (d1, 1), 1 - self.first)

        def second_far(self, d1):
            for cp in self.far[d1]:
                cp.wait_recv()

        def to_mate(self, d2):
            def ref():
                if self.first == 0:
                    return self.buf.at[ys[d2], :, :, :, self.all]
                return self.buf.at[:, xs[d2], :, :, self.all]

            self.rows[d2] = share(ref, mate)

        def spot_to_mate(self, d1, d2, cores=slice(None)):
            self.rows[d1, d2] = share(functools.partial(self.ref, d1, d2, self.all, cores), mate)

        def home_to_mate(self):
            self.spot_to_mate(0, 0, pl.ds(self.own, 1))
            for d1 in range(1, R):
                self.spot_to_mate(d1, 0)

        def mate_rows(self, row):
            for key, cp in self.rows.items():
                if key == row or (isinstance(key, tuple) and key[1] == row):
                    cp.wait_recv()

    class Gather:
        def __init__(self, buf, own):
            self.halves = (Half(buf, 0, own), Half(buf, 1, own))

        def __getattr__(self, name):
            def both(*args):
                for h in self.halves:
                    getattr(h, name)(*args)
            return both

    def prepare():
        g_f = ug[...].astype(F32)
        u_f = uu[...].astype(F32)
        z_t[...] = (g_f * jax.nn.sigmoid(g_f) * u_f).astype(BF16)
        gate[...] = g_f.T
        up[...] = u_f.T

    def grads():
        mid[...] = lax.dot_general(dyf[...].reshape(tokens, hidden), wd[...], NT, preferred_element_type=F32)
        step = tokens // 8
        for i in range(8):
            tok = pl.ds(i * step, step)
            g_mid, g_f, u_f = mid[tok, :], gate[tok, :], up[tok, :]
            s = jax.nn.sigmoid(g_f)
            dgs[tok, :] = (g_mid * u_f * s * (1.0 + g_f * (1.0 - s))).astype(BF16)
            dus[tok, :] = (g_mid * (g_f * s)).astype(BF16)

    kinds = ((0, 1, 0), (1, 1, H2), (0, -1, Q), (1, -1, H2 + Q))
    widths = [t * MXU_TILE for t in GROUPS]
    starts = [sum(widths[:g]) for g in range(len(widths))]
    pair, leaf, raw, merged, leaf2, raw2, merged2 = {}, {}, {}, {}, {}, {}, {}

    def piece_cols(n, g):
        return pl.ds(kinds[n][2] + starts[g], widths[g])

    def partial(g, *ns):
        dg, du = dgs[...], dus[...]
        for n in ns:
            for t in range(GROUPS[g]):
                cols = pl.ds(kinds[n][2] + starts[g] + t * MXU_TILE, MXU_TILE)
                p = (jnp.dot(dg, wg[:, cols], preferred_element_type=F32)
                     + jnp.dot(du, wu[:, cols], preferred_element_type=F32))
                pb[:, :, :, :, cols] = p.astype(BF16).reshape(R, R, CORES, rows, MXU_TILE)
        for n in ns:
            cols = piece_cols(n, g)
            pair[n, g] = send(pb.at[:, :, oc, :, cols], pr.at[:, :, :, cols], mate)

    def line(n, d, cols):
        if kinds[n][0] == 0:
            return sx.at[:, xs[d], :, cols]
        return sx.at[ys[d], :, :, cols]

    def spot(n, d):
        return (ys if kinds[n][0] == 0 else xs)[d]

    def scatter_first(n, g):
        axis, s, _ = kinds[n]
        cols = piece_cols(n, g)
        pair[n, g].wait_recv()
        for yy in range(R):
            sx[yy, :, :, cols] = pb[yy, :, c, :, cols].astype(F32) + pr[yy, :, :, cols].astype(F32)
        leaf[n, g] = send(line(n, 2, cols), lf.at[:, :, cols], nbr[axis, s])

    def scatter_raw(n, g):
        axis, s, _ = kinds[n]
        cols = piece_cols(n, g)
        raw[n, g] = send(line(n, -s % R, cols), rw.at[:, :, cols], nbr[axis, -s])

    def scatter_merge(n, g):
        axis, s, _ = kinds[n]
        cols = piece_cols(n, g)
        leaf[n, g].wait_recv()
        mg[:, :, cols] = lf[:, :, cols] + line(n, s % R, cols)[...]
        merged[n, g] = send(mg.at[:, :, cols], rm.at[:, :, cols], nbr[axis, s])

    def scatter_second(n, g):
        axis, s, _ = kinds[n]
        cols = piece_cols(n, g)
        raw[n, g].wait_recv()
        merged[n, g].wait_recv()
        sy[:, :, cols] = line(n, 0, cols)[...] + rm[:, :, cols] + rw[:, :, cols]
        direct = g >= MERGED
        leaf2[n, g] = send(sy.at[spot(n, 2), :, cols], lf2.at[:, cols], nbr[1 - axis, 2 if direct else s])
        if direct:
            merged2[n, g] = send(sy.at[spot(n, s % R), :, cols], rm2.at[:, cols], nbr[1 - axis, s])
        raw2[n, g] = send(sy.at[spot(n, -s % R), :, cols], rw2.at[:, cols], nbr[1 - axis, -s])

    def scatter_merge2(n, g):
        assert g < MERGED
        axis, s, _ = kinds[n]
        cols = piece_cols(n, g)
        leaf2[n, g].wait_recv()
        mg2[:, cols] = lf2[:, cols] + sy[spot(n, s % R), :, cols]
        merged2[n, g] = send(mg2.at[:, cols], rm2.at[:, cols], nbr[1 - axis, s])

    def scatter_last(n, g):
        cols = piece_cols(n, g)
        raw2[n, g].wait_recv()
        merged2[n, g].wait_recv()
        total = sy[spot(n, 0), :, cols] + rm2[:, cols] + rw2[:, cols]
        if g >= MERGED:
            leaf2[n, g].wait_recv()
            total = total + lf2[:, cols]
        dx_ref[:, cols] = total.astype(BF16)

    def pieces(f, g):
        for n in range(len(kinds)):
            f(n, g)

    def transposes():
        dg_t[...] = dgs[...].astype(F32).T.astype(BF16)
        du_t[...] = dus[...].astype(F32).T.astype(BF16)

    gd, gx = Gather(dyf, 1), Gather(xf, 0)
    only = ([], [])

    def on(core):
        def run(f):
            @pl.when(c == core)
            def _():
                n = len(sent)
                f()
                only[core].extend(sent[n:])
        return run

    cp_dy.wait()
    swap = []

    @on(0)
    def _():
        gd.first_send(0)
        gd.second_home(0)
        gd.first_direct(0)
        gate = sent[-2:]
        swap.append(share(lambda: dyf.at[y, x, 0], mate))
        cp_x.wait()
        cp_ug.wait()
        cp_uu.wait()
        prepare()
        for cp in gate:
            cp.wait_send()
        gx.first_send(0)

    @on(1)
    def _():
        gd.first_send(1)
        gd.second_home(1)
        gd.first_direct(1)
        cp_x.wait()
        swap.append(share(lambda: xf.at[y, x, 1], mate))
        cp_ug.wait()
        cp_uu.wait()
        prepare()
        gd.first_near()
        gd.second_send(R - 1)
        gd.second_send(1)
        gx.first_send(1)
        gd.first_far()
        gd.second_send(2)
        gd.second_relay(0)
        swap[0].wait_recv()
        gd.home_to_mate()
        gd.second_relay(R - 1)
        gd.second_relay(1)
        gd.second_relay(2)
        gd.to_mate(R - 1)
        gd.to_mate(1)
        gx.second_home(1)
        gd.second_far(0)
        gd.spot_to_mate(0, 2)
        gd.second_far(R - 1)
        gd.spot_to_mate(R - 1, 2)
        gd.second_far(1)
        gd.spot_to_mate(1, 2)
        gd.second_far(2)
        gd.spot_to_mate(2, 2)
        cp_wd.wait()

    @on(0)
    def _():
        gx.first_relay()
        gd.mate_rows(0)
        gx.first_far()
        gx.second_home(0)
        gx.second_send(R - 1)
        gx.second_send(1)
        gx.second_send(2)
        gd.mate_rows(R - 1)
        gd.mate_rows(1)
        gx.second_relay(0)
        cp_wd.wait()
        gd.mate_rows(2)

    grads()

    def x_relay(d1):
        @on(0)
        def _():
            gx.second_relay(d1)

    cp_wg.wait()
    cp_wu.wait()
    partial(0, 0)
    partial(0, 1)
    partial(0, 2)
    partial(0, 3)
    scatter_first(0, 0)
    scatter_first(1, 0)
    x_relay(R - 1)
    partial(1, 0)
    scatter_first(2, 0)
    scatter_first(3, 0)
    x_relay(1)
    pieces(scatter_raw, 0)
    partial(1, 1)
    x_relay(2)
    partial(1, 2)
    partial(1, 3)
    partial(2, 0, 1)
    scatter_first(0, 1)
    scatter_first(1, 1)
    partial(2, 2, 3)
    scatter_first(2, 1)
    scatter_first(3, 1)
    pieces(scatter_merge, 0)
    pieces(scatter_raw, 1)
    pieces(scatter_first, 2)

    @on(0)
    def _():
        swap[1].wait_recv()
        gx.home_to_mate()
        gx.to_mate(R - 1)
        gx.to_mate(1)

    pieces(scatter_merge, 1)
    pieces(scatter_raw, 2)
    transposes()
    pieces(scatter_second, 0)
    pieces(scatter_merge, 2)
    pieces(scatter_second, 1)
    pieces(scatter_merge2, 0)

    @on(0)
    def _():
        gx.second_far(0)
        gx.second_far(R - 1)
        gx.second_far(1)
        gx.second_far(2)
        gx.to_mate(2)

    pieces(scatter_second, 2)

    @on(1)
    def _():
        for d in range(R):
            gx.mate_rows(d)

    pieces(scatter_last, 0)
    pieces(scatter_last, 1)
    pieces(scatter_last, 2)
    common = [cp for cp in sent if not any(cp is other for other in only[0] + only[1])]
    for core in range(CORES):
        @on(core)
        def _():
            for cp in list(only[core]):
                cp.wait_send()

    for cp in common:
        cp.wait_send()
    assert len(sent) == n_copies, len(sent)


def weight_kernel(xf, dyf, dg_t, du_t, z_t, dx, og, ou, od, odx, buf, sem, dx_sem):
    slots, tile = buf.shape[1], buf.shape[3]
    tokens, hidden = dg_t.shape[1], og.shape[1]
    out = pltpu.make_async_copy(dx, odx, dx_sem)
    out.start()
    jobs = ((dg_t, xf, og), (du_t, xf, ou), (z_t, dyf, od))
    flight = {}
    for t in range(hidden // tile):
        cols = pl.ds(t * tile, tile)
        for i, (lhs, rhs, dst) in enumerate(jobs):
            slot = t % slots
            if (i, t - slots) in flight:
                flight[i, t - slots].wait()
            buf[i, slot] = jnp.dot(lhs[...], rhs[:, :, :, :, cols].reshape(tokens, tile), preferred_element_type=F32)
            flight[i, t] = pltpu.make_async_copy(buf.at[i, slot], dst.at[:, cols], sem.at[i, slot])
            flight[i, t].start()
    for t in range(hidden // tile - slots, hidden // tile):
        for i in range(len(jobs)):
            flight[i, t].wait()
    out.wait()


def solution(mesh):
    tp = mesh.shape["tp"]
    ring = math.isqrt(tp // CORES)

    def local_backward(x_loc, wg_loc, wu_loc, wd_loc, ug_loc, uu_loc, dy_loc):
        rows, hidden = x_loc.shape
        ffn = wd_loc.shape[0]
        tokens = tp * rows
        R = ring
        n_copies = 2 + 2 * (6 + 4 * R + 3 * R) + 2 * (8 + 4 * R + 2 * R - 1) + 4 * len(GROUPS) * 7
        full = (R, R, CORES, rows, hidden)
        vm = pltpu.VMEM
        out_bytes = 2 * (rows * hidden + 2 * tokens * hidden + 3 * ffn * tokens)
        dx, xf, dyf, dg_t, du_t, z_t = pl.pallas_call(
            lambda *refs: comm_kernel(R, n_copies, *refs),
            name="comm",
            out_shape=(vm((rows, hidden), BF16), vm(full, BF16), vm(full, BF16),
                       vm((ffn, tokens), BF16), vm((ffn, tokens), BF16), vm((ffn, tokens), BF16)),
            in_specs=[pl.BlockSpec(memory_space=pltpu.HBM)] * 7,
            out_specs=(pl.BlockSpec(memory_space=vm),) * 6,
            scratch_shapes=[
                vm((ffn, hidden), BF16), vm((ffn, hidden), BF16), vm((ffn, hidden), BF16),
                vm((ffn, tokens), BF16), vm((ffn, tokens), BF16),
                vm((tokens, ffn), F32), vm((tokens, ffn), F32), vm((tokens, ffn), F32),
                vm((tokens, ffn), BF16), vm((tokens, ffn), BF16),
                vm(full, BF16), vm((R, R, rows, hidden), BF16),
                vm((R, R, rows, hidden), F32), vm((R, rows, hidden), F32),
                *[vm((R, rows, hidden), F32)] * 4, *[vm((rows, hidden), F32)] * 4,
                pltpu.SemaphoreType.DMA((7,)),
                pltpu.SemaphoreType.DMA((n_copies,)),
                pltpu.SemaphoreType.DMA((n_copies,)),
            ],
            compiler_params=pltpu.CompilerParams(collective_id=0, has_side_effects=True,
                                                 vmem_limit_bytes=VMEM_BYTES - out_bytes - 40960),
        )(x_loc, dy_loc, wd_loc, wg_loc.T, wu_loc.T, ug_loc.T, uu_loc.T)
        out = jax.ShapeDtypeStruct((ffn, hidden), F32)
        hbm = pl.BlockSpec(memory_space=pltpu.HBM)
        gw_g, gw_u, gw_d, dx = pl.pallas_call(
            weight_kernel,
            name="weight_grads",
            out_shape=(out, out, out, jax.ShapeDtypeStruct((rows, hidden), BF16)),
            in_specs=[pl.BlockSpec(memory_space=vm)] * 6,
            out_specs=(hbm,) * 4,
            scratch_shapes=[vm((3, SLOTS, ffn, COL_TILE), F32), pltpu.SemaphoreType.DMA((3, SLOTS)),
                            pltpu.SemaphoreType.DMA],
            compiler_params=pltpu.CompilerParams(vmem_limit_bytes=28 << 20),
        )(xf, dyf, dg_t, du_t, z_t, dx)
        return dx, gw_g.T, gw_u.T, gw_d

    row_spec = P(("dp", "tp"), None)
    col_spec = P(None, "tp")
    part_cols = P("dp", "tp")
    return jax.shard_map(local_backward, mesh=mesh,
                         in_specs=(row_spec, col_spec, col_spec, P("tp", None), part_cols, part_cols, row_spec),
                         out_specs=(row_spec, part_cols, part_cols, row_spec),
                         check_vma=False)
```

```python
import functools
import math

import jax
import jax.numpy as jnp
from jax import lax
from jax.experimental import pallas as pl
from jax.experimental.pallas import tpu as pltpu
from jax.sharding import PartitionSpec as P

MESH = pl.DeviceIdType.MESH
BF16 = jnp.bfloat16
F32 = jnp.float32
CORES = 2
COL_TILE = 512
SLOTS = 4
MXU_TILE = 256
MERGED = 1
GROUPS = (2, 2, 1)
VMEM_BYTES = 67043328
NT = (((1,), (1,)), ((), ()))


def comm_kernel(ring, n_copies, x_hbm, dy_hbm, wd_hbm, wg_hbm, wu_hbm, ug_hbm, uu_hbm,
                dx_ref, xf, dyf, dg_t, du_t, z_t,
                wd, wg, wu, ug, uu, gate, up, mid, dgs, dus, pb, pr, sx, sy,
                lf, mg, rw, rm, lf2, mg2, rw2, rm2, lsem, ssem, rsem):
    R = ring
    me = lax.axis_index("tp")
    c = lax.rem(me, CORES)
    x = lax.rem(me // CORES, R)
    y = me // (CORES * R)
    oc = 1 - c
    rows, hidden = x_hbm.shape
    tokens = R * R * CORES * rows
    H2, Q = hidden // 2, hidden // 4
    xs = [lax.rem(x + d, R) for d in range(R)]
    ys = [lax.rem(y + d, R) for d in range(R)]

    def dev(yy, xx, cc):
        return {"tp": (yy * R + xx) * CORES + cc}

    def at(axis, s, core):
        return dev(y, xs[s % R], core) if axis == 0 else dev(ys[s % R], x, core)

    steps = [(axis, s) for axis in (0, 1) for s in (1, -1, 2)]
    nbr = {step: at(*step, c) for step in steps}
    across = {step: at(*step, oc) for step in steps}
    to_core = [{step: at(*step, core) for step in steps} for core in range(CORES)]
    mate = dev(y, x, oc)

    def local(src, dst, i):
        cp = pltpu.make_async_copy(src, dst, lsem.at[i])
        cp.start()
        return cp

    cp_dy = local(dy_hbm, dyf.at[y, x, c], 0)
    cp_x = local(x_hbm, xf.at[y, x, c], 1)
    cp_ug = local(ug_hbm, ug, 2)
    cp_uu = local(uu_hbm, uu, 3)
    cp_wd = local(wd_hbm, wd, 4)
    cp_wg = local(wg_hbm, wg, 5)
    cp_wu = local(wu_hbm, wu, 6)

    barrier = pltpu.get_barrier_semaphore()
    for d in (*nbr.values(), *across.values(), mate):
        pl.semaphore_signal(barrier, inc=1, device_id=d, device_id_type=MESH)
    pl.semaphore_wait(barrier, 2 * len(nbr) + 1)

    sent = []

    class Copy:
        def __init__(self, make, device):
            self.make, self.device, self.i, self.left = make, device, len(sent), False
            sent.append(self)
            self.describe().start()

        def describe(self):
            src, dst = self.make()
            return pltpu.make_async_remote_copy(src_ref=src, dst_ref=dst, send_sem=ssem.at[self.i],
                                                recv_sem=rsem.at[self.i], device_id=self.device,
                                                device_id_type=MESH)

        def wait_recv(self):
            self.describe().wait_recv()

        def wait_send(self):
            if not self.left:
                self.describe().wait_send()
            self.left = True

    def send(src, dst, device):
        return Copy(lambda: (src, dst), device)

    def share(make, device):
        return Copy(lambda: (make(), make()), device)

    class Half:
        def __init__(self, buf, first, own):
            self.buf, self.first, self.own = buf, first, own
            base = first * H2
            self.all, self.lo, self.hi = pl.ds(base, H2), pl.ds(base, Q), pl.ds(base + Q, Q)
            self.near, self.far, self.rows = {}, {}, {}

        def ref(self, d1, d2, cols, cores=slice(None)):
            if self.first == 0:
                return self.buf.at[ys[d2], xs[d1], cores, :, cols]
            return self.buf.at[ys[d1], xs[d2], cores, :, cols]

        def push(self, key, d1, axis, core=None):
            cores = slice(None) if core is None else pl.ds(core, 1)
            ref = functools.partial(self.ref, d1, 0, self.all, cores)
            to = to_core[self.own]
            self.near.setdefault(key, []).append((share(ref, to[axis, 1]), share(ref, to[axis, -1])))

        def relay(self, key, minus, plus, axis):
            for cp, _ in self.near[key]:
                cp.wait_recv()
            a = share(functools.partial(self.ref, *minus, self.lo), nbr[axis, 1])
            for _, cp in self.near[key]:
                cp.wait_recv()
            self.far[key] = [a, share(functools.partial(self.ref, *plus, self.hi), nbr[axis, -1])]

        def first_send(self, core):
            self.push("f", 0, self.first, core)

        def first_direct(self, core):
            ref = functools.partial(self.ref, 0, 0, self.all, pl.ds(core, 1))
            self.far.setdefault("f", []).append(share(ref, to_core[self.own][self.first, 2]))

        def first_near(self):
            for pair in self.near["f"]:
                for cp in pair:
                    cp.wait_recv()

        def first_relay(self):
            self.relay("f", (R - 1, 0), (1, 0), self.first)

        def first_far(self):
            for cp in self.far["f"]:
                cp.wait_recv()

        def second_home(self, core):
            self.push(0, 0, 1 - self.first, core)

        def second_send(self, d1):
            self.push(d1, d1, 1 - self.first)

        def second_relay(self, d1):
            self.relay(d1, (d1, R - 1), (d1, 1), 1 - self.first)

        def second_far(self, d1):
            for cp in self.far[d1]:
                cp.wait_recv()

        def to_mate(self, d2):
            def ref():
                if self.first == 0:
                    return self.buf.at[ys[d2], :, :, :, self.all]
                return self.buf.at[:, xs[d2], :, :, self.all]

            self.rows[d2] = share(ref, mate)

        def spot_to_mate(self, d1, d2, cores=slice(None)):
            self.rows[d1, d2] = share(functools.partial(self.ref, d1, d2, self.all, cores), mate)

        def home_to_mate(self):
            self.spot_to_mate(0, 0, pl.ds(self.own, 1))
            for d1 in range(1, R):
                self.spot_to_mate(d1, 0)

        def mate_rows(self, row):
            for key, cp in self.rows.items():
                if key == row or (isinstance(key, tuple) and key[1] == row):
                    cp.wait_recv()

    class Gather:
        def __init__(self, buf, own):
            self.halves = (Half(buf, 0, own), Half(buf, 1, own))

        def __getattr__(self, name):
            def both(*args):
                for h in self.halves:
                    getattr(h, name)(*args)
            return both

    def prepare():
        g_f = ug[...].astype(F32)
        u_f = uu[...].astype(F32)
        z_t[...] = (g_f * jax.nn.sigmoid(g_f) * u_f).astype(BF16)
        gate[...] = g_f.T
        up[...] = u_f.T

    def grads():
        mid[...] = lax.dot_general(dyf[...].reshape(tokens, hidden), wd[...], NT, preferred_element_type=F32)
        step = tokens // 8
        for i in range(8):
            tok = pl.ds(i * step, step)
            g_mid, g_f, u_f = mid[tok, :], gate[tok, :], up[tok, :]
            s = jax.nn.sigmoid(g_f)
            dgs[tok, :] = (g_mid * u_f * s * (1.0 + g_f * (1.0 - s))).astype(BF16)
            dus[tok, :] = (g_mid * (g_f * s)).astype(BF16)

    kinds = ((0, 1, 0), (1, 1, H2), (0, -1, Q), (1, -1, H2 + Q))
    widths = [t * MXU_TILE for t in GROUPS]
    starts = [sum(widths[:g]) for g in range(len(widths))]
    pair, leaf, raw, merged, leaf2, raw2, merged2 = {}, {}, {}, {}, {}, {}, {}

    def piece_cols(n, g):
        return pl.ds(kinds[n][2] + starts[g], widths[g])

    def partial(g, *ns):
        dg, du = dgs[...], dus[...]
        for n in ns:
            for t in range(GROUPS[g]):
                cols = pl.ds(kinds[n][2] + starts[g] + t * MXU_TILE, MXU_TILE)
                p = (jnp.dot(dg, wg[:, cols], preferred_element_type=F32)
                     + jnp.dot(du, wu[:, cols], preferred_element_type=F32))
                pb[:, :, :, :, cols] = p.astype(BF16).reshape(R, R, CORES, rows, MXU_TILE)
        for n in ns:
            cols = piece_cols(n, g)
            pair[n, g] = send(pb.at[:, :, oc, :, cols], pr.at[:, :, :, cols], mate)

    def line(n, d, cols):
        if kinds[n][0] == 0:
            return sx.at[:, xs[d], :, cols]
        return sx.at[ys[d], :, :, cols]

    def spot(n, d):
        return (ys if kinds[n][0] == 0 else xs)[d]

    def scatter_first(n, g):
        axis, s, _ = kinds[n]
        cols = piece_cols(n, g)
        pair[n, g].wait_recv()
        for yy in range(R):
            sx[yy, :, :, cols] = pb[yy, :, c, :, cols].astype(F32) + pr[yy, :, :, cols].astype(F32)
        leaf[n, g] = send(line(n, 2, cols), lf.at[:, :, cols], nbr[axis, s])

    def scatter_raw(n, g):
        axis, s, _ = kinds[n]
        cols = piece_cols(n, g)
        raw[n, g] = send(line(n, -s % R, cols), rw.at[:, :, cols], nbr[axis, -s])

    def scatter_merge(n, g):
        axis, s, _ = kinds[n]
        cols = piece_cols(n, g)
        leaf[n, g].wait_recv()
        mg[:, :, cols] = lf[:, :, cols] + line(n, s % R, cols)[...]
        merged[n, g] = send(mg.at[:, :, cols], rm.at[:, :, cols], nbr[axis, s])

    def scatter_second(n, g):
        axis, s, _ = kinds[n]
        cols = piece_cols(n, g)
        raw[n, g].wait_recv()
        merged[n, g].wait_recv()
        sy[:, :, cols] = line(n, 0, cols)[...] + rm[:, :, cols] + rw[:, :, cols]
        direct = g >= MERGED
        leaf2[n, g] = send(sy.at[spot(n, 2), :, cols], lf2.at[:, cols], nbr[1 - axis, 2 if direct else s])
        if direct:
            merged2[n, g] = send(sy.at[spot(n, s % R), :, cols], rm2.at[:, cols], nbr[1 - axis, s])
        raw2[n, g] = send(sy.at[spot(n, -s % R), :, cols], rw2.at[:, cols], nbr[1 - axis, -s])

    def scatter_merge2(n, g):
        assert g < MERGED
        axis, s, _ = kinds[n]
        cols = piece_cols(n, g)
        leaf2[n, g].wait_recv()
        mg2[:, cols] = lf2[:, cols] + sy[spot(n, s % R), :, cols]
        merged2[n, g] = send(mg2.at[:, cols], rm2.at[:, cols], nbr[1 - axis, s])

    def scatter_last(n, g):
        cols = piece_cols(n, g)
        raw2[n, g].wait_recv()
        merged2[n, g].wait_recv()
        total = sy[spot(n, 0), :, cols] + rm2[:, cols] + rw2[:, cols]
        if g >= MERGED:
            leaf2[n, g].wait_recv()
            total = total + lf2[:, cols]
        dx_ref[:, cols] = total.astype(BF16)

    def pieces(f, g):
        for n in range(len(kinds)):
            f(n, g)

    def transposes():
        dg_t[...] = dgs[...].astype(F32).T.astype(BF16)
        du_t[...] = dus[...].astype(F32).T.astype(BF16)

    gd, gx = Gather(dyf, 1), Gather(xf, 0)
    only = ([], [])

    def on(core):
        def run(f):
            @pl.when(c == core)
            def _():
                n = len(sent)
                f()
                only[core].extend(sent[n:])
        return run

    cp_dy.wait()
    swap = []

    @on(0)
    def _():
        gd.first_send(0)
        gd.second_home(0)
        gd.first_direct(0)
        swap.append(share(lambda: dyf.at[y, x, 0], mate))
        cp_x.wait()
        gx.first_send(0)
        cp_ug.wait()
        cp_uu.wait()
        prepare()

    @on(1)
    def _():
        gd.first_send(1)
        gd.second_home(1)
        gd.first_direct(1)
        cp_x.wait()
        gx.first_send(1)
        swap.append(share(lambda: xf.at[y, x, 1], mate))
        cp_ug.wait()
        cp_uu.wait()
        prepare()
        gd.first_near()
        gd.second_send(R - 1)
        gd.second_send(1)
        gd.first_far()
        gd.second_send(2)
        gd.second_relay(0)
        gx.second_home(1)
        swap[0].wait_recv()
        gd.home_to_mate()
        gd.second_relay(R - 1)
        gd.second_relay(1)
        gd.second_relay(2)
        gd.to_mate(R - 1)
        gd.to_mate(1)
        gd.second_far(0)
        gd.spot_to_mate(0, 2)
        gd.second_far(R - 1)
        gd.spot_to_mate(R - 1, 2)
        gd.second_far(1)
        gd.spot_to_mate(1, 2)
        gd.second_far(2)
        gd.spot_to_mate(2, 2)
        cp_wd.wait()

    @on(0)
    def _():
        gx.first_relay()
        gx.second_home(0)
        gd.mate_rows(0)
        gx.first_far()
        gx.second_send(R - 1)
        gx.second_send(1)
        gx.second_send(2)
        gd.mate_rows(R - 1)
        gd.mate_rows(1)
        gx.second_relay(0)
        cp_wd.wait()
        gd.mate_rows(2)

    grads()

    def x_relay(d1):
        @on(0)
        def _():
            gx.second_relay(d1)

    cp_wg.wait()
    cp_wu.wait()
    partial(0, 0)
    partial(0, 1)
    partial(0, 2)
    partial(0, 3)
    scatter_first(0, 0)
    scatter_first(1, 0)
    x_relay(R - 1)
    partial(1, 0)
    scatter_first(2, 0)
    scatter_first(3, 0)
    x_relay(1)
    pieces(scatter_raw, 0)
    partial(1, 1)
    x_relay(2)
    partial(1, 2)
    partial(1, 3)
    partial(2, 0, 1)
    scatter_first(0, 1)
    scatter_first(1, 1)
    partial(2, 2, 3)
    scatter_first(2, 1)
    scatter_first(3, 1)
    pieces(scatter_merge, 0)
    pieces(scatter_raw, 1)
    pieces(scatter_first, 2)

    @on(0)
    def _():
        swap[1].wait_recv()
        gx.home_to_mate()
        gx.to_mate(R - 1)
        gx.to_mate(1)

    pieces(scatter_merge, 1)
    pieces(scatter_raw, 2)
    transposes()
    pieces(scatter_second, 0)
    pieces(scatter_merge, 2)
    pieces(scatter_second, 1)
    pieces(scatter_merge2, 0)

    @on(0)
    def _():
        gx.second_far(0)
        gx.second_far(R - 1)
        gx.second_far(1)
        gx.second_far(2)
        gx.to_mate(2)

    pieces(scatter_second, 2)

    @on(1)
    def _():
        for d in range(R):
            gx.mate_rows(d)

    pieces(scatter_last, 0)
    pieces(scatter_last, 1)
    pieces(scatter_last, 2)
    common = [cp for cp in sent if not any(cp is other for other in only[0] + only[1])]
    for core in range(CORES):
        @on(core)
        def _():
            for cp in list(only[core]):
                cp.wait_send()

    for cp in common:
        cp.wait_send()
    assert len(sent) == n_copies, len(sent)


def weight_kernel(xf, dyf, dg_t, du_t, z_t, dx, og, ou, od, odx, buf, sem, dx_sem):
    slots, tile = buf.shape[1], buf.shape[3]
    tokens, hidden = dg_t.shape[1], og.shape[1]
    out = pltpu.make_async_copy(dx, odx, dx_sem)
    out.start()
    jobs = ((dg_t, xf, og), (du_t, xf, ou), (z_t, dyf, od))
    flight = {}
    for t in range(hidden // tile):
        cols = pl.ds(t * tile, tile)
        for i, (lhs, rhs, dst) in enumerate(jobs):
            slot = t % slots
            if (i, t - slots) in flight:
                flight[i, t - slots].wait()
            buf[i, slot] = jnp.dot(lhs[...], rhs[:, :, :, :, cols].reshape(tokens, tile), preferred_element_type=F32)
            flight[i, t] = pltpu.make_async_copy(buf.at[i, slot], dst.at[:, cols], sem.at[i, slot])
            flight[i, t].start()
    for t in range(hidden // tile - slots, hidden // tile):
        for i in range(len(jobs)):
            flight[i, t].wait()
    out.wait()


def solution(mesh):
    tp = mesh.shape["tp"]
    ring = math.isqrt(tp // CORES)

    def local_backward(x_loc, wg_loc, wu_loc, wd_loc, ug_loc, uu_loc, dy_loc):
        rows, hidden = x_loc.shape
        ffn = wd_loc.shape[0]
        tokens = tp * rows
        R = ring
        n_copies = 2 + 2 * (6 + 4 * R + 3 * R) + 2 * (8 + 4 * R + 2 * R - 1) + 4 * len(GROUPS) * 7
        full = (R, R, CORES, rows, hidden)
        vm = pltpu.VMEM
        out_bytes = 2 * (rows * hidden + 2 * tokens * hidden + 3 * ffn * tokens)
        dx, xf, dyf, dg_t, du_t, z_t = pl.pallas_call(
            lambda *refs: comm_kernel(R, n_copies, *refs),
            name="comm",
            out_shape=(vm((rows, hidden), BF16), vm(full, BF16), vm(full, BF16),
                       vm((ffn, tokens), BF16), vm((ffn, tokens), BF16), vm((ffn, tokens), BF16)),
            in_specs=[pl.BlockSpec(memory_space=pltpu.HBM)] * 7,
            out_specs=(pl.BlockSpec(memory_space=vm),) * 6,
            scratch_shapes=[
                vm((ffn, hidden), BF16), vm((ffn, hidden), BF16), vm((ffn, hidden), BF16),
                vm((ffn, tokens), BF16), vm((ffn, tokens), BF16),
                vm((tokens, ffn), F32), vm((tokens, ffn), F32), vm((tokens, ffn), F32),
                vm((tokens, ffn), BF16), vm((tokens, ffn), BF16),
                vm(full, BF16), vm((R, R, rows, hidden), BF16),
                vm((R, R, rows, hidden), F32), vm((R, rows, hidden), F32),
                *[vm((R, rows, hidden), F32)] * 4, *[vm((rows, hidden), F32)] * 4,
                pltpu.SemaphoreType.DMA((7,)),
                pltpu.SemaphoreType.DMA((n_copies,)),
                pltpu.SemaphoreType.DMA((n_copies,)),
            ],
            compiler_params=pltpu.CompilerParams(collective_id=0, has_side_effects=True,
                                                 vmem_limit_bytes=VMEM_BYTES - out_bytes - 40960),
        )(x_loc, dy_loc, wd_loc, wg_loc.T, wu_loc.T, ug_loc.T, uu_loc.T)
        out = jax.ShapeDtypeStruct((ffn, hidden), F32)
        hbm = pl.BlockSpec(memory_space=pltpu.HBM)
        gw_g, gw_u, gw_d, dx = pl.pallas_call(
            weight_kernel,
            name="weight_grads",
            out_shape=(out, out, out, jax.ShapeDtypeStruct((rows, hidden), BF16)),
            in_specs=[pl.BlockSpec(memory_space=vm)] * 6,
            out_specs=(hbm,) * 4,
            scratch_shapes=[vm((3, SLOTS, ffn, COL_TILE), F32), pltpu.SemaphoreType.DMA((3, SLOTS)),
                            pltpu.SemaphoreType.DMA],
            compiler_params=pltpu.CompilerParams(vmem_limit_bytes=28 << 20),
        )(xf, dyf, dg_t, du_t, z_t, dx)
        return dx, gw_g.T, gw_u.T, gw_d

    row_spec = P(("dp", "tp"), None)
    col_spec = P(None, "tp")
    part_cols = P("dp", "tp")
    return jax.shard_map(local_backward, mesh=mesh,
                         in_specs=(row_spec, col_spec, col_spec, P("tp", None), part_cols, part_cols, row_spec),
                         out_specs=(row_spec, part_cols, part_cols, row_spec),
                         check_vma=False)
```

```python
import functools
import math

import jax
import jax.numpy as jnp
from jax import lax
from jax.experimental import pallas as pl
from jax.experimental.pallas import tpu as pltpu
from jax.sharding import PartitionSpec as P

MESH = pl.DeviceIdType.MESH
BF16 = jnp.bfloat16
F32 = jnp.float32
CORES = 2
COL_TILE = 512
SLOTS = 4
MXU_TILE = 256
MERGED = 1
GROUPS = (2, 2, 1)
VMEM_BYTES = 67043328
NT = (((1,), (1,)), ((), ()))


def comm_kernel(ring, n_copies, x_hbm, dy_hbm, wd_hbm, wg_hbm, wu_hbm, ug_hbm, uu_hbm,
                dx_ref, xf, dyf, dg_t, du_t, z_t,
                wd, wg, wu, ug, uu, gate, up, mid, dgs, dus, pb, pr, sx, sy,
                lf, mg, rw, rm, lf2, mg2, rw2, rm2, lsem, ssem, rsem):
    R = ring
    me = lax.axis_index("tp")
    c = lax.rem(me, CORES)
    x = lax.rem(me // CORES, R)
    y = me // (CORES * R)
    oc = 1 - c
    rows, hidden = x_hbm.shape
    tokens = R * R * CORES * rows
    H2, Q = hidden // 2, hidden // 4
    xs = [lax.rem(x + d, R) for d in range(R)]
    ys = [lax.rem(y + d, R) for d in range(R)]

    def dev(yy, xx, cc):
        return {"tp": (yy * R + xx) * CORES + cc}

    def at(axis, s, core):
        return dev(y, xs[s % R], core) if axis == 0 else dev(ys[s % R], x, core)

    steps = [(axis, s) for axis in (0, 1) for s in (1, -1, 2)]
    nbr = {step: at(*step, c) for step in steps}
    across = {step: at(*step, oc) for step in steps}
    to_core = [{step: at(*step, core) for step in steps} for core in range(CORES)]
    mate = dev(y, x, oc)

    def local(src, dst, i):
        cp = pltpu.make_async_copy(src, dst, lsem.at[i])
        cp.start()
        return cp

    cp_dy = local(dy_hbm, dyf.at[y, x, c], 0)
    cp_x = local(x_hbm, xf.at[y, x, c], 1)
    cp_ug = local(ug_hbm, ug, 2)
    cp_uu = local(uu_hbm, uu, 3)
    cp_wd = local(wd_hbm, wd, 4)
    cp_wg = local(wg_hbm, wg, 5)
    cp_wu = local(wu_hbm, wu, 6)

    barrier = pltpu.get_barrier_semaphore()
    for d in (*nbr.values(), *across.values(), mate):
        pl.semaphore_signal(barrier, inc=1, device_id=d, device_id_type=MESH)
    pl.semaphore_wait(barrier, 2 * len(nbr) + 1)

    sent = []

    class Copy:
        def __init__(self, make, device):
            self.make, self.device, self.i = make, device, len(sent)
            sent.append(self)
            self.describe().start()

        def describe(self):
            src, dst = self.make()
            return pltpu.make_async_remote_copy(src_ref=src, dst_ref=dst, send_sem=ssem.at[self.i],
                                                recv_sem=rsem.at[self.i], device_id=self.device,
                                                device_id_type=MESH)

        def wait_recv(self):
            self.describe().wait_recv()

        def wait_send(self):
            self.describe().wait_send()

    def send(src, dst, device):
        return Copy(lambda: (src, dst), device)

    def share(make, device):
        return Copy(lambda: (make(), make()), device)

    class Half:
        def __init__(self, buf, first, own):
            self.buf, self.first, self.own = buf, first, own
            base = first * H2
            self.all, self.lo, self.hi = pl.ds(base, H2), pl.ds(base, Q), pl.ds(base + Q, Q)
            self.near, self.far, self.rows = {}, {}, {}

        def ref(self, d1, d2, cols, cores=slice(None)):
            if self.first == 0:
                return self.buf.at[ys[d2], xs[d1], cores, :, cols]
            return self.buf.at[ys[d1], xs[d2], cores, :, cols]

        def push(self, key, d1, axis, core=None):
            cores = slice(None) if core is None else pl.ds(core, 1)
            ref = functools.partial(self.ref, d1, 0, self.all, cores)
            to = to_core[self.own]
            self.near.setdefault(key, []).append((share(ref, to[axis, 1]), share(ref, to[axis, -1])))
            return ref

        def relay(self, key, minus, plus, axis):
            for cp, _ in self.near[key]:
                cp.wait_recv()
            a = share(functools.partial(self.ref, *minus, self.lo), nbr[axis, 1])
            for _, cp in self.near[key]:
                cp.wait_recv()
            self.far[key] = [a, share(functools.partial(self.ref, *plus, self.hi), nbr[axis, -1])]

        def first_send(self, core):
            self.push("f", 0, self.first, core)

        def first_direct(self, core):
            ref = self.push("f", 0, self.first, core)
            self.far.setdefault("f", []).append(share(ref, to_core[self.own][self.first, 2]))

        def first_near(self):
            for pair in self.near["f"]:
                for cp in pair:
                    cp.wait_recv()

        def first_relay(self):
            self.relay("f", (R - 1, 0), (1, 0), self.first)

        def first_far(self):
            for cp in self.far["f"]:
                cp.wait_recv()

        def second_home(self, core):
            self.push(0, 0, 1 - self.first, core)

        def second_send(self, d1):
            self.push(d1, d1, 1 - self.first)

        def second_relay(self, d1):
            self.relay(d1, (d1, R - 1), (d1, 1), 1 - self.first)

        def second_far(self, d1):
            for cp in self.far[d1]:
                cp.wait_recv()

        def to_mate(self, d2):
            def ref():
                if self.first == 0:
                    return self.buf.at[ys[d2], :, :, :, self.all]
                return self.buf.at[:, xs[d2], :, :, self.all]

            self.rows[d2] = share(ref, mate)

        def spot_to_mate(self, d1, d2, cores=slice(None)):
            self.rows[d1, d2] = share(functools.partial(self.ref, d1, d2, self.all, cores), mate)

        def home_to_mate(self):
            self.spot_to_mate(0, 0, pl.ds(self.own, 1))
            for d1 in range(1, R):
                self.spot_to_mate(d1, 0)

        def mate_rows(self, row):
            for key, cp in self.rows.items():
                if key == row or (isinstance(key, tuple) and key[1] == row):
                    cp.wait_recv()

    class Gather:
        def __init__(self, buf, own):
            self.halves = (Half(buf, 0, own), Half(buf, 1, own))

        def __getattr__(self, name):
            def both(*args):
                for h in self.halves:
                    getattr(h, name)(*args)
            return both

    def prepare():
        g_f = ug[...].astype(F32)
        u_f = uu[...].astype(F32)
        z_t[...] = (g_f * jax.nn.sigmoid(g_f) * u_f).astype(BF16)
        gate[...] = g_f.T
        up[...] = u_f.T

    def grads():
        mid[...] = lax.dot_general(dyf[...].reshape(tokens, hidden), wd[...], NT, preferred_element_type=F32)
        step = tokens // 8
        for i in range(8):
            tok = pl.ds(i * step, step)
            g_mid, g_f, u_f = mid[tok, :], gate[tok, :], up[tok, :]
            s = jax.nn.sigmoid(g_f)
            dgs[tok, :] = (g_mid * u_f * s * (1.0 + g_f * (1.0 - s))).astype(BF16)
            dus[tok, :] = (g_mid * (g_f * s)).astype(BF16)

    kinds = ((0, 1, 0), (1, 1, H2), (0, -1, Q), (1, -1, H2 + Q))
    widths = [t * MXU_TILE for t in GROUPS]
    starts = [sum(widths[:g]) for g in range(len(widths))]
    pair, leaf, raw, merged, leaf2, raw2, merged2 = {}, {}, {}, {}, {}, {}, {}

    def piece_cols(n, g):
        return pl.ds(kinds[n][2] + starts[g], widths[g])

    def partial(g, *ns):
        dg, du = dgs[...], dus[...]
        for n in ns:
            for t in range(GROUPS[g]):
                cols = pl.ds(kinds[n][2] + starts[g] + t * MXU_TILE, MXU_TILE)
                p = (jnp.dot(dg, wg[:, cols], preferred_element_type=F32)
                     + jnp.dot(du, wu[:, cols], preferred_element_type=F32))
                pb[:, :, :, :, cols] = p.astype(BF16).reshape(R, R, CORES, rows, MXU_TILE)
        for n in ns:
            cols = piece_cols(n, g)
            pair[n, g] = send(pb.at[:, :, oc, :, cols], pr.at[:, :, :, cols], mate)

    def line(n, d, cols):
        if kinds[n][0] == 0:
            return sx.at[:, xs[d], :, cols]
        return sx.at[ys[d], :, :, cols]

    def spot(n, d):
        return (ys if kinds[n][0] == 0 else xs)[d]

    def scatter_first(n, g):
        axis, s, _ = kinds[n]
        cols = piece_cols(n, g)
        pair[n, g].wait_recv()
        for yy in range(R):
            sx[yy, :, :, cols] = pb[yy, :, c, :, cols].astype(F32) + pr[yy, :, :, cols].astype(F32)
        leaf[n, g] = send(line(n, 2, cols), lf.at[:, :, cols], nbr[axis, s])

    def scatter_raw(n, g):
        axis, s, _ = kinds[n]
        cols = piece_cols(n, g)
        raw[n, g] = send(line(n, -s % R, cols), rw.at[:, :, cols], nbr[axis, -s])

    def scatter_merge(n, g):
        axis, s, _ = kinds[n]
        cols = piece_cols(n, g)
        leaf[n, g].wait_recv()
        mg[:, :, cols] = lf[:, :, cols] + line(n, s % R, cols)[...]
        merged[n, g] = send(mg.at[:, :, cols], rm.at[:, :, cols], nbr[axis, s])

    def scatter_second(n, g):
        axis, s, _ = kinds[n]
        cols = piece_cols(n, g)
        raw[n, g].wait_recv()
        merged[n, g].wait_recv()
        sy[:, :, cols] = line(n, 0, cols)[...] + rm[:, :, cols] + rw[:, :, cols]
        direct = g >= MERGED
        leaf2[n, g] = send(sy.at[spot(n, 2), :, cols], lf2.at[:, cols], nbr[1 - axis, 2 if direct else s])
        if direct:
            merged2[n, g] = send(sy.at[spot(n, s % R), :, cols], rm2.at[:, cols], nbr[1 - axis, s])
        raw2[n, g] = send(sy.at[spot(n, -s % R), :, cols], rw2.at[:, cols], nbr[1 - axis, -s])

    def scatter_merge2(n, g):
        assert g < MERGED
        axis, s, _ = kinds[n]
        cols = piece_cols(n, g)
        leaf2[n, g].wait_recv()
        mg2[:, cols] = lf2[:, cols] + sy[spot(n, s % R), :, cols]
        merged2[n, g] = send(mg2.at[:, cols], rm2.at[:, cols], nbr[1 - axis, s])

    def scatter_last(n, g):
        cols = piece_cols(n, g)
        raw2[n, g].wait_recv()
        merged2[n, g].wait_recv()
        total = sy[spot(n, 0), :, cols] + rm2[:, cols] + rw2[:, cols]
        if g >= MERGED:
            leaf2[n, g].wait_recv()
            total = total + lf2[:, cols]
        dx_ref[:, cols] = total.astype(BF16)

    def pieces(f, g):
        for n in range(len(kinds)):
            f(n, g)

    def transposes():
        dg_t[...] = dgs[...].astype(F32).T.astype(BF16)
        du_t[...] = dus[...].astype(F32).T.astype(BF16)

    gd, gx = Gather(dyf, 1), Gather(xf, 0)
    only = ([], [])

    def on(core):
        def run(f):
            @pl.when(c == core)
            def _():
                n = len(sent)
                f()
                only[core].extend(sent[n:])
        return run

    cp_dy.wait()
    swap = []

    @on(0)
    def _():
        gd.first_direct(0)
        gd.second_home(0)
        swap.append(share(lambda: dyf.at[y, x, 0], mate))
        cp_x.wait()
        gx.first_send(0)
        cp_ug.wait()
        cp_uu.wait()
        prepare()

    @on(1)
    def _():
        gd.first_direct(1)
        gd.second_home(1)
        cp_x.wait()
        gx.first_send(1)
        swap.append(share(lambda: xf.at[y, x, 1], mate))
        cp_ug.wait()
        cp_uu.wait()
        prepare()
        gd.first_near()
        gd.second_send(R - 1)
        gd.second_send(1)
        gd.first_far()
        gd.second_send(2)
        gd.second_relay(0)
        swap[0].wait_recv()
        gd.home_to_mate()
        gd.second_relay(R - 1)
        gd.second_relay(1)
        gd.second_relay(2)
        gd.to_mate(R - 1)
        gd.to_mate(1)
        gx.second_home(1)
        gd.second_far(0)
        gd.spot_to_mate(0, 2)
        gd.second_far(R - 1)
        gd.spot_to_mate(R - 1, 2)
        gd.second_far(1)
        gd.spot_to_mate(1, 2)
        gd.second_far(2)
        gd.spot_to_mate(2, 2)
        cp_wd.wait()

    @on(0)
    def _():
        gx.first_relay()
        gd.mate_rows(0)
        gx.first_far()
        gd.mate_rows(R - 1)
        gd.mate_rows(1)
        gx.second_home(0)
        gx.second_send(R - 1)
        gx.second_send(1)
        gx.second_send(2)
        cp_wd.wait()
        gd.mate_rows(2)

    grads()

    def x_relay(d1):
        @on(0)
        def _():
            gx.second_relay(d1)

    cp_wg.wait()
    cp_wu.wait()
    partial(0, 0)
    partial(0, 1)
    partial(0, 2)
    partial(0, 3)
    scatter_first(0, 0)
    scatter_first(1, 0)
    x_relay(0)
    partial(1, 0)
    scatter_first(2, 0)
    scatter_first(3, 0)
    x_relay(R - 1)
    pieces(scatter_raw, 0)
    x_relay(1)
    partial(1, 1)
    x_relay(2)
    partial(1, 2)
    partial(1, 3)
    partial(2, 0, 1)
    scatter_first(0, 1)
    scatter_first(1, 1)
    partial(2, 2, 3)
    scatter_first(2, 1)
    scatter_first(3, 1)
    pieces(scatter_merge, 0)
    pieces(scatter_raw, 1)
    pieces(scatter_first, 2)

    @on(0)
    def _():
        swap[1].wait_recv()
        gx.home_to_mate()
        gx.to_mate(R - 1)
        gx.to_mate(1)

    pieces(scatter_merge, 1)
    pieces(scatter_raw, 2)
    transposes()
    pieces(scatter_second, 0)
    pieces(scatter_merge, 2)
    pieces(scatter_second, 1)
    pieces(scatter_merge2, 0)

    @on(0)
    def _():
        gx.second_far(0)
        gx.second_far(R - 1)
        gx.second_far(1)
        gx.second_far(2)
        gx.to_mate(2)

    pieces(scatter_second, 2)

    @on(1)
    def _():
        for d in range(R):
            gx.mate_rows(d)

    pieces(scatter_last, 0)
    pieces(scatter_last, 1)
    pieces(scatter_last, 2)
    common = [cp for cp in sent if not any(cp is other for other in only[0] + only[1])]
    for core in range(CORES):
        @on(core)
        def _():
            for cp in list(only[core]):
                cp.wait_send()

    for cp in common:
        cp.wait_send()
    assert len(sent) == n_copies, len(sent)


def weight_kernel(xf, dyf, dg_t, du_t, z_t, dx, og, ou, od, odx, buf, sem, dx_sem):
    slots, tile = buf.shape[1], buf.shape[3]
    tokens, hidden = dg_t.shape[1], og.shape[1]
    out = pltpu.make_async_copy(dx, odx, dx_sem)
    out.start()
    jobs = ((dg_t, xf, og), (du_t, xf, ou), (z_t, dyf, od))
    flight = {}
    for t in range(hidden // tile):
        cols = pl.ds(t * tile, tile)
        for i, (lhs, rhs, dst) in enumerate(jobs):
            slot = t % slots
            if (i, t - slots) in flight:
                flight[i, t - slots].wait()
            buf[i, slot] = jnp.dot(lhs[...], rhs[:, :, :, :, cols].reshape(tokens, tile), preferred_element_type=F32)
            flight[i, t] = pltpu.make_async_copy(buf.at[i, slot], dst.at[:, cols], sem.at[i, slot])
            flight[i, t].start()
    for t in range(hidden // tile - slots, hidden // tile):
        for i in range(len(jobs)):
            flight[i, t].wait()
    out.wait()


def solution(mesh):
    tp = mesh.shape["tp"]
    ring = math.isqrt(tp // CORES)

    def local_backward(x_loc, wg_loc, wu_loc, wd_loc, ug_loc, uu_loc, dy_loc):
        rows, hidden = x_loc.shape
        ffn = wd_loc.shape[0]
        tokens = tp * rows
        R = ring
        n_copies = 2 + 2 * (6 + 4 * R + 3 * R) + 2 * (8 + 4 * R + 2 * R - 1) + 4 * len(GROUPS) * 7
        full = (R, R, CORES, rows, hidden)
        vm = pltpu.VMEM
        out_bytes = 2 * (rows * hidden + 2 * tokens * hidden + 3 * ffn * tokens)
        dx, xf, dyf, dg_t, du_t, z_t = pl.pallas_call(
            lambda *refs: comm_kernel(R, n_copies, *refs),
            name="comm",
            out_shape=(vm((rows, hidden), BF16), vm(full, BF16), vm(full, BF16),
                       vm((ffn, tokens), BF16), vm((ffn, tokens), BF16), vm((ffn, tokens), BF16)),
            in_specs=[pl.BlockSpec(memory_space=pltpu.HBM)] * 7,
            out_specs=(pl.BlockSpec(memory_space=vm),) * 6,
            scratch_shapes=[
                vm((ffn, hidden), BF16), vm((ffn, hidden), BF16), vm((ffn, hidden), BF16),
                vm((ffn, tokens), BF16), vm((ffn, tokens), BF16),
                vm((tokens, ffn), F32), vm((tokens, ffn), F32), vm((tokens, ffn), F32),
                vm((tokens, ffn), BF16), vm((tokens, ffn), BF16),
                vm(full, BF16), vm((R, R, rows, hidden), BF16),
                vm((R, R, rows, hidden), F32), vm((R, rows, hidden), F32),
                *[vm((R, rows, hidden), F32)] * 4, *[vm((rows, hidden), F32)] * 4,
                pltpu.SemaphoreType.DMA((7,)),
                pltpu.SemaphoreType.DMA((n_copies,)),
                pltpu.SemaphoreType.DMA((n_copies,)),
            ],
            compiler_params=pltpu.CompilerParams(collective_id=0, has_side_effects=True,
                                                 vmem_limit_bytes=VMEM_BYTES - out_bytes - 40960),
        )(x_loc, dy_loc, wd_loc, wg_loc.T, wu_loc.T, ug_loc.T, uu_loc.T)
        out = jax.ShapeDtypeStruct((ffn, hidden), F32)
        hbm = pl.BlockSpec(memory_space=pltpu.HBM)
        gw_g, gw_u, gw_d, dx = pl.pallas_call(
            weight_kernel,
            name="weight_grads",
            out_shape=(out, out, out, jax.ShapeDtypeStruct((rows, hidden), BF16)),
            in_specs=[pl.BlockSpec(memory_space=vm)] * 6,
            out_specs=(hbm,) * 4,
            scratch_shapes=[vm((3, SLOTS, ffn, COL_TILE), F32), pltpu.SemaphoreType.DMA((3, SLOTS)),
                            pltpu.SemaphoreType.DMA],
            compiler_params=pltpu.CompilerParams(vmem_limit_bytes=24 << 20),
        )(xf, dyf, dg_t, du_t, z_t, dx)
        return dx, gw_g.T, gw_u.T, gw_d

    row_spec = P(("dp", "tp"), None)
    col_spec = P(None, "tp")
    part_cols = P("dp", "tp")
    return jax.shard_map(local_backward, mesh=mesh,
                         in_specs=(row_spec, col_spec, col_spec, P("tp", None), part_cols, part_cols, row_spec),
                         out_specs=(row_spec, part_cols, part_cols, row_spec),
                         check_vma=False)
```

```python
import functools
import math

import jax
import jax.numpy as jnp
from jax import lax
from jax.experimental import pallas as pl
from jax.experimental.pallas import tpu as pltpu
from jax.sharding import PartitionSpec as P

MESH = pl.DeviceIdType.MESH
BF16 = jnp.bfloat16
F32 = jnp.float32
CORES = 2
COL_TILE = 512
SLOTS = 4
MXU_TILE = 256
MERGED = 1
GROUPS = (2, 2, 1)
VMEM_BYTES = 67043328
NT = (((1,), (1,)), ((), ()))


def comm_kernel(ring, n_copies, x_hbm, dy_hbm, wd_hbm, wg_hbm, wu_hbm, ug_hbm, uu_hbm,
                dx_ref, xf, dyf, dg_t, du_t, z_t,
                wd, wg, wu, ug, uu, gate, up, mid, dgs, dus, pb, pr, sx, sy,
                lf, mg, rw, rm, lf2, mg2, rw2, rm2, lsem, ssem, rsem):
    R = ring
    me = lax.axis_index("tp")
    c = lax.rem(me, CORES)
    x = lax.rem(me // CORES, R)
    y = me // (CORES * R)
    oc = 1 - c
    rows, hidden = x_hbm.shape
    tokens = R * R * CORES * rows
    H2, Q = hidden // 2, hidden // 4
    xs = [lax.rem(x + d, R) for d in range(R)]
    ys = [lax.rem(y + d, R) for d in range(R)]

    def dev(yy, xx, cc):
        return {"tp": (yy * R + xx) * CORES + cc}

    def at(axis, s, core):
        return dev(y, xs[s % R], core) if axis == 0 else dev(ys[s % R], x, core)

    steps = [(axis, s) for axis in (0, 1) for s in (1, -1, 2)]
    nbr = {step: at(*step, c) for step in steps}
    across = {step: at(*step, oc) for step in steps}
    to_core = [{step: at(*step, core) for step in steps} for core in range(CORES)]
    mate = dev(y, x, oc)

    def local(src, dst, i):
        cp = pltpu.make_async_copy(src, dst, lsem.at[i])
        cp.start()
        return cp

    cp_dy = local(dy_hbm, dyf.at[y, x, c], 0)
    cp_x = local(x_hbm, xf.at[y, x, c], 1)
    cp_ug = local(ug_hbm, ug, 2)
    cp_uu = local(uu_hbm, uu, 3)
    cp_wd = local(wd_hbm, wd, 4)
    cp_wg = local(wg_hbm, wg, 5)
    cp_wu = local(wu_hbm, wu, 6)

    barrier = pltpu.get_barrier_semaphore()
    for d in (*nbr.values(), *across.values(), mate):
        pl.semaphore_signal(barrier, inc=1, device_id=d, device_id_type=MESH)
    pl.semaphore_wait(barrier, 2 * len(nbr) + 1)

    sent = []

    class Copy:
        def __init__(self, make, device):
            self.make, self.device, self.i = make, device, len(sent)
            sent.append(self)
            self.describe().start()

        def describe(self):
            src, dst = self.make()
            return pltpu.make_async_remote_copy(src_ref=src, dst_ref=dst, send_sem=ssem.at[self.i],
                                                recv_sem=rsem.at[self.i], device_id=self.device,
                                                device_id_type=MESH)

        def wait_recv(self):
            self.describe().wait_recv()

        def wait_send(self):
            self.describe().wait_send()

    def send(src, dst, device):
        return Copy(lambda: (src, dst), device)

    def share(make, device):
        return Copy(lambda: (make(), make()), device)

    class Half:
        def __init__(self, buf, first, own):
            self.buf, self.first, self.own = buf, first, own
            base = first * H2
            self.all, self.lo, self.hi = pl.ds(base, H2), pl.ds(base, Q), pl.ds(base + Q, Q)
            self.near, self.far, self.rows = {}, {}, {}

        def ref(self, d1, d2, cols, cores=slice(None)):
            if self.first == 0:
                return self.buf.at[ys[d2], xs[d1], cores, :, cols]
            return self.buf.at[ys[d1], xs[d2], cores, :, cols]

        def push(self, key, d1, axis, core=None):
            cores = slice(None) if core is None else pl.ds(core, 1)
            ref = functools.partial(self.ref, d1, 0, self.all, cores)
            to = to_core[self.own]
            self.near.setdefault(key, []).append((share(ref, to[axis, 1]), share(ref, to[axis, -1])))
            return ref

        def relay(self, key, minus, plus, axis):
            for cp, _ in self.near[key]:
                cp.wait_recv()
            a = share(functools.partial(self.ref, *minus, self.lo), nbr[axis, 1])
            for _, cp in self.near[key]:
                cp.wait_recv()
            self.far[key] = [a, share(functools.partial(self.ref, *plus, self.hi), nbr[axis, -1])]

        def first_send(self, core):
            self.push("f", 0, self.first, core)

        def first_direct(self, core):
            ref = self.push("f", 0, self.first, core)
            self.far.setdefault("f", []).append(share(ref, to_core[self.own][self.first, 2]))

        def first_near(self):
            for pair in self.near["f"]:
                for cp in pair:
                    cp.wait_recv()

        def first_relay(self):
            self.relay("f", (R - 1, 0), (1, 0), self.first)

        def first_far(self):
            for cp in self.far["f"]:
                cp.wait_recv()

        def second_home(self, core):
            self.push(0, 0, 1 - self.first, core)

        def second_send(self, d1):
            self.push(d1, d1, 1 - self.first)

        def second_relay(self, d1):
            self.relay(d1, (d1, R - 1), (d1, 1), 1 - self.first)

        def second_far(self, d1):
            for cp in self.far[d1]:
                cp.wait_recv()

        def to_mate(self, d2):
            def ref():
                if self.first == 0:
                    return self.buf.at[ys[d2], :, :, :, self.all]
                return self.buf.at[:, xs[d2], :, :, self.all]

            self.rows[d2] = share(ref, mate)

        def spot_to_mate(self, d1, d2, cores=slice(None)):
            self.rows[d1, d2] = share(functools.partial(self.ref, d1, d2, self.all, cores), mate)

        def home_to_mate(self):
            self.spot_to_mate(0, 0, pl.ds(self.own, 1))
            for d1 in range(1, R):
                self.spot_to_mate(d1, 0)

        def mate_rows(self, row):
            for key, cp in self.rows.items():
                if key == row or (isinstance(key, tuple) and key[1] == row):
                    cp.wait_recv()

    class Gather:
        def __init__(self, buf, own):
            self.halves = (Half(buf, 0, own), Half(buf, 1, own))

        def __getattr__(self, name):
            def both(*args):
                for h in self.halves:
                    getattr(h, name)(*args)
            return both

    def prepare():
        g_f = ug[...].astype(F32)
        u_f = uu[...].astype(F32)
        z_t[...] = (g_f * jax.nn.sigmoid(g_f) * u_f).astype(BF16)
        gate[...] = g_f.T
        up[...] = u_f.T

    def grads():
        mid[...] = lax.dot_general(dyf[...].reshape(tokens, hidden), wd[...], NT, preferred_element_type=F32)
        step = tokens // 8
        for i in range(8):
            tok = pl.ds(i * step, step)
            g_mid, g_f, u_f = mid[tok, :], gate[tok, :], up[tok, :]
            s = jax.nn.sigmoid(g_f)
            dgs[tok, :] = (g_mid * u_f * s * (1.0 + g_f * (1.0 - s))).astype(BF16)
            dus[tok, :] = (g_mid * (g_f * s)).astype(BF16)

    kinds = ((0, 1, 0), (1, 1, H2), (0, -1, Q), (1, -1, H2 + Q))
    widths = [t * MXU_TILE for t in GROUPS]
    starts = [sum(widths[:g]) for g in range(len(widths))]
    pair, leaf, raw, merged, leaf2, raw2, merged2 = {}, {}, {}, {}, {}, {}, {}

    def piece_cols(n, g):
        return pl.ds(kinds[n][2] + starts[g], widths[g])

    def partial(g, *ns):
        dg, du = dgs[...], dus[...]
        for n in ns:
            for t in range(GROUPS[g]):
                cols = pl.ds(kinds[n][2] + starts[g] + t * MXU_TILE, MXU_TILE)
                p = (jnp.dot(dg, wg[:, cols], preferred_element_type=F32)
                     + jnp.dot(du, wu[:, cols], preferred_element_type=F32))
                pb[:, :, :, :, cols] = p.astype(BF16).reshape(R, R, CORES, rows, MXU_TILE)
        for n in ns:
            cols = piece_cols(n, g)
            pair[n, g] = send(pb.at[:, :, oc, :, cols], pr.at[:, :, :, cols], mate)

    def line(n, d, cols):
        if kinds[n][0] == 0:
            return sx.at[:, xs[d], :, cols]
        return sx.at[ys[d], :, :, cols]

    def spot(n, d):
        return (ys if kinds[n][0] == 0 else xs)[d]

    def scatter_first(n, g):
        axis, s, _ = kinds[n]
        cols = piece_cols(n, g)
        pair[n, g].wait_recv()
        for yy in range(R):
            sx[yy, :, :, cols] = pb[yy, :, c, :, cols].astype(F32) + pr[yy, :, :, cols].astype(F32)
        leaf[n, g] = send(line(n, 2, cols), lf.at[:, :, cols], nbr[axis, s])

    def scatter_raw(n, g):
        axis, s, _ = kinds[n]
        cols = piece_cols(n, g)
        raw[n, g] = send(line(n, -s % R, cols), rw.at[:, :, cols], nbr[axis, -s])

    def scatter_merge(n, g):
        axis, s, _ = kinds[n]
        cols = piece_cols(n, g)
        leaf[n, g].wait_recv()
        mg[:, :, cols] = lf[:, :, cols] + line(n, s % R, cols)[...]
        merged[n, g] = send(mg.at[:, :, cols], rm.at[:, :, cols], nbr[axis, s])

    def scatter_second(n, g):
        axis, s, _ = kinds[n]
        cols = piece_cols(n, g)
        raw[n, g].wait_recv()
        merged[n, g].wait_recv()
        sy[:, :, cols] = line(n, 0, cols)[...] + rm[:, :, cols] + rw[:, :, cols]
        direct = g >= MERGED
        leaf2[n, g] = send(sy.at[spot(n, 2), :, cols], lf2.at[:, cols], nbr[1 - axis, 2 if direct else s])
        if direct:
            merged2[n, g] = send(sy.at[spot(n, s % R), :, cols], rm2.at[:, cols], nbr[1 - axis, s])
        raw2[n, g] = send(sy.at[spot(n, -s % R), :, cols], rw2.at[:, cols], nbr[1 - axis, -s])

    def scatter_merge2(n, g):
        assert g < MERGED
        axis, s, _ = kinds[n]
        cols = piece_cols(n, g)
        leaf2[n, g].wait_recv()
        mg2[:, cols] = lf2[:, cols] + sy[spot(n, s % R), :, cols]
        merged2[n, g] = send(mg2.at[:, cols], rm2.at[:, cols], nbr[1 - axis, s])

    def scatter_last(n, g):
        cols = piece_cols(n, g)
        raw2[n, g].wait_recv()
        merged2[n, g].wait_recv()
        total = sy[spot(n, 0), :, cols] + rm2[:, cols] + rw2[:, cols]
        if g >= MERGED:
            leaf2[n, g].wait_recv()
            total = total + lf2[:, cols]
        dx_ref[:, cols] = total.astype(BF16)

    def pieces(f, g):
        for n in range(len(kinds)):
            f(n, g)

    def transposes():
        dg_t[...] = dgs[...].astype(F32).T.astype(BF16)
        du_t[...] = dus[...].astype(F32).T.astype(BF16)

    gd, gx = Gather(dyf, 1), Gather(xf, 0)
    only = ([], [])

    def on(core):
        def run(f):
            @pl.when(c == core)
            def _():
                n = len(sent)
                f()
                only[core].extend(sent[n:])
        return run

    cp_dy.wait()
    swap = []

    @on(0)
    def _():
        gd.first_direct(0)
        gd.second_home(0)
        swap.append(share(lambda: dyf.at[y, x, 0], mate))
        cp_x.wait()
        gx.first_send(0)
        cp_ug.wait()
        cp_uu.wait()
        prepare()

    @on(1)
    def _():
        gd.first_direct(1)
        gd.second_home(1)
        cp_x.wait()
        gx.first_send(1)
        swap.append(share(lambda: xf.at[y, x, 1], mate))
        cp_ug.wait()
        cp_uu.wait()
        prepare()
        gd.first_near()
        gd.second_send(R - 1)
        gd.second_send(1)
        gd.first_far()
        gd.second_send(2)
        gd.second_relay(0)
        swap[0].wait_recv()
        gd.home_to_mate()
        gd.second_relay(R - 1)
        gd.second_relay(1)
        gd.second_relay(2)
        gd.to_mate(R - 1)
        gd.to_mate(1)
        gx.second_home(1)
        gd.second_far(0)
        gd.spot_to_mate(0, 2)
        gd.second_far(R - 1)
        gd.spot_to_mate(R - 1, 2)
        gd.second_far(1)
        gd.spot_to_mate(1, 2)
        gd.second_far(2)
        gd.spot_to_mate(2, 2)
        cp_wd.wait()

    @on(0)
    def _():
        gx.first_relay()
        gd.mate_rows(0)
        gx.first_far()
        gd.mate_rows(R - 1)
        gd.mate_rows(1)
        gx.second_home(0)
        gx.second_send(R - 1)
        gx.second_send(1)
        gx.second_send(2)
        cp_wd.wait()
        gd.mate_rows(2)

    grads()

    @on(0)
    def _():
        gx.second_relay(0)

    cp_wg.wait()
    cp_wu.wait()
    partial(0, 0)
    partial(0, 1)
    partial(0, 2)

    @on(0)
    def _():
        gx.second_relay(R - 1)

    partial(0, 3)
    scatter_first(0, 0)
    scatter_first(1, 0)
    partial(1, 0)
    scatter_first(2, 0)
    scatter_first(3, 0)

    @on(0)
    def _():
        gx.second_relay(1)

    pieces(scatter_raw, 0)
    partial(1, 1)
    partial(1, 2)

    @on(0)
    def _():
        gx.second_relay(2)

    partial(1, 3)
    partial(2, 0, 1)
    scatter_first(0, 1)
    scatter_first(1, 1)
    scatter_first(2, 1)
    scatter_first(3, 1)
    pieces(scatter_merge, 0)
    partial(2, 2, 3)
    pieces(scatter_raw, 1)
    pieces(scatter_first, 2)

    @on(0)
    def _():
        swap[1].wait_recv()
        gx.home_to_mate()
        gx.to_mate(R - 1)
        gx.to_mate(1)

    pieces(scatter_merge, 1)
    pieces(scatter_raw, 2)
    transposes()
    pieces(scatter_second, 0)
    pieces(scatter_merge, 2)
    pieces(scatter_merge2, 0)
    pieces(scatter_second, 1)

    @on(0)
    def _():
        gx.second_far(0)
        gx.second_far(R - 1)
        gx.second_far(1)
        gx.second_far(2)
        gx.to_mate(2)

    pieces(scatter_second, 2)

    @on(1)
    def _():
        for d in range(R):
            gx.mate_rows(d)

    pieces(scatter_last, 0)
    pieces(scatter_last, 1)
    pieces(scatter_last, 2)
    common = [cp for cp in sent if not any(cp is other for other in only[0] + only[1])]
    for core in range(CORES):
        @on(core)
        def _():
            for cp in list(only[core]):
                cp.wait_send()

    for cp in common:
        cp.wait_send()
    assert len(sent) == n_copies, len(sent)


def weight_kernel(xf, dyf, dg_t, du_t, z_t, dx, og, ou, od, odx, buf, sem, dx_sem):
    slots, tile = buf.shape[1], buf.shape[3]
    tokens, hidden = dg_t.shape[1], og.shape[1]
    out = pltpu.make_async_copy(dx, odx, dx_sem)
    out.start()
    jobs = ((dg_t, xf, og), (du_t, xf, ou), (z_t, dyf, od))
    flight = {}
    for t in range(hidden // tile):
        cols = pl.ds(t * tile, tile)
        for i, (lhs, rhs, dst) in enumerate(jobs):
            slot = t % slots
            if (i, t - slots) in flight:
                flight[i, t - slots].wait()
            buf[i, slot] = jnp.dot(lhs[...], rhs[:, :, :, :, cols].reshape(tokens, tile), preferred_element_type=F32)
            flight[i, t] = pltpu.make_async_copy(buf.at[i, slot], dst.at[:, cols], sem.at[i, slot])
            flight[i, t].start()
    for t in range(hidden // tile - slots, hidden // tile):
        for i in range(len(jobs)):
            flight[i, t].wait()
    out.wait()


def solution(mesh):
    tp = mesh.shape["tp"]
    ring = math.isqrt(tp // CORES)

    def local_backward(x_loc, wg_loc, wu_loc, wd_loc, ug_loc, uu_loc, dy_loc):
        rows, hidden = x_loc.shape
        ffn = wd_loc.shape[0]
        tokens = tp * rows
        R = ring
        n_copies = 2 + 2 * (6 + 4 * R + 3 * R) + 2 * (8 + 4 * R + 2 * R - 1) + 4 * len(GROUPS) * 7
        full = (R, R, CORES, rows, hidden)
        vm = pltpu.VMEM
        out_bytes = 2 * (rows * hidden + 2 * tokens * hidden + 3 * ffn * tokens)
        dx, xf, dyf, dg_t, du_t, z_t = pl.pallas_call(
            lambda *refs: comm_kernel(R, n_copies, *refs),
            name="comm",
            out_shape=(vm((rows, hidden), BF16), vm(full, BF16), vm(full, BF16),
                       vm((ffn, tokens), BF16), vm((ffn, tokens), BF16), vm((ffn, tokens), BF16)),
            in_specs=[pl.BlockSpec(memory_space=pltpu.HBM)] * 7,
            out_specs=(pl.BlockSpec(memory_space=vm),) * 6,
            scratch_shapes=[
                vm((ffn, hidden), BF16), vm((ffn, hidden), BF16), vm((ffn, hidden), BF16),
                vm((ffn, tokens), BF16), vm((ffn, tokens), BF16),
                vm((tokens, ffn), F32), vm((tokens, ffn), F32), vm((tokens, ffn), F32),
                vm((tokens, ffn), BF16), vm((tokens, ffn), BF16),
                vm(full, BF16), vm((R, R, rows, hidden), BF16),
                vm((R, R, rows, hidden), F32), vm((R, rows, hidden), F32),
                *[vm((R, rows, hidden), F32)] * 4, *[vm((rows, hidden), F32)] * 4,
                pltpu.SemaphoreType.DMA((7,)),
                pltpu.SemaphoreType.DMA((n_copies,)),
                pltpu.SemaphoreType.DMA((n_copies,)),
            ],
            compiler_params=pltpu.CompilerParams(collective_id=0, has_side_effects=True,
                                                 vmem_limit_bytes=VMEM_BYTES - out_bytes - 40960),
        )(x_loc, dy_loc, wd_loc, wg_loc.T, wu_loc.T, ug_loc.T, uu_loc.T)
        out = jax.ShapeDtypeStruct((ffn, hidden), F32)
        hbm = pl.BlockSpec(memory_space=pltpu.HBM)
        gw_g, gw_u, gw_d, dx = pl.pallas_call(
            weight_kernel,
            name="weight_grads",
            out_shape=(out, out, out, jax.ShapeDtypeStruct((rows, hidden), BF16)),
            in_specs=[pl.BlockSpec(memory_space=vm)] * 6,
            out_specs=(hbm,) * 4,
            scratch_shapes=[vm((3, SLOTS, ffn, COL_TILE), F32), pltpu.SemaphoreType.DMA((3, SLOTS)),
                            pltpu.SemaphoreType.DMA],
            compiler_params=pltpu.CompilerParams(vmem_limit_bytes=24 << 20),
        )(xf, dyf, dg_t, du_t, z_t, dx)
        return dx, gw_g.T, gw_u.T, gw_d

    row_spec = P(("dp", "tp"), None)
    col_spec = P(None, "tp")
    part_cols = P("dp", "tp")
    return jax.shard_map(local_backward, mesh=mesh,
                         in_specs=(row_spec, col_spec, col_spec, P("tp", None), part_cols, part_cols, row_spec),
                         out_specs=(row_spec, part_cols, part_cols, row_spec),
                         check_vma=False)
```
